32 devices in a mesh: replica: 1 (over z), yz: 4 (over y), x: 8 (over x, core).
Axes of the slice: x: 4, y: 4, z: 1, core: 2. Of those that a mesh axis runs over, the one named last changes fastest.
The devices are a block of a 4x4x8 slice.
Arguments:
- hidden: bfloat16 [512, 1536], P('replica', ('x', 'yz'))
- seq_lens: int32 [512], P(('replica', 'yz', 'x'))
- attn_gain: bfloat16 [1, 1536], replicated
- mlp_gain: bfloat16 [1, 1536], replicated
- w_qkv: bfloat16 [1, 1536, 1792], P(None, None, 'yz')
- w_out: bfloat16 [1, 1536, 1536], P(None, 'yz')
- w_gate_up: bfloat16 [1, 1536, 2, 8960], P(None, None, None, 'yz')
- w_down: bfloat16 [1, 8960, 1536], P(None, 'yz')
- k_cache: bfloat16 [1, 512, 2048, 128], P(None, ('replica', 'yz', 'x'))
- v_cache: bfloat16 [1, 512, 2048, 128], P(None, ('replica', 'yz', 'x'))
Outputs:
- output 1: bfloat16 [512, 1536], P('replica', ('x', 'yz'))
- output 2: bfloat16 [1, 512, 2048, 128], P(None, ('replica', 'yz', 'x'))
- output 3: bfloat16 [1, 512, 2048, 128], P(None, ('replica', 'yz', 'x'))
All inputs are finite; a program needn't handle non-finite values.
Results may differ from the reference program's by a relative error of at most 0.0155586.
Values are sent between devices in bfloat16 or wider.
A program may use at most 768 MiB of HBM per device.

```python
import jax
import jax.numpy as jnp
from jax import lax

MODEL_DIM = 1536
Q_HEADS = 12
HEAD_DIM = 128
FFN_DIM = 8960
LAYERS = 1
SEQ_LEN = 2048
PART_BATCH = 512
BLOCK_ROWS = 8
ATTN_WIDTH = Q_HEADS * HEAD_DIM
QKV_WIDTH = ATTN_WIDTH + 2 * HEAD_DIM
NORM_EPS = 1e-5


def setup_inputs(seed: int = 0, part: int = 0) -> dict:
    root_key = jax.random.key(seed)
    shared = jax.random.split(root_key, 6)
    own_keys = jax.random.split(jax.random.fold_in(root_key, part), 6)
    cache_shape = (LAYERS, PART_BATCH, SEQ_LEN, HEAD_DIM)
    profile = 0.3 + 1.7 * jnp.arange(MODEL_DIM, dtype=jnp.float32) / MODEL_DIM
    row_scale = jnp.exp(0.5 * jax.random.normal(own_keys[0], (PART_BATCH, 1), jnp.float32))
    hidden = jax.random.normal(own_keys[1], (PART_BATCH, MODEL_DIM), jnp.float32) * profile * row_scale
    seq_lens = jax.random.randint(own_keys[2], (PART_BATCH,), 1, SEQ_LEN, dtype=jnp.int32)
    seq_lens = seq_lens.at[0].set(SEQ_LEN - 1).at[1].set(1)
    attn_gain = 1.0 + 0.5 * jax.random.normal(shared[0], (LAYERS, MODEL_DIM), jnp.float32)
    mlp_gain = 1.0 + 0.5 * jax.random.normal(shared[1], (LAYERS, MODEL_DIM), jnp.float32)
    w_qkv = jax.random.normal(shared[2], (LAYERS, MODEL_DIM, QKV_WIDTH), jnp.float32) * MODEL_DIM ** -0.5
    w_out = jax.random.normal(shared[3], (LAYERS, ATTN_WIDTH, MODEL_DIM), jnp.float32) * ATTN_WIDTH ** -0.5
    w_gate_up = jax.random.normal(shared[4], (LAYERS, MODEL_DIM, 2, FFN_DIM), jnp.float32) * MODEL_DIM ** -0.5
    w_down = jax.random.normal(shared[5], (LAYERS, FFN_DIM, MODEL_DIM), jnp.float32) * FFN_DIM ** -0.5
    k_cache = 2.0 * jax.random.normal(own_keys[3], cache_shape, jnp.float32)
    rand_walk = jnp.cumsum(jax.random.normal(own_keys[4], cache_shape, jnp.float32), axis=2)
    v_cache = rand_walk * (2.0 / SEQ_LEN ** 0.5) + jax.random.normal(own_keys[5], cache_shape, jnp.float32)
    return {
        'hidden': hidden.astype(jnp.bfloat16),
        'seq_lens': seq_lens,
        'attn_gain': attn_gain.astype(jnp.bfloat16),
        'mlp_gain': mlp_gain.astype(jnp.bfloat16),
        'w_qkv': w_qkv.astype(jnp.bfloat16),
        'w_out': w_out.astype(jnp.bfloat16),
        'w_gate_up': w_gate_up.astype(jnp.bfloat16),
        'w_down': w_down.astype(jnp.bfloat16),
        'k_cache': k_cache.astype(jnp.bfloat16),
        'v_cache': v_cache.astype(jnp.bfloat16),
    }


def rms_bf16(hid_state, gain):
    hid_f = hid_state.astype(jnp.float32)
    inv_scale = lax.rsqrt(jnp.mean(hid_f * hid_f, axis=-1, keepdims=True) + NORM_EPS)
    return (hid_f * inv_scale * gain.astype(jnp.float32)).astype(jnp.bfloat16)


def attend_block(row_block):
    z_rows, k_layer, v_layer, lens_blk = row_block
    queries = z_rows[:, :ATTN_WIDTH].reshape(BLOCK_ROWS, Q_HEADS, HEAD_DIM)
    k_new = z_rows[:, ATTN_WIDTH:ATTN_WIDTH + HEAD_DIM]
    v_new = z_rows[:, ATTN_WIDTH + HEAD_DIM:]
    slot_ids = jnp.arange(SEQ_LEN)
    at_slot = (slot_ids[None, :] == lens_blk[:, None])[:, :, None]
    k_upd = jnp.where(at_slot, k_new[:, None, :], k_layer)
    v_upd = jnp.where(at_slot, v_new[:, None, :], v_layer)
    scores = jnp.einsum('bhd,bsd->bhs', queries.astype(jnp.float32), k_upd.astype(jnp.float32)) * HEAD_DIM ** -0.5
    visible = (slot_ids[None, :] <= lens_blk[:, None])[:, None, :]
    scores = jnp.where(visible, scores, -1e30)
    probs_bf = jax.nn.softmax(scores, axis=-1).astype(jnp.bfloat16)
    outputs = jnp.einsum('bhs,bsd->bhd', probs_bf.astype(jnp.float32), v_upd.astype(jnp.float32)).astype(jnp.bfloat16)
    return outputs.reshape(BLOCK_ROWS, ATTN_WIDTH), k_upd, v_upd


def reference(hidden, seq_lens, attn_gain, mlp_gain, w_qkv, w_out, w_gate_up, w_down, k_cache, v_cache):
    num_blocks = PART_BATCH // BLOCK_ROWS

    def layer_step(hid_state, per_layer):
        gain_attn, gain_mlp, layer_qkv, layer_out, layer_gu, layer_down, k_layer, v_layer = per_layer
        normed = rms_bf16(hid_state, gain_attn)
        z_rows = jnp.dot(normed, layer_qkv, preferred_element_type=jnp.float32).astype(jnp.bfloat16)
        attn_out, k_upd, v_upd = lax.map(attend_block, (
            z_rows.reshape(num_blocks, BLOCK_ROWS, QKV_WIDTH),
            k_layer.reshape(num_blocks, BLOCK_ROWS, SEQ_LEN, HEAD_DIM),
            v_layer.reshape(num_blocks, BLOCK_ROWS, SEQ_LEN, HEAD_DIM),
            seq_lens.reshape(num_blocks, BLOCK_ROWS)))
        attn_out = attn_out.reshape(PART_BATCH, ATTN_WIDTH)
        hid_state = (hid_state.astype(jnp.float32) + jnp.dot(attn_out, layer_out, preferred_element_type=jnp.float32)).astype(jnp.bfloat16)
        normed = rms_bf16(hid_state, gain_mlp)
        gate_up = jnp.dot(normed, layer_gu.reshape(MODEL_DIM, 2 * FFN_DIM), preferred_element_type=jnp.float32).astype(jnp.bfloat16)
        gate_val = gate_up[:, :FFN_DIM].astype(jnp.float32)
        up_val = gate_up[:, FFN_DIM:].astype(jnp.float32)
        mlp_mixed = (jax.nn.silu(gate_val) * up_val).astype(jnp.bfloat16)
        hid_state = (hid_state.astype(jnp.float32) + jnp.dot(mlp_mixed, layer_down, preferred_element_type=jnp.float32)).astype(jnp.bfloat16)
        return hid_state, (k_upd.reshape(PART_BATCH, SEQ_LEN, HEAD_DIM), v_upd.reshape(PART_BATCH, SEQ_LEN, HEAD_DIM))

    hidden_out, caches = lax.scan(layer_step, hidden, (attn_gain, mlp_gain, w_qkv, w_out, w_gate_up, w_down, k_cache, v_cache))
    return hidden_out, caches[0], caches[1]
```

```python
import functools

import jax
import jax.numpy as jnp
from jax import lax
from jax.experimental import pallas as pl
from jax.experimental.pallas import tpu as pltpu
from jax.sharding import PartitionSpec as P

NORM_EPS = 1e-5
MESH = pl.DeviceIdType.MESH
F32 = jnp.float32
BF16 = jnp.bfloat16
NT = (((1,), (1,)), ((), ()))
NN = (((1,), (0,)), ((), ()))


def lane_ids(shape):
    return lax.broadcasted_iota(jnp.int32, shape, len(shape) - 1)


def lane_roll(v, shift):
    shift = shift % v.shape[-1]
    return v if shift == 0 else pltpu.roll(v, shift, v.ndim - 1)


def position(ny, nx):
    return lax.axis_index('yz'), lax.axis_index('x')


def peer(y, x, d, ny, nx):
    dy, dx = d // nx, d % nx
    ahead = ((y + dy) % ny, (x + dx) % nx)
    return ahead


def greet_all(y, x, ny, nx):
    barrier = pltpu.get_barrier_semaphore()
    total = ny * nx

    def hello(d, carry):
        py, px = peer(y, x, d, ny, nx)
        pl.semaphore_signal(barrier, inc=1, device_id={'yz': py, 'x': px}, device_id_type=MESH)
        return carry

    lax.fori_loop(1, total, hello, 0)
    return barrier


def remote(src, dst, send_sem, recv_sem, py, px):
    return pltpu.make_async_remote_copy(src_ref=src, dst_ref=dst, send_sem=send_sem, recv_sem=recv_sem,
                                        device_id={'yz': py, 'x': px}, device_id_type=MESH)


def qkv_kernel(ny, nx, cols, rows, width, ht_ref, gain_ref, w_hbm, z_ref, hrow_ref,
               send_buf, recv_buf, w_vmem, gain_col, h_full, u_full, zt_buf, z_send, z_recv, h_rows,
               w_sem, send_sem, recv_sem, zsend_sem, zrecv_sem):
    y, x = position(ny, nx)
    total = ny * nx
    me = x * ny + y
    qcols = w_hbm.shape[0]
    w_copy = pltpu.make_async_copy(w_hbm, w_vmem.at[pl.ds(0, qcols)], w_sem)
    w_copy.start()
    barrier = greet_all(y, x, ny, nx)

    lane = lane_ids((cols, 128))
    lane16 = lane_ids((16, 128))
    tiles = [ht_ref[:, 128 * t:128 * (t + 1)].astype(F32) for t in range(ny)]
    for px in range(nx):
        block = jnp.zeros((cols, 128), F32)
        for t in range(ny):
            piece = lane_roll(tiles[t], rows * t - rows * px)
            block = jnp.where((lane >= rows * t) & (lane < rows * (t + 1)), piece, block)
        high = lane_roll(block[32:48], 64)
        send_buf[px, 0:16] = jnp.where(lane16 < 64, block[0:16], high).astype(BF16)
        send_buf[px, 16:32] = block[16:32].astype(BF16)

    pl.semaphore_wait(barrier, total - 1)

    def send(d, carry):
        py, px = peer(y, x, d, ny, nx)
        remote(send_buf.at[px], recv_buf.at[me], send_sem.at[d], recv_sem.at[d], py, px).start()
        return carry

    lax.fori_loop(1, total, send, 0)
    recv_buf[me] = send_buf[x]

    for j in range(width // 128):
        row = gain_ref[0:1, 128 * j:128 * (j + 1)].astype(F32)
        gain_col[128 * j:128 * (j + 1), :] = jnp.transpose(jnp.broadcast_to(row, (128, 128)))
    w_vmem[qcols:, :] = jnp.zeros((w_vmem.shape[0] - qcols, width), BF16)

    def land(d, carry):
        py, px = peer(y, x, d, ny, nx)
        remote(send_buf.at[px], recv_buf.at[me], send_sem.at[d], recv_sem.at[d], py, px).wait()
        return carry

    lax.fori_loop(1, total, land, 0)

    square = jnp.zeros((16, 128), F32)
    for s in range(total):
        low = recv_buf[s, 0:16].astype(F32)
        mid = recv_buf[s, 16:32].astype(F32)
        high = lane_roll(low, 64)
        h_full[cols * s:cols * s + 16, :] = low
        h_full[cols * s + 16:cols * s + 32, :] = mid
        h_full[cols * s + 32:cols * s + 48, :] = high
        square = square + low * low + mid * mid + high * high
    power = jnp.sum(square, axis=0, keepdims=True)
    inv = lax.rsqrt(power / width + NORM_EPS)
    u_full[...] = (h_full[...] * inv * gain_col[...]).astype(BF16)
    w_copy.wait()
    zt_buf[...] = lax.dot_general(w_vmem[...], u_full[...], NN, preferred_element_type=F32)
    for j in range(zt_buf.shape[0] // 128):
        zj = jnp.transpose(zt_buf[128 * j:128 * (j + 1), :])
        for t in range(ny):
            z_send[t, :, 128 * j:128 * (j + 1)] = zj[rows * t:rows * (t + 1)].astype(BF16)
    for d in range(1, ny):
        py = (y + d) % ny
        remote(z_send.at[py], z_recv.at[y], zsend_sem.at[d], zrecv_sem.at[d], py, x).start()
    z_recv[y] = z_send[y]

    for j in range(width // 128):
        h_rows[:, 128 * j:128 * (j + 1)] = jnp.transpose(h_full[128 * j:128 * (j + 1), :])
    hrow_ref[...] = h_rows[pl.ds(pl.multiple_of(y * rows, rows), rows), :]

    for d in range(1, ny):
        py = (y + d) % ny
        remote(z_send.at[py], z_recv.at[y], zsend_sem.at[d], zrecv_sem.at[d], py, x).wait()

    zs = [[z_recv[t, :, 128 * j:128 * (j + 1)].astype(F32) for j in range(w_vmem.shape[0] // 128)] for t in range(ny)]
    for g in range(ny * qcols // 128):
        start = 128 * g
        t = start // qcols
        off = start - t * qcols
        j, sh = off // 128, off % 128
        take = min(128, qcols - off)
        out = lane_roll(zs[t][j], -sh)
        if sh and take > 128 - sh:
            out = jnp.where(lane16 < 128 - sh, out, lane_roll(zs[t][j + 1], -sh))
        if take < 128:
            out = jnp.where(lane16 < take, out, lane_roll(zs[t + 1][0], take))
        z_ref[:, g, :] = out
    for g in range(ny * qcols // 128, z_ref.shape[1]):
        z_ref[:, g, :] = jnp.zeros((rows, 128), F32)


def attend_kernel(heads, scale, len_ref, z_ref, k_ref, v_ref, o_ref, ko_ref, vo_ref, o_acc):
    b = pl.program_id(0)
    slots = k_ref.shape[1]
    length = len_ref[b]
    base = pl.multiple_of((length // 16) * 16, 16)
    here = lax.broadcasted_iota(jnp.int32, (16, 128), 0) == length - base
    z = z_ref[b]
    ko_ref[...] = k_ref[...]
    vo_ref[...] = v_ref[...]
    k_new = jnp.broadcast_to(z[heads:heads + 1], (16, 128)).astype(BF16)
    v_new = jnp.broadcast_to(z[heads + 1:heads + 2], (16, 128)).astype(BF16)
    ko_ref[0, pl.ds(base, 16), :] = jnp.where(here, k_new, k_ref[0, pl.ds(base, 16), :])
    vo_ref[0, pl.ds(base, 16), :] = jnp.where(here, v_new, v_ref[0, pl.ds(base, 16), :])
    s = lax.dot_general(z.astype(BF16), ko_ref[0], NT, preferred_element_type=F32) * scale
    s = jnp.where(lane_ids(s.shape) <= length, s, -1e30)
    e = jnp.exp(s - jnp.max(s, axis=1, keepdims=True))
    p = (e / jnp.sum(e, axis=1, keepdims=True)).astype(BF16)
    o_acc[b] = lax.dot_general(p, vo_ref[0], NN, preferred_element_type=F32)

    @pl.when(b == pl.num_programs(0) - 1)
    def _():
        for h in range(heads):
            o_ref[h] = o_acc[:, h, :].astype(BF16)


def mlp_kernel(ny, nx, cols, rows, width, heads, o_ref, hrow_ref, gain_ref, wo_hbm, wgu_hbm, wd_hbm, out_ref,
               wo, wgu, wd, o_recv, part, p_send, p_recv, hm_send, hm_recv, hm_cols, tail, u_full, m_cols, m_rows,
               f_part, f_cols, f_send, f_recv,
               wo_sem, wgu_sem, wd_sem, os_sem, or_sem, ps_sem, pr_sem, hs_sem, hr_sem, fs_sem, fr_sem):
    y, x = position(ny, nx)
    total = ny * nx
    me = x * ny + y
    slot = y * nx + x
    heads_y = heads // ny
    many = ny * rows
    ffn = wgu_hbm.shape[1]
    chunk = wgu_sem.shape[0]
    step = ffn // chunk
    wo_copy = pltpu.make_async_copy(wo_hbm, wo, wo_sem)
    wo_copy.start()
    wgu_copies = []
    for c in range(chunk):
        wgu_copies.append(pltpu.make_async_copy(wgu_hbm.at[:, pl.ds(c * step, step)], wgu.at[:, pl.ds(c * step, step)], wgu_sem.at[c]))
        wgu_copies[-1].start()
    wd_copy = pltpu.make_async_copy(wd_hbm, wd.at[pl.ds(0, ffn)], wd_sem)
    wd_copy.start()
    barrier = greet_all(y, x, ny, nx)
    wd[ffn:, :] = jnp.zeros((wd.shape[0] - ffn, width), BF16)
    m_cols[ffn:, :] = jnp.zeros((m_cols.shape[0] - ffn, 128), F32)
    f_part[many:, :] = jnp.zeros((f_part.shape[0] - many, width), F32)
    pl.semaphore_wait(barrier, total - 1)

    def o_copy(d):
        py = (y + d) % ny
        return remote(o_ref.at[pl.ds(py * heads_y, heads_y)], o_recv.at[y], os_sem.at[d], or_sem.at[d], py, x)

    for d in range(1, ny):
        o_copy(d).start()
    o_recv[y] = o_ref[pl.ds(y * heads_y, heads_y)]
    for d in range(1, ny):
        o_copy(d).wait()
    wo_copy.wait()
    o_rows = [jnp.concatenate([o_recv[t, h] for t in range(ny)], axis=0) for h in range(heads_y)]
    o_full = jnp.concatenate(o_rows, axis=1)
    part[...] = lax.dot_general(o_full, wo[...], NN, preferred_element_type=F32)
    for t in range(ny):
        p_send[t] = part[rows * t:rows * (t + 1), :].astype(BF16)

    def p_copy(d):
        py = (y + d) % ny
        return remote(p_send.at[py], p_recv.at[y], ps_sem.at[d], pr_sem.at[d], py, x)

    for d in range(1, ny):
        p_copy(d).start()
    p_recv[y] = p_send[y]
    for d in range(1, ny):
        p_copy(d).wait()
    summed = p_recv[0].astype(F32)
    for t in range(1, ny):
        summed = summed + p_recv[t].astype(F32)
    h_mid = (hrow_ref[...] + summed).astype(BF16)
    hm_send[...] = h_mid

    def h_copy(d):
        py = (y + d) % ny
        return remote(hm_send, hm_recv.at[y], hs_sem.at[d], hr_sem.at[d], py, x)

    for d in range(1, ny):
        h_copy(d).start()
    hm_recv[y] = h_mid

    hm_cols[0:rows, :] = h_mid.astype(F32)
    hm_cols[rows:, :] = jnp.zeros((hm_cols.shape[0] - rows, width), F32)
    for j in range(width // 128):
        f_cols[128 * j:128 * (j + 1), :] = jnp.transpose(hm_cols[:, 128 * j:128 * (j + 1)])
    lane16 = lane_ids((16, 128))
    for s in range(total):
        corner = jnp.zeros((16, 128), F32)
        for k in range(cols // 16):
            corner = corner + lane_roll(f_cols[cols * s + 16 * k:cols * s + 16 * (k + 1), :], 64 + 16 * k)
        tail[s] = corner

    for d in range(1, ny):
        h_copy(d).wait()
    h64 = jnp.concatenate([hm_recv[t] for t in range(ny)], axis=0).astype(F32)
    inv = lax.rsqrt(jnp.sum(h64 * h64, axis=1, keepdims=True) / width + NORM_EPS)
    u_full[...] = (h64 * inv * gain_ref[...].astype(F32)).astype(BF16)

    def gate_up(c, carry):
        at = pl.multiple_of(c * step, step)
        pltpu.make_async_copy(wgu_hbm.at[:, pl.ds(at, step)], wgu.at[:, pl.ds(at, step)], wgu_sem.at[c]).wait()
        gate = lax.dot_general(wgu[0, pl.ds(at, step), :], u_full[...], NT, preferred_element_type=F32)
        up = lax.dot_general(wgu[1, pl.ds(at, step), :], u_full[...], NT, preferred_element_type=F32)
        gate = gate.astype(BF16).astype(F32)
        up = up.astype(BF16).astype(F32)
        m_cols[pl.ds(at, step), 0:many] = jax.nn.silu(gate) * up
        return carry

    m_cols[:, many:] = jnp.zeros((m_cols.shape[0], 128 - many), F32)
    lax.fori_loop(0, chunk, gate_up, 0)
    for j in range(m_rows.shape[1] // 128):
        m_rows[:, 128 * j:128 * (j + 1)] = jnp.transpose(m_cols[128 * j:128 * (j + 1), :])[0:many].astype(BF16)
    wd_copy.wait()
    wide = 256
    for n in range(width // wide):
        f_part[0:many, wide * n:wide * (n + 1)] = lax.dot_general(
            m_rows[...], wd[:, wide * n:wide * (n + 1)], NN, preferred_element_type=F32)
    for j in range(width // 128):
        f_cols[128 * j:128 * (j + 1), :] = jnp.transpose(f_part[:, 128 * j:128 * (j + 1)])
    for s in range(total):
        a0 = f_cols[cols * s:cols * s + 16, :]
        a1 = f_cols[cols * s + 16:cols * s + 32, :]
        a2 = lane_roll(f_cols[cols * s + 32:cols * s + 48, :], 64)
        f_send[s, 0:16] = jnp.where(lane16 < 64, a0, a2).astype(BF16)
        f_send[s, 16:32] = jnp.where(lane16 < 64, a1, tail[s]).astype(BF16)

    def f_copy(d):
        py, px = peer(y, x, d, ny, nx)
        return remote(f_send.at[px * ny + py], f_recv.at[slot], fs_sem.at[d], fr_sem.at[d], py, px)

    def f_start(d, carry):
        f_copy(d).start()
        return carry

    def f_wait(d, carry):
        f_copy(d).wait()
        return carry

    lax.fori_loop(1, total, f_start, 0)
    f_recv[slot] = f_send[me]
    lax.fori_loop(1, total, f_wait, 0)

    sums = [[jnp.zeros((16, 128), F32) for _ in range(3)] for _ in range(ny)]
    olds = [[jnp.zeros((16, 128), F32) for _ in range(3)] for _ in range(ny)]
    for px in range(nx):
        mine = (lane16 >= rows * px) & (lane16 < rows * (px + 1))
        low = f_recv[px, 0:16].astype(F32)
        for t in range(1, ny):
            low = low + f_recv[t * nx + px, 0:16].astype(F32)
        corner = [f_recv[t * nx + px, 16:32].astype(F32) for t in range(ny)]
        mid = corner[0]
        for t in range(1, ny):
            mid = mid + corner[t]
        high = lane_roll(low, 64)
        for t in range(ny):
            for k, v in enumerate((low, mid, high)):
                sums[t][k] = jnp.where(mine, lane_roll(v, rows * px - rows * t), sums[t][k])
                olds[t][k] = jnp.where(mine, lane_roll(corner[t], rows * px - 64 - 16 * k), olds[t][k])
    for t in range(ny):
        for k in range(3):
            out_ref[16 * k:16 * (k + 1), 128 * t:128 * (t + 1)] = (olds[t][k] + sums[t][k]).astype(BF16)


def solution(mesh):
    group_axes = ('yz', 'x')
    batch_axes = ('replica', 'yz', 'x')
    hidden_spec = P('replica', ('x', 'yz'))
    cache_spec = P(None, batch_axes, None, None)
    ny, nx = mesh.shape['yz'], mesh.shape['x']
    vmem = pl.BlockSpec(memory_space=pltpu.VMEM)
    hbm = pl.BlockSpec(memory_space=pl.ANY)
    dma = pltpu.SemaphoreType.DMA

    def layer(ht, seq_lens, attn_gain, mlp_gain, w_qkv, w_out, w_gate_up, w_down, k_cache, v_cache):
        cols = ht.shape[0]
        rows, slots, head_dim = k_cache.shape
        width = attn_gain.shape[1]
        qcols = w_qkv.shape[0]
        qpad = -(-qcols // 128) * 128
        heads = (qcols * ny) // head_dim - 2
        total = ny * nx
        many = ny * rows
        ffn = w_down.shape[0]
        ffn_pad = -(-ffn // 128) * 128
        z, hrow = pl.pallas_call(
            functools.partial(qkv_kernel, ny, nx, cols, rows, width),
            out_shape=(jax.ShapeDtypeStruct((rows, 16, head_dim), F32), jax.ShapeDtypeStruct((rows, width), F32)),
            in_specs=[vmem, vmem, hbm],
            out_specs=(vmem, vmem),
            scratch_shapes=[
                pltpu.VMEM((nx, 32, 128), BF16), pltpu.VMEM((total, 32, 128), BF16), pltpu.VMEM((qpad, width), BF16),
                pltpu.VMEM((width, 128), F32), pltpu.VMEM((width, 128), F32), pltpu.VMEM((width, 128), BF16),
                pltpu.VMEM((qpad, 128), F32), pltpu.VMEM((ny, rows, qpad), BF16), pltpu.VMEM((ny, rows, qpad), BF16),
                pltpu.VMEM((128, width), F32),
                dma, dma((total,)), dma((total,)), dma((ny,)), dma((ny,))],
            compiler_params=pltpu.CompilerParams(collective_id=0, has_side_effects=True, vmem_limit_bytes=24 << 20),
            name='qkv',
        )(ht, attn_gain, w_qkv)
        o, k_new, v_new = pl.pallas_call(
            functools.partial(attend_kernel, heads, head_dim ** -0.5),
            out_shape=(jax.ShapeDtypeStruct((heads, rows, head_dim), BF16),
                       jax.ShapeDtypeStruct(k_cache.shape, BF16), jax.ShapeDtypeStruct(v_cache.shape, BF16)),
            grid_spec=pltpu.PrefetchScalarGridSpec(
                num_scalar_prefetch=1, grid=(rows,),
                in_specs=[pl.BlockSpec((rows, 16, head_dim), lambda b, _: (0, 0, 0)),
                          pl.BlockSpec((1, slots, head_dim), lambda b, _: (b, 0, 0)),
                          pl.BlockSpec((1, slots, head_dim), lambda b, _: (b, 0, 0))],
                out_specs=(pl.BlockSpec((heads, rows, head_dim), lambda b, _: (0, 0, 0)),
                           pl.BlockSpec((1, slots, head_dim), lambda b, _: (b, 0, 0)),
                           pl.BlockSpec((1, slots, head_dim), lambda b, _: (b, 0, 0))),
                scratch_shapes=[pltpu.VMEM((rows, 16, head_dim), F32)]),
            compiler_params=pltpu.CompilerParams(dimension_semantics=('arbitrary',), vmem_limit_bytes=24 << 20),
            name='attend',
        )(seq_lens, z, k_cache, v_cache)
        chunk = 5
        out = pl.pallas_call(
            functools.partial(mlp_kernel, ny, nx, cols, rows, width, heads),
            out_shape=jax.ShapeDtypeStruct(ht.shape, BF16),
            in_specs=[vmem, vmem, vmem, hbm, hbm, hbm],
            out_specs=vmem,
            scratch_shapes=[
                pltpu.VMEM(w_out.shape, BF16), pltpu.VMEM(w_gate_up.shape, BF16), pltpu.VMEM((ffn_pad, width), BF16),
                pltpu.VMEM((ny, heads // ny, rows, head_dim), BF16), pltpu.VMEM((many, width), F32),
                pltpu.VMEM((ny, rows, width), BF16), pltpu.VMEM((ny, rows, width), BF16),
                pltpu.VMEM((rows, width), BF16), pltpu.VMEM((ny, rows, width), BF16),
                pltpu.VMEM((128, width), F32), pltpu.VMEM((total, 16, 128), F32),
                pltpu.VMEM((many, width), BF16), pltpu.VMEM((ffn_pad, 128), F32), pltpu.VMEM((many, ffn_pad), BF16),
                pltpu.VMEM((128, width), F32), pltpu.VMEM((width, 128), F32),
                pltpu.VMEM((total, 32, 128), BF16), pltpu.VMEM((total, 32, 128), BF16),
                dma, dma((chunk,)), dma, dma((ny,)), dma((ny,)), dma((ny,)), dma((ny,)), dma((ny,)), dma((ny,)),
                dma((total,)), dma((total,))],
            compiler_params=pltpu.CompilerParams(collective_id=1, has_side_effects=True, vmem_limit_bytes=44 << 20),
            name='mlp',
        )(o, hrow, mlp_gain, w_out, w_gate_up, w_down)
        return out, k_new, v_new

    def local_step(hidden, seq_lens, attn_gain, mlp_gain, w_qkv, w_out, w_gate_up, w_down, k_cache, v_cache):
        ht = hidden.T
        k_layers = []
        v_layers = []
        for i in range(w_qkv.shape[0]):
            ht, k_new, v_new = layer(ht, seq_lens, attn_gain[i:i + 1], mlp_gain[i:i + 1], w_qkv[i].T, w_out[i],
                                     jnp.transpose(w_gate_up[i], (1, 2, 0)), w_down[i], k_cache[i], v_cache[i])
            k_layers.append(k_new)
            v_layers.append(v_new)
        return ht.T, jnp.stack(k_layers), jnp.stack(v_layers)

    return jax.shard_map(
        local_step,
        mesh=mesh,
        in_specs=(hidden_spec, P(batch_axes), P(None, None), P(None, None), P(None, None, 'yz'), P(None, 'yz', None),
                  P(None, None, None, 'yz'), P(None, 'yz', None), cache_spec, cache_spec),
        out_specs=(hidden_spec, cache_spec, cache_spec),
        check_vma=False)
```

```python
import functools

import jax
import jax.numpy as jnp
from jax import lax
from jax.experimental import pallas as pl
from jax.experimental.pallas import tpu as pltpu
from jax.sharding import PartitionSpec as P

NORM_EPS = 1e-5
MESH = pl.DeviceIdType.MESH
F32 = jnp.float32
BF16 = jnp.bfloat16
NT = (((1,), (1,)), ((), ()))
NN = (((1,), (0,)), ((), ()))


def lane_ids(shape):
    return lax.broadcasted_iota(jnp.int32, shape, len(shape) - 1)


def lane_roll(v, shift):
    shift = shift % v.shape[-1]
    return v if shift == 0 else pltpu.roll(v, shift, v.ndim - 1)


def position(ny, nx):
    return lax.axis_index('yz'), lax.axis_index('x')


def peer(y, x, d, ny, nx):
    dy, dx = d // nx, d % nx
    ahead = ((y + dy) % ny, (x + dx) % nx)
    return ahead


def greet_all(y, x, ny, nx):
    barrier = pltpu.get_barrier_semaphore()
    total = ny * nx

    def hello(d, carry):
        py, px = peer(y, x, d, ny, nx)
        pl.semaphore_signal(barrier, inc=1, device_id={'yz': py, 'x': px}, device_id_type=MESH)
        return carry

    lax.fori_loop(1, total, hello, 0)
    return barrier


def remote(src, dst, send_sem, recv_sem, py, px):
    return pltpu.make_async_remote_copy(src_ref=src, dst_ref=dst, send_sem=send_sem, recv_sem=recv_sem,
                                        device_id={'yz': py, 'x': px}, device_id_type=MESH)


def qkv_kernel(ny, nx, cols, rows, width, ht_hbm, gain_hbm, w_hbm, k_hbm, v_hbm, z_ref, hrow_ref, k_ref, v_ref,
               ht_ref, gain_ref, send_buf, recv_buf, w_vmem, gain_col, h_full, u_full, zt_buf, z_send, z_recv, h_rows,
               h_sem, g_sem, w_sem, kv_sem, send_sem, recv_sem, zsend_sem, zrecv_sem):
    y, x = position(ny, nx)
    total = ny * nx
    me = x * ny + y
    qcols = w_hbm.shape[0]
    h_copy = pltpu.make_async_copy(ht_hbm, ht_ref, h_sem)
    h_copy.start()
    barrier = greet_all(y, x, ny, nx)
    g_copy = pltpu.make_async_copy(gain_hbm, gain_ref, g_sem)
    g_copy.start()
    w_copy = pltpu.make_async_copy(w_hbm, w_vmem.at[pl.ds(0, qcols)], w_sem)
    w_copy.start()
    parts = kv_sem.shape[1]
    share = k_hbm.shape[0] // parts
    kv_copies = [pltpu.make_async_copy(src.at[pl.ds(i * share, share)], dst.at[pl.ds(i * share, share)], kv_sem.at[c, i])
                 for i in range(parts) for c, (src, dst) in enumerate(((k_hbm, k_ref), (v_hbm, v_ref)))]
    for copy in kv_copies:
        copy.start()
    h_copy.wait()

    lane = lane_ids((cols, 128))
    lane16 = lane_ids((16, 128))
    tiles = [ht_ref[:, 128 * t:128 * (t + 1)].astype(F32) for t in range(ny)]
    for px in range(nx):
        block = jnp.zeros((cols, 128), F32)
        for t in range(ny):
            piece = lane_roll(tiles[t], rows * t - rows * px)
            block = jnp.where((lane >= rows * t) & (lane < rows * (t + 1)), piece, block)
        high = lane_roll(block[32:48], 64)
        send_buf[px, 0:16] = jnp.where(lane16 < 64, block[0:16], high).astype(BF16)
        send_buf[px, 16:32] = block[16:32].astype(BF16)

    pl.semaphore_wait(barrier, total - 1)

    def send(d, carry):
        py, px = peer(y, x, d, ny, nx)
        remote(send_buf.at[px], recv_buf.at[me], send_sem.at[d], recv_sem.at[d], py, px).start()
        return carry

    lax.fori_loop(1, total, send, 0)
    recv_buf[me] = send_buf[x]

    g_copy.wait()
    for j in range(width // 128):
        row = gain_ref[0:1, 128 * j:128 * (j + 1)].astype(F32)
        gain_col[128 * j:128 * (j + 1), :] = jnp.transpose(jnp.broadcast_to(row, (128, 128)))
    w_vmem[qcols:, :] = jnp.zeros((w_vmem.shape[0] - qcols, width), BF16)

    def land(d, carry):
        py, px = peer(y, x, d, ny, nx)
        remote(send_buf.at[px], recv_buf.at[me], send_sem.at[d], recv_sem.at[d], py, px).wait()
        return carry

    lax.fori_loop(1, total, land, 0)

    square = jnp.zeros((16, 128), F32)
    for s in range(total):
        low = recv_buf[s, 0:16].astype(F32)
        mid = recv_buf[s, 16:32].astype(F32)
        high = lane_roll(low, 64)
        h_full[cols * s:cols * s + 16, :] = low
        h_full[cols * s + 16:cols * s + 32, :] = mid
        h_full[cols * s + 32:cols * s + 48, :] = high
        square = square + low * low + mid * mid + high * high
    power = jnp.sum(square, axis=0, keepdims=True)
    inv = lax.rsqrt(power / width + NORM_EPS)
    u_full[...] = (h_full[...] * inv * gain_col[...]).astype(BF16)
    w_copy.wait()
    zt_buf[...] = lax.dot_general(w_vmem[...], u_full[...], NN, preferred_element_type=F32)
    for j in range(zt_buf.shape[0] // 128):
        zj = jnp.transpose(zt_buf[128 * j:128 * (j + 1), :])
        for t in range(ny):
            z_send[t, :, 128 * j:128 * (j + 1)] = zj[rows * t:rows * (t + 1)].astype(BF16)
    for d in range(1, ny):
        py = (y + d) % ny
        remote(z_send.at[py], z_recv.at[y], zsend_sem.at[d], zrecv_sem.at[d], py, x).start()
    z_recv[y] = z_send[y]

    for j in range(width // 128):
        h_rows[:, 128 * j:128 * (j + 1)] = jnp.transpose(h_full[128 * j:128 * (j + 1), :])
    hrow_ref[...] = h_rows[pl.ds(pl.multiple_of(y * rows, rows), rows), :]

    for d in range(1, ny):
        py = (y + d) % ny
        remote(z_send.at[py], z_recv.at[y], zsend_sem.at[d], zrecv_sem.at[d], py, x).wait()

    zs = [[z_recv[t, :, 128 * j:128 * (j + 1)].astype(F32) for j in range(w_vmem.shape[0] // 128)] for t in range(ny)]
    for g in range(ny * qcols // 128):
        start = 128 * g
        t = start // qcols
        off = start - t * qcols
        j, sh = off // 128, off % 128
        take = min(128, qcols - off)
        out = lane_roll(zs[t][j], -sh)
        if sh and take > 128 - sh:
            out = jnp.where(lane16 < 128 - sh, out, lane_roll(zs[t][j + 1], -sh))
        if take < 128:
            out = jnp.where(lane16 < take, out, lane_roll(zs[t + 1][0], take))
        z_ref[:, g, :] = out
    for g in range(ny * qcols // 128, z_ref.shape[1]):
        z_ref[:, g, :] = jnp.zeros((rows, 128), F32)
    for copy in kv_copies:
        copy.wait()


def attend_kernel(heads, scale, len_ref, z_ref, k_in, v_in, k_hbm, v_hbm, o_ref, k_ref, v_ref, s_buf, o_acc, k_sem, v_sem):
    rows, slots = k_ref.shape[:2]

    def place(b, carry):
        length = len_ref[b]
        base = pl.multiple_of((length // 16) * 16, 16)
        here = lax.broadcasted_iota(jnp.int32, (16, 128), 0) == length - base
        k_new = jnp.broadcast_to(z_ref[b, heads:heads + 1, :], (16, 128)).astype(BF16)
        v_new = jnp.broadcast_to(z_ref[b, heads + 1:heads + 2, :], (16, 128)).astype(BF16)
        k_ref[b, pl.ds(base, 16), :] = jnp.where(here, k_new, k_ref[b, pl.ds(base, 16), :])
        v_ref[b, pl.ds(base, 16), :] = jnp.where(here, v_new, v_ref[b, pl.ds(base, 16), :])
        return carry

    def k_copy(b):
        return pltpu.make_async_copy(k_ref.at[b], k_hbm.at[b], k_sem.at[b])

    def v_copy(b):
        return pltpu.make_async_copy(v_ref.at[b], v_hbm.at[b], v_sem.at[b])

    def leave(b, carry):
        k_copy(b).start()
        v_copy(b).start()
        return carry

    def score(b):
        s = lax.dot_general(z_ref[b].astype(BF16), k_ref[b], NT, preferred_element_type=F32) * scale
        s_buf[b % 2] = s

    def finish(b):
        s = s_buf[b % 2]
        s = jnp.where(lane_ids(s.shape) <= len_ref[b], s, -1e30)
        e = jnp.exp(s - jnp.max(s, axis=1, keepdims=True))
        p = (e * (1.0 / jnp.sum(e, axis=1, keepdims=True))).astype(BF16)
        o_acc[b] = lax.dot_general(p, v_ref[b], NN, preferred_element_type=F32)

    lax.fori_loop(0, rows, place, 0)
    lax.fori_loop(0, rows, leave, 0)
    score(0)

    def step(b, carry):
        score(b + 1)
        finish(b)
        return carry

    lax.fori_loop(0, rows - 1, step, 0)
    finish(rows - 1)
    for h in range(heads):
        o_ref[h] = o_acc[:, h, :].astype(BF16)

    def drain(b, carry):
        k_copy(b).wait()
        v_copy(b).wait()
        return carry

    lax.fori_loop(0, rows, drain, 0)


def mlp_kernel(ny, nx, cols, rows, width, heads, o_ref, hrow_ref, gain_hbm, wo_hbm, wgu_hbm, wd_hbm, out_ref,
               gain_ref, wo, wgu, wd, o_recv, part, p_send, p_recv, hm_send, hm_recv, hm_cols, tail, u_full, m_cols, m_rows,
               f_part, f_cols, f_send, f_recv,
               gain_sem, wo_sem, wgu_sem, wd_sem, os_sem, or_sem, ps_sem, pr_sem, hs_sem, hr_sem, fs_sem, fr_sem):
    y, x = position(ny, nx)
    total = ny * nx
    me = x * ny + y
    slot = y * nx + x
    heads_y = heads // ny
    many = ny * rows
    ffn = wgu_hbm.shape[1]
    chunk = wgu_sem.shape[0]
    step = ffn // chunk
    gain_copy = pltpu.make_async_copy(gain_hbm, gain_ref, gain_sem)
    gain_copy.start()
    wo_copy = pltpu.make_async_copy(wo_hbm, wo, wo_sem)
    wo_copy.start()
    wgu_copies = []
    for c in range(chunk):
        wgu_copies.append(pltpu.make_async_copy(wgu_hbm.at[:, pl.ds(c * step, step)], wgu.at[:, pl.ds(c * step, step)], wgu_sem.at[c]))
        wgu_copies[-1].start()
    wd_copy = pltpu.make_async_copy(wd_hbm, wd.at[pl.ds(0, ffn)], wd_sem)
    wd_copy.start()
    barrier = greet_all(y, x, ny, nx)
    wd[ffn:, :] = jnp.zeros((wd.shape[0] - ffn, width), BF16)
    m_cols[ffn:, :] = jnp.zeros((m_cols.shape[0] - ffn, 128), F32)
    f_part[many:, :] = jnp.zeros((f_part.shape[0] - many, width), F32)
    pl.semaphore_wait(barrier, total - 1)

    def o_copy(d):
        py = (y + d) % ny
        return remote(o_ref.at[pl.ds(py * heads_y, heads_y)], o_recv.at[y], os_sem.at[d], or_sem.at[d], py, x)

    for d in range(1, ny):
        o_copy(d).start()
    o_recv[y] = o_ref[pl.ds(y * heads_y, heads_y)]
    for d in range(1, ny):
        o_copy(d).wait()
    wo_copy.wait()
    o_rows = [jnp.concatenate([o_recv[t, h] for t in range(ny)], axis=0) for h in range(heads_y)]
    o_full = jnp.concatenate(o_rows, axis=1)
    part[...] = lax.dot_general(o_full, wo[...], NN, preferred_element_type=F32)
    for t in range(ny):
        p_send[t] = part[rows * t:rows * (t + 1), :].astype(BF16)

    def p_copy(d):
        py = (y + d) % ny
        return remote(p_send.at[py], p_recv.at[y], ps_sem.at[d], pr_sem.at[d], py, x)

    for d in range(1, ny):
        p_copy(d).start()
    p_recv[y] = p_send[y]
    for d in range(1, ny):
        p_copy(d).wait()
    summed = p_recv[0].astype(F32)
    for t in range(1, ny):
        summed = summed + p_recv[t].astype(F32)
    h_mid = (hrow_ref[...] + summed).astype(BF16)
    hm_send[...] = h_mid

    def h_copy(d):
        py = (y + d) % ny
        return remote(hm_send, hm_recv.at[y], hs_sem.at[d], hr_sem.at[d], py, x)

    for d in range(1, ny):
        h_copy(d).start()
    hm_recv[y] = h_mid

    hm_cols[0:rows, :] = h_mid.astype(F32)
    hm_cols[rows:, :] = jnp.zeros((hm_cols.shape[0] - rows, width), F32)
    for j in range(width // 128):
        f_cols[128 * j:128 * (j + 1), :] = jnp.transpose(hm_cols[:, 128 * j:128 * (j + 1)])
    lane16 = lane_ids((16, 128))
    for s in range(total):
        corner = jnp.zeros((16, 128), F32)
        for k in range(cols // 16):
            corner = corner + lane_roll(f_cols[cols * s + 16 * k:cols * s + 16 * (k + 1), :], 64 + 16 * k)
        tail[s] = corner

    for d in range(1, ny):
        h_copy(d).wait()
    gain_copy.wait()
    h64 = jnp.concatenate([hm_recv[t] for t in range(ny)], axis=0).astype(F32)
    inv = lax.rsqrt(jnp.sum(h64 * h64, axis=1, keepdims=True) / width + NORM_EPS)
    u_full[...] = (h64 * inv * gain_ref[...].astype(F32)).astype(BF16)

    def gate_up(c, carry):
        at = pl.multiple_of(c * step, step)
        pltpu.make_async_copy(wgu_hbm.at[:, pl.ds(at, step)], wgu.at[:, pl.ds(at, step)], wgu_sem.at[c]).wait()
        gate = lax.dot_general(wgu[0, pl.ds(at, step), :], u_full[...], NT, preferred_element_type=F32)
        up = lax.dot_general(wgu[1, pl.ds(at, step), :], u_full[...], NT, preferred_element_type=F32)
        gate = gate.astype(BF16).astype(F32)
        up = up.astype(BF16).astype(F32)
        m_cols[pl.ds(at, step), 0:many] = jax.nn.silu(gate) * up
        return carry

    m_cols[:, many:] = jnp.zeros((m_cols.shape[0], 128 - many), F32)
    lax.fori_loop(0, chunk, gate_up, 0)
    for j in range(m_rows.shape[1] // 128):
        m_rows[:, 128 * j:128 * (j + 1)] = jnp.transpose(m_cols[128 * j:128 * (j + 1), :])[0:many].astype(BF16)
    wd_copy.wait()
    wide = 256
    for n in range(width // wide):
        f_part[0:many, wide * n:wide * (n + 1)] = lax.dot_general(
            m_rows[...], wd[:, wide * n:wide * (n + 1)], NN, preferred_element_type=F32)
    for j in range(width // 128):
        f_cols[128 * j:128 * (j + 1), :] = jnp.transpose(f_part[:, 128 * j:128 * (j + 1)])
    for s in range(total):
        a0 = f_cols[cols * s:cols * s + 16, :]
        a1 = f_cols[cols * s + 16:cols * s + 32, :]
        a2 = lane_roll(f_cols[cols * s + 32:cols * s + 48, :], 64)
        f_send[s, 0:16] = jnp.where(lane16 < 64, a0, a2).astype(BF16)
        f_send[s, 16:32] = jnp.where(lane16 < 64, a1, tail[s]).astype(BF16)

    def f_copy(d):
        py, px = peer(y, x, d, ny, nx)
        return remote(f_send.at[px * ny + py], f_recv.at[slot], fs_sem.at[d], fr_sem.at[d], py, px)

    def f_start(d, carry):
        f_copy(d).start()
        return carry

    def f_wait(d, carry):
        f_copy(d).wait()
        return carry

    lax.fori_loop(1, total, f_start, 0)
    f_recv[slot] = f_send[me]
    lax.fori_loop(1, total, f_wait, 0)

    sums = [[jnp.zeros((16, 128), F32) for _ in range(3)] for _ in range(ny)]
    olds = [[jnp.zeros((16, 128), F32) for _ in range(3)] for _ in range(ny)]
    for px in range(nx):
        mine = (lane16 >= rows * px) & (lane16 < rows * (px + 1))
        low = f_recv[px, 0:16].astype(F32)
        for t in range(1, ny):
            low = low + f_recv[t * nx + px, 0:16].astype(F32)
        corner = [f_recv[t * nx + px, 16:32].astype(F32) for t in range(ny)]
        mid = corner[0]
        for t in range(1, ny):
            mid = mid + corner[t]
        high = lane_roll(low, 64)
        for t in range(ny):
            for k, v in enumerate((low, mid, high)):
                sums[t][k] = jnp.where(mine, lane_roll(v, rows * px - rows * t), sums[t][k])
                olds[t][k] = jnp.where(mine, lane_roll(corner[t], rows * px - 64 - 16 * k), olds[t][k])
    for t in range(ny):
        for k in range(3):
            out_ref[16 * k:16 * (k + 1), 128 * t:128 * (t + 1)] = (olds[t][k] + sums[t][k]).astype(BF16)


def solution(mesh):
    group_axes = ('yz', 'x')
    batch_axes = ('replica', 'yz', 'x')
    hidden_spec = P('replica', ('x', 'yz'))
    cache_spec = P(None, batch_axes, None, None)
    ny, nx = mesh.shape['yz'], mesh.shape['x']
    vmem = pl.BlockSpec(memory_space=pltpu.VMEM)
    hbm = pl.BlockSpec(memory_space=pl.ANY)
    dma = pltpu.SemaphoreType.DMA

    def layer(ht, seq_lens, attn_gain, mlp_gain, w_qkv, w_out, w_gate_up, w_down, k_cache, v_cache):
        cols = ht.shape[0]
        rows, slots, head_dim = k_cache.shape
        width = attn_gain.shape[1]
        qcols = w_qkv.shape[0]
        qpad = -(-qcols // 128) * 128
        heads = (qcols * ny) // head_dim - 2
        total = ny * nx
        many = ny * rows
        ffn = w_down.shape[0]
        ffn_pad = -(-ffn // 128) * 128
        in_hbm = functools.partial(pltpu.with_memory_space_constraint, memory_space=pltpu.HBM)
        parts = 4
        z, hrow, k_vmem, v_vmem = pl.pallas_call(
            functools.partial(qkv_kernel, ny, nx, cols, rows, width),
            out_shape=(jax.ShapeDtypeStruct((rows, 16, head_dim), F32), jax.ShapeDtypeStruct((rows, width), F32),
                       pltpu.VMEM(k_cache.shape, BF16), pltpu.VMEM(v_cache.shape, BF16)),
            in_specs=[hbm] * 5,
            out_specs=(vmem,) * 4,
            scratch_shapes=[
                pltpu.VMEM(ht.shape, BF16), pltpu.VMEM(attn_gain.shape, BF16),
                pltpu.VMEM((nx, 32, 128), BF16), pltpu.VMEM((total, 32, 128), BF16), pltpu.VMEM((qpad, width), BF16),
                pltpu.VMEM((width, 128), F32), pltpu.VMEM((width, 128), F32), pltpu.VMEM((width, 128), BF16),
                pltpu.VMEM((qpad, 128), F32), pltpu.VMEM((ny, rows, qpad), BF16), pltpu.VMEM((ny, rows, qpad), BF16),
                pltpu.VMEM((128, width), F32),
                dma, dma, dma, dma((2, parts)), dma((total,)), dma((total,)), dma((ny,)), dma((ny,))],
            compiler_params=pltpu.CompilerParams(collective_id=0, has_side_effects=True, vmem_limit_bytes=12 << 20),
            cost_estimate=pl.CostEstimate(flops=8_000_000_000, bytes_accessed=20_000_000, transcendentals=0),
            name='qkv',
        )(in_hbm(ht), in_hbm(attn_gain), in_hbm(w_qkv), in_hbm(k_cache), in_hbm(v_cache))
        k_new, v_new, o, _, _ = pl.pallas_call(
            functools.partial(attend_kernel, heads, head_dim ** -0.5),
            out_shape=(pltpu.HBM(k_cache.shape, BF16), pltpu.HBM(v_cache.shape, BF16),
                       jax.ShapeDtypeStruct((heads, rows, head_dim), BF16),
                       pltpu.VMEM(k_cache.shape, BF16), pltpu.VMEM(v_cache.shape, BF16)),
            in_specs=[pl.BlockSpec(memory_space=pltpu.SMEM), vmem, vmem, vmem],
            out_specs=(hbm, hbm, vmem, vmem, vmem),
            input_output_aliases={2: 3, 3: 4},
            scratch_shapes=[pltpu.VMEM((2, 16, slots), F32), pltpu.VMEM((rows, 16, head_dim), F32), dma((rows,)), dma((rows,))],
            compiler_params=pltpu.CompilerParams(vmem_limit_bytes=8 << 20),
            cost_estimate=pl.CostEstimate(flops=8_000_000_000, bytes_accessed=20_000_000, transcendentals=0),
            name='attend',
        )(seq_lens, z, k_vmem, v_vmem)
        chunk = 5
        out = pl.pallas_call(
            functools.partial(mlp_kernel, ny, nx, cols, rows, width, heads),
            out_shape=jax.ShapeDtypeStruct(ht.shape, BF16),
            in_specs=[vmem, vmem, hbm, hbm, hbm, hbm],
            out_specs=vmem,
            scratch_shapes=[
                pltpu.VMEM(mlp_gain.shape, BF16),
                pltpu.VMEM(w_out.shape, BF16), pltpu.VMEM(w_gate_up.shape, BF16), pltpu.VMEM((ffn_pad, width), BF16),
                pltpu.VMEM((ny, heads // ny, rows, head_dim), BF16), pltpu.VMEM((many, width), F32),
                pltpu.VMEM((ny, rows, width), BF16), pltpu.VMEM((ny, rows, width), BF16),
                pltpu.VMEM((rows, width), BF16), pltpu.VMEM((ny, rows, width), BF16),
                pltpu.VMEM((128, width), F32), pltpu.VMEM((total, 16, 128), F32),
                pltpu.VMEM((many, width), BF16), pltpu.VMEM((ffn_pad, 128), F32), pltpu.VMEM((many, ffn_pad), BF16),
                pltpu.VMEM((128, width), F32), pltpu.VMEM((width, 128), F32),
                pltpu.VMEM((total, 32, 128), BF16), pltpu.VMEM((total, 32, 128), BF16),
                dma, dma, dma((chunk,)), dma, dma((ny,)), dma((ny,)), dma((ny,)), dma((ny,)), dma((ny,)), dma((ny,)),
                dma((total,)), dma((total,))],
            compiler_params=pltpu.CompilerParams(collective_id=1, has_side_effects=True, vmem_limit_bytes=44 << 20),
            name='mlp',
        )(o, hrow, in_hbm(mlp_gain), in_hbm(w_out), in_hbm(w_gate_up), in_hbm(w_down))
        return out, k_new, v_new

    def local_step(hidden, seq_lens, attn_gain, mlp_gain, w_qkv, w_out, w_gate_up, w_down, k_cache, v_cache):
        ht = hidden.T
        k_layers = []
        v_layers = []
        for i in range(w_qkv.shape[0]):
            ht, k_new, v_new = layer(ht, seq_lens, attn_gain[i:i + 1], mlp_gain[i:i + 1], w_qkv[i].T, w_out[i],
                                     jnp.transpose(w_gate_up[i], (1, 2, 0)), w_down[i], k_cache[i], v_cache[i])
            k_layers.append(k_new)
            v_layers.append(v_new)
        return ht.T, jnp.stack(k_layers), jnp.stack(v_layers)

    return jax.shard_map(
        local_step,
        mesh=mesh,
        in_specs=(hidden_spec, P(batch_axes), P(None, None), P(None, None), P(None, None, 'yz'), P(None, 'yz', None),
                  P(None, None, None, 'yz'), P(None, 'yz', None), cache_spec, cache_spec),
        out_specs=(hidden_spec, cache_spec, cache_spec),
        check_vma=False)
```

```python
import functools

import jax
import jax.numpy as jnp
from jax import lax
from jax.experimental import pallas as pl
from jax.experimental.pallas import tpu as pltpu
from jax.sharding import PartitionSpec as P

NORM_EPS = 1e-5
MESH = pl.DeviceIdType.MESH
F32 = jnp.float32
BF16 = jnp.bfloat16
NT = (((1,), (1,)), ((), ()))
NN = (((1,), (0,)), ((), ()))


def lane_ids(shape):
    return lax.broadcasted_iota(jnp.int32, shape, len(shape) - 1)


def lane_roll(v, shift):
    shift = shift % v.shape[-1]
    return v if shift == 0 else pltpu.roll(v, shift, v.ndim - 1)


def position(ny, nx):
    return lax.axis_index('yz'), lax.axis_index('x')


def peers(y, x, ny, nx):
    ys = [(y + d) % ny for d in range(ny)]
    xs = [(x + d) % nx for d in range(nx)]
    far_y = sorted(range(ny), key=lambda d: -min(d, ny - d))
    far_x = sorted(range(nx), key=lambda d: -min(d, nx - d))
    return [(dy * nx + dx, ys[dy], xs[dx]) for dx in far_x for dy in far_y if dy or dx]


def greet_all(others):
    barrier = pltpu.get_barrier_semaphore()
    for _, py, px in others:
        pl.semaphore_signal(barrier, inc=1, device_id={'yz': py, 'x': px}, device_id_type=MESH)
    return barrier


def remote(src, dst, send_sem, recv_sem, py, px):
    return pltpu.make_async_remote_copy(src_ref=src, dst_ref=dst, send_sem=send_sem, recv_sem=recv_sem,
                                        device_id={'yz': py, 'x': px}, device_id_type=MESH)


def qkv_kernel(ny, nx, cols, rows, width, ht_hbm, gain_hbm, w_hbm, k_hbm, v_hbm, z_ref, hrow_ref, k_ref, v_ref,
               ht_ref, gain_ref, send_buf, recv_buf, w_vmem, gain_col, h_full, u_full, zt_buf, z_send, z_recv, h_rows,
               h_sem, g_sem, w_sem, kv_sem, send_sem, recv_sem, zsend_sem, zrecv_sem):
    y, x = position(ny, nx)
    total = ny * nx
    me = x * ny + y
    qcols = w_hbm.shape[0]
    h_copy = pltpu.make_async_copy(ht_hbm, ht_ref, h_sem)
    h_copy.start()
    others = peers(y, x, ny, nx)
    barrier = greet_all(others)
    g_copy = pltpu.make_async_copy(gain_hbm, gain_ref, g_sem)
    g_copy.start()
    w_copy = pltpu.make_async_copy(w_hbm, w_vmem.at[pl.ds(0, qcols)], w_sem)
    w_copy.start()
    parts = kv_sem.shape[1]
    share = k_hbm.shape[0] // parts
    kv_copies = [pltpu.make_async_copy(src.at[pl.ds(i * share, share)], dst.at[pl.ds(i * share, share)], kv_sem.at[c, i])
                 for i in range(parts) for c, (src, dst) in enumerate(((k_hbm, k_ref), (v_hbm, v_ref)))]
    for copy in kv_copies:
        copy.start()
    h_copy.wait()

    lane = lane_ids((cols, 128))
    lane16 = lane_ids((16, 128))
    tiles = [ht_ref[:, 128 * t:128 * (t + 1)].astype(F32) for t in range(ny)]
    for px in range(nx):
        block = jnp.zeros((cols, 128), F32)
        for t in range(ny):
            piece = lane_roll(tiles[t], rows * t - rows * px)
            block = jnp.where((lane >= rows * t) & (lane < rows * (t + 1)), piece, block)
        high = lane_roll(block[32:48], 64)
        send_buf[px, 0:16] = jnp.where(lane16 < 64, block[0:16], high).astype(BF16)
        send_buf[px, 16:32] = block[16:32].astype(BF16)

    pl.semaphore_wait(barrier, total - 1)

    h_sends = [remote(send_buf.at[px], recv_buf.at[me], send_sem.at[d], recv_sem.at[d], py, px) for d, py, px in others]
    for copy in h_sends:
        copy.start()
    recv_buf[me] = send_buf[x]

    g_copy.wait()
    for j in range(width // 128):
        row = gain_ref[0:1, 128 * j:128 * (j + 1)].astype(F32)
        gain_col[128 * j:128 * (j + 1), :] = jnp.transpose(jnp.broadcast_to(row, (128, 128)))
    w_vmem[qcols:, :] = jnp.zeros((w_vmem.shape[0] - qcols, width), BF16)

    for copy in h_sends:
        copy.wait()

    square = jnp.zeros((16, 128), F32)
    for s in range(total):
        low = recv_buf[s, 0:16].astype(F32)
        mid = recv_buf[s, 16:32].astype(F32)
        high = lane_roll(low, 64)
        h_full[cols * s:cols * s + 16, :] = low
        h_full[cols * s + 16:cols * s + 32, :] = mid
        h_full[cols * s + 32:cols * s + 48, :] = high
        square = square + low * low + mid * mid + high * high
    power = jnp.sum(square, axis=0, keepdims=True)
    inv = lax.rsqrt(power / width + NORM_EPS)
    u_full[...] = (h_full[...] * inv * gain_col[...]).astype(BF16)
    w_copy.wait()
    zt_buf[...] = lax.dot_general(w_vmem[...], u_full[...], NN, preferred_element_type=F32)
    for j in range(zt_buf.shape[0] // 128):
        zj = jnp.transpose(zt_buf[128 * j:128 * (j + 1), :])
        for t in range(ny):
            z_send[t, :, 128 * j:128 * (j + 1)] = zj[rows * t:rows * (t + 1)].astype(BF16)
    for d in range(1, ny):
        py = (y + d) % ny
        remote(z_send.at[py], z_recv.at[y], zsend_sem.at[d], zrecv_sem.at[d], py, x).start()
    z_recv[y] = z_send[y]

    for j in range(width // 128):
        h_rows[:, 128 * j:128 * (j + 1)] = jnp.transpose(h_full[128 * j:128 * (j + 1), :])
    hrow_ref[...] = h_rows[pl.ds(pl.multiple_of(y * rows, rows), rows), :]

    for d in range(1, ny):
        py = (y + d) % ny
        remote(z_send.at[py], z_recv.at[y], zsend_sem.at[d], zrecv_sem.at[d], py, x).wait()

    zs = [[z_recv[t, :, 128 * j:128 * (j + 1)].astype(F32) for j in range(w_vmem.shape[0] // 128)] for t in range(ny)]
    for g in range(ny * qcols // 128):
        start = 128 * g
        t = start // qcols
        off = start - t * qcols
        j, sh = off // 128, off % 128
        take = min(128, qcols - off)
        out = lane_roll(zs[t][j], -sh)
        if sh and take > 128 - sh:
            out = jnp.where(lane16 < 128 - sh, out, lane_roll(zs[t][j + 1], -sh))
        if take < 128:
            out = jnp.where(lane16 < take, out, lane_roll(zs[t + 1][0], take))
        z_ref[:, g, :] = out
    for g in range(ny * qcols // 128, z_ref.shape[1]):
        z_ref[:, g, :] = jnp.zeros((rows, 128), F32)
    for copy in kv_copies:
        copy.wait()


def attend_kernel(heads, scale, len_ref, z_ref, k_in, v_in, k_hbm, v_hbm, o_ref, k_ref, v_ref, s_buf, o_acc, k_sem, v_sem):
    rows, slots = k_ref.shape[:2]

    def place(b, carry):
        length = len_ref[b]
        base = pl.multiple_of((length // 16) * 16, 16)
        here = lax.broadcasted_iota(jnp.int32, (16, 128), 0) == length - base
        k_new = jnp.broadcast_to(z_ref[b, heads:heads + 1, :], (16, 128)).astype(BF16)
        v_new = jnp.broadcast_to(z_ref[b, heads + 1:heads + 2, :], (16, 128)).astype(BF16)
        k_ref[b, pl.ds(base, 16), :] = jnp.where(here, k_new, k_ref[b, pl.ds(base, 16), :])
        v_ref[b, pl.ds(base, 16), :] = jnp.where(here, v_new, v_ref[b, pl.ds(base, 16), :])
        return carry

    def k_copy(b):
        return pltpu.make_async_copy(k_ref.at[b], k_hbm.at[b], k_sem.at[b])

    def v_copy(b):
        return pltpu.make_async_copy(v_ref.at[b], v_hbm.at[b], v_sem.at[b])

    def leave(b, carry):
        k_copy(b).start()
        v_copy(b).start()
        return carry

    def score(i):
        blank = jnp.zeros((16, 128), BF16)
        q0, q1 = z_ref[2 * i].astype(BF16), z_ref[2 * i + 1].astype(BF16)
        q = jnp.concatenate([jnp.concatenate([q0, blank], axis=1), jnp.concatenate([blank, q1], axis=1)], axis=0)
        keys = jnp.concatenate([k_ref[2 * i], k_ref[2 * i + 1]], axis=1)
        s_buf[i % 2] = lax.dot_general(q, keys, NT, preferred_element_type=F32) * scale

    def finish(i):
        s = s_buf[i % 2]
        first = lax.broadcasted_iota(jnp.int32, (32, 1), 0) < 16
        length = jnp.where(first, len_ref[2 * i], len_ref[2 * i + 1])
        s = jnp.where(lane_ids(s.shape) <= length, s, -1e30)
        e = jnp.exp(s - jnp.max(s, axis=1, keepdims=True))
        p = (e * (1.0 / jnp.sum(e, axis=1, keepdims=True))).astype(BF16)
        values = jnp.concatenate([v_ref[2 * i], v_ref[2 * i + 1]], axis=1)
        o = lax.dot_general(p, values, NN, preferred_element_type=F32)
        o_acc[2 * i] = o[0:16, 0:128]
        o_acc[2 * i + 1] = o[16:32, 128:256]

    lax.fori_loop(0, rows, place, 0)
    lax.fori_loop(0, rows, leave, 0)
    score(0)

    def step(i, carry):
        score(i + 1)
        finish(i)
        return carry

    lax.fori_loop(0, rows // 2 - 1, step, 0)
    finish(rows // 2 - 1)
    for h in range(heads):
        o_ref[h] = o_acc[:, h, :].astype(BF16)

    def drain(b, carry):
        k_copy(b).wait()
        v_copy(b).wait()
        return carry

    lax.fori_loop(0, rows, drain, 0)


def mlp_kernel(ny, nx, cols, rows, width, heads, o_ref, hrow_ref, gain_hbm, wo_hbm, wgu_hbm, wd_hbm, out_ref,
               gain_ref, wo, wgu, wd, o_recv, p_send, p_recv, hm_send, hm_recv, hm_cols, tail, u_full, m_cols, m_rows,
               f_part, f_cols, f_send, f_recv,
               gain_sem, wo_sem, wgu_sem, wd_sem, os_sem, or_sem, ps_sem, pr_sem, hs_sem, hr_sem, fs_sem, fr_sem):
    y, x = position(ny, nx)
    total = ny * nx
    me = x * ny + y
    slot = y * nx + x
    heads_y = heads // ny
    many = ny * rows
    ffn = wgu_hbm.shape[1]
    chunk = wgu_sem.shape[0]
    step = ffn // chunk
    gain_copy = pltpu.make_async_copy(gain_hbm, gain_ref, gain_sem)
    gain_copy.start()
    wo_copy = pltpu.make_async_copy(wo_hbm, wo, wo_sem)
    wo_copy.start()
    wgu_copies = []
    for c in range(chunk):
        wgu_copies.append(pltpu.make_async_copy(wgu_hbm.at[:, pl.ds(c * step, step)], wgu.at[:, pl.ds(c * step, step)], wgu_sem.at[c]))
        wgu_copies[-1].start()
    wd_copy = pltpu.make_async_copy(wd_hbm, wd.at[pl.ds(0, ffn)], wd_sem)
    wd_copy.start()
    others = peers(y, x, ny, nx)
    barrier = greet_all(others)
    wd[ffn:, :] = jnp.zeros((wd.shape[0] - ffn, width), BF16)
    m_cols[ffn:, :] = jnp.zeros((m_cols.shape[0] - ffn, 128), F32)
    f_part[many:, :] = jnp.zeros((f_part.shape[0] - many, f_part.shape[1]), F32)
    pl.semaphore_wait(barrier, total - 1)

    def o_copy(d):
        py = (y + d) % ny
        return remote(o_ref.at[pl.ds(py * heads_y, heads_y)], o_recv.at[y], os_sem.at[d], or_sem.at[d], py, x)

    for d in range(1, ny):
        o_copy(d).start()
    o_recv[y] = o_ref[pl.ds(y * heads_y, heads_y)]
    for d in range(1, ny):
        o_copy(d).wait()
    wo_copy.wait()
    o_rows = [jnp.concatenate([o_recv[t, h] for t in range(ny)], axis=0) for h in range(heads_y)]
    o_full = jnp.concatenate(o_rows, axis=1)
    halves = ps_sem.shape[0]
    wide = width // halves

    def p_copy(c, d):
        py = (y + d) % ny
        at = pl.ds(c * wide, wide)
        return remote(p_send.at[py, :, at], p_recv.at[y, :, at], ps_sem.at[c, d], pr_sem.at[c, d], py, x)

    def h_copy(c, d):
        py = (y + d) % ny
        at = pl.ds(c * wide, wide)
        return remote(hm_send.at[:, at], hm_recv.at[y, :, at], hs_sem.at[c, d], hr_sem.at[c, d], py, x)

    for c in range(halves):
        at = slice(c * wide, (c + 1) * wide)
        part = lax.dot_general(o_full, wo[:, at], NN, preferred_element_type=F32).astype(BF16)
        for t in range(ny):
            p_send[t, :, at] = part[rows * t:rows * (t + 1)]
        for d in (2, 1, 3):
            p_copy(c, d).start()
        p_recv[y, :, at] = p_send[y, :, at]
    for c in range(halves):
        at = slice(c * wide, (c + 1) * wide)
        for d in range(1, ny):
            p_copy(c, d).wait()
        summed = p_recv[0, :, at].astype(F32)
        for t in range(1, ny):
            summed = summed + p_recv[t, :, at].astype(F32)
        hm_send[:, at] = (hrow_ref[:, at] + summed).astype(BF16)
        for d in (2, 1, 3):
            h_copy(c, d).start()
    h_mid = hm_send[...]
    hm_recv[y] = h_mid

    hm_cols[0:rows, :] = h_mid.astype(F32)
    hm_cols[rows:, :] = jnp.zeros((hm_cols.shape[0] - rows, width), F32)
    for j in range(width // 128):
        f_cols[128 * j:128 * (j + 1), :] = jnp.transpose(hm_cols[:, 128 * j:128 * (j + 1)])
    lane16 = lane_ids((16, 128))
    for s in range(total):
        corner = jnp.zeros((16, 128), F32)
        for k in range(cols // 16):
            corner = corner + lane_roll(f_cols[cols * s + 16 * k:cols * s + 16 * (k + 1), :], 64 + 16 * k)
        tail[s] = corner

    for c in range(halves):
        for d in range(1, ny):
            h_copy(c, d).wait()
    gain_copy.wait()
    h64 = jnp.concatenate([hm_recv[t] for t in range(ny)], axis=0).astype(F32)
    inv = lax.rsqrt(jnp.sum(h64 * h64, axis=1, keepdims=True) / width + NORM_EPS)
    u_full[...] = (h64 * inv * gain_ref[...].astype(F32)).astype(BF16)

    def gate_up(c, carry):
        at = pl.multiple_of(c * step, step)
        pltpu.make_async_copy(wgu_hbm.at[:, pl.ds(at, step)], wgu.at[:, pl.ds(at, step)], wgu_sem.at[c]).wait()
        gate = lax.dot_general(wgu[0, pl.ds(at, step), :], u_full[...], NT, preferred_element_type=F32)
        up = lax.dot_general(wgu[1, pl.ds(at, step), :], u_full[...], NT, preferred_element_type=F32)
        gate = gate.astype(BF16).astype(F32)
        up = up.astype(BF16).astype(F32)
        m_cols[pl.ds(at, step), 0:many] = jax.nn.silu(gate) * up
        return carry

    m_cols[:, many:] = jnp.zeros((m_cols.shape[0], 128 - many), F32)
    lax.fori_loop(0, chunk, gate_up, 0)
    for j in range(m_rows.shape[1] // 128):
        m_rows[:, 128 * j:128 * (j + 1)] = jnp.transpose(m_cols[128 * j:128 * (j + 1), :])[0:many].astype(BF16)
    wd_copy.wait()
    group = 384 // cols
    pair = group // ny
    own = (x % pair) * ny + y
    f_sends = []
    for i in range(total // group):
        c = (x // pair + 1 + i) % (total // group)
        at = pl.ds(pl.multiple_of(c * 384, 384), 384)
        f_part[0:many, :] = lax.dot_general(m_rows[...], wd[:, at], NN, preferred_element_type=F32)
        for j in range(3):
            f_cols[128 * j:128 * (j + 1), :] = jnp.transpose(f_part[:, 128 * j:128 * (j + 1)])
        for s in range(group):
            a0 = f_cols[cols * s:cols * s + 16, :]
            a1 = f_cols[cols * s + 16:cols * s + 32, :]
            a2 = lane_roll(f_cols[cols * s + 32:cols * s + 48, :], 64)
            f_send[c * group + s, 0:16] = jnp.where(lane16 < 64, a0, a2).astype(BF16)
            f_send[c * group + s, 16:32] = jnp.where(lane16 < 64, a1, tail[c * group + s]).astype(BF16)
        last = i == total // group - 1
        for k in range(1 if last else 0, group):
            j = (own + k) % group
            s = c * group + j
            f_sends.append(remote(f_send.at[s], f_recv.at[slot], fs_sem.at[s], fr_sem.at[slot], j % ny, c * pair + j // ny))
            f_sends[-1].start()
    f_recv[slot] = f_send[me]
    for copy in f_sends:
        copy.wait_send()
    for k in range(1, total):
        s = (slot + k) % total
        remote(f_send.at[s], f_recv.at[s], fs_sem.at[s], fr_sem.at[s], (y + 1) % ny, x).wait_recv()

    sums = [[jnp.zeros((16, 128), F32) for _ in range(3)] for _ in range(ny)]
    olds = [[jnp.zeros((16, 128), F32) for _ in range(3)] for _ in range(ny)]
    for px in range(nx):
        mine = (lane16 >= rows * px) & (lane16 < rows * (px + 1))
        low = f_recv[px, 0:16].astype(F32)
        for t in range(1, ny):
            low = low + f_recv[t * nx + px, 0:16].astype(F32)
        corner = [f_recv[t * nx + px, 16:32].astype(F32) for t in range(ny)]
        mid = corner[0]
        for t in range(1, ny):
            mid = mid + corner[t]
        high = lane_roll(low, 64)
        for t in range(ny):
            for k, v in enumerate((low, mid, high)):
                sums[t][k] = jnp.where(mine, lane_roll(v, rows * px - rows * t), sums[t][k])
                olds[t][k] = jnp.where(mine, lane_roll(corner[t], rows * px - 64 - 16 * k), olds[t][k])
    for t in range(ny):
        for k in range(3):
            out_ref[16 * k:16 * (k + 1), 128 * t:128 * (t + 1)] = (olds[t][k] + sums[t][k]).astype(BF16)


def solution(mesh):
    group_axes = ('yz', 'x')
    batch_axes = ('replica', 'yz', 'x')
    hidden_spec = P('replica', ('x', 'yz'))
    cache_spec = P(None, batch_axes, None, None)
    ny, nx = mesh.shape['yz'], mesh.shape['x']
    vmem = pl.BlockSpec(memory_space=pltpu.VMEM)
    hbm = pl.BlockSpec(memory_space=pl.ANY)
    dma = pltpu.SemaphoreType.DMA

    def layer(ht, seq_lens, attn_gain, mlp_gain, w_qkv, w_out, w_gate_up, w_down, k_cache, v_cache):
        cols = ht.shape[0]
        rows, slots, head_dim = k_cache.shape
        width = attn_gain.shape[1]
        qcols = w_qkv.shape[0]
        qpad = -(-qcols // 128) * 128
        heads = (qcols * ny) // head_dim - 2
        total = ny * nx
        many = ny * rows
        ffn = w_down.shape[0]
        ffn_pad = -(-ffn // 128) * 128
        in_hbm = functools.partial(pltpu.with_memory_space_constraint, memory_space=pltpu.HBM)
        parts = 4
        z, hrow, k_vmem, v_vmem = pl.pallas_call(
            functools.partial(qkv_kernel, ny, nx, cols, rows, width),
            out_shape=(jax.ShapeDtypeStruct((rows, 16, head_dim), F32), jax.ShapeDtypeStruct((rows, width), F32),
                       pltpu.VMEM(k_cache.shape, BF16), pltpu.VMEM(v_cache.shape, BF16)),
            in_specs=[hbm] * 5,
            out_specs=(vmem,) * 4,
            scratch_shapes=[
                pltpu.VMEM(ht.shape, BF16), pltpu.VMEM(attn_gain.shape, BF16),
                pltpu.VMEM((nx, 32, 128), BF16), pltpu.VMEM((total, 32, 128), BF16), pltpu.VMEM((qpad, width), BF16),
                pltpu.VMEM((width, 128), F32), pltpu.VMEM((width, 128), F32), pltpu.VMEM((width, 128), BF16),
                pltpu.VMEM((qpad, 128), F32), pltpu.VMEM((ny, rows, qpad), BF16), pltpu.VMEM((ny, rows, qpad), BF16),
                pltpu.VMEM((128, width), F32),
                dma, dma, dma, dma((2, parts)), dma((total,)), dma((total,)), dma((ny,)), dma((ny,))],
            compiler_params=pltpu.CompilerParams(collective_id=0, has_side_effects=True, vmem_limit_bytes=12 << 20),
            cost_estimate=pl.CostEstimate(flops=8_000_000_000, bytes_accessed=20_000_000, transcendentals=0),
            name='qkv',
        )(in_hbm(ht), in_hbm(attn_gain), in_hbm(w_qkv), in_hbm(k_cache), in_hbm(v_cache))
        k_new, v_new, o, _, _ = pl.pallas_call(
            functools.partial(attend_kernel, heads, head_dim ** -0.5),
            out_shape=(pltpu.HBM(k_cache.shape, BF16), pltpu.HBM(v_cache.shape, BF16),
                       jax.ShapeDtypeStruct((heads, rows, head_dim), BF16),
                       pltpu.VMEM(k_cache.shape, BF16), pltpu.VMEM(v_cache.shape, BF16)),
            in_specs=[pl.BlockSpec(memory_space=pltpu.SMEM), vmem, vmem, vmem],
            out_specs=(hbm, hbm, vmem, vmem, vmem),
            input_output_aliases={2: 3, 3: 4},
            scratch_shapes=[pltpu.VMEM((2, 32, slots), F32), pltpu.VMEM((rows, 16, head_dim), F32), dma((rows,)), dma((rows,))],
            compiler_params=pltpu.CompilerParams(vmem_limit_bytes=8 << 20),
            cost_estimate=pl.CostEstimate(flops=8_000_000_000, bytes_accessed=20_000_000, transcendentals=0),
            name='attend',
        )(seq_lens, z, k_vmem, v_vmem)
        chunk = 5
        out = pl.pallas_call(
            functools.partial(mlp_kernel, ny, nx, cols, rows, width, heads),
            out_shape=jax.ShapeDtypeStruct(ht.shape, BF16),
            in_specs=[vmem, vmem, hbm, hbm, hbm, hbm],
            out_specs=vmem,
            scratch_shapes=[
                pltpu.VMEM(mlp_gain.shape, BF16),
                pltpu.VMEM(w_out.shape, BF16), pltpu.VMEM(w_gate_up.shape, BF16), pltpu.VMEM((ffn_pad, width), BF16),
                pltpu.VMEM((ny, heads // ny, rows, head_dim), BF16),
                pltpu.VMEM((ny, rows, width), BF16), pltpu.VMEM((ny, rows, width), BF16),
                pltpu.VMEM((rows, width), BF16), pltpu.VMEM((ny, rows, width), BF16),
                pltpu.VMEM((128, width), F32), pltpu.VMEM((total, 16, 128), F32),
                pltpu.VMEM((many, width), BF16), pltpu.VMEM((ffn_pad, 128), F32), pltpu.VMEM((many, ffn_pad), BF16),
                pltpu.VMEM((128, 384), F32), pltpu.VMEM((width, 128), F32),
                pltpu.VMEM((total, 32, 128), BF16), pltpu.VMEM((total, 32, 128), BF16),
                dma, dma, dma((chunk,)), dma, dma((ny,)), dma((ny,)),
                dma((2, ny)), dma((2, ny)), dma((2, ny)), dma((2, ny)),
                dma((total,)), dma((total,))],
            compiler_params=pltpu.CompilerParams(collective_id=1, has_side_effects=True, vmem_limit_bytes=44 << 20),
            name='mlp',
        )(o, hrow, in_hbm(mlp_gain), in_hbm(w_out), in_hbm(w_gate_up), in_hbm(w_down))
        return out, k_new, v_new

    def local_step(hidden, seq_lens, attn_gain, mlp_gain, w_qkv, w_out, w_gate_up, w_down, k_cache, v_cache):
        ht = hidden.T
        k_layers = []
        v_layers = []
        for i in range(w_qkv.shape[0]):
            ht, k_new, v_new = layer(ht, seq_lens, attn_gain[i:i + 1], mlp_gain[i:i + 1], w_qkv[i].T, w_out[i],
                                     jnp.transpose(w_gate_up[i], (1, 2, 0)), w_down[i], k_cache[i], v_cache[i])
            k_layers.append(k_new)
            v_layers.append(v_new)
        return ht.T, jnp.stack(k_layers), jnp.stack(v_layers)

    return jax.shard_map(
        local_step,
        mesh=mesh,
        in_specs=(hidden_spec, P(batch_axes), P(None, None), P(None, None), P(None, None, 'yz'), P(None, 'yz', None),
                  P(None, None, None, 'yz'), P(None, 'yz', None), cache_spec, cache_spec),
        out_specs=(hidden_spec, cache_spec, cache_spec),
        check_vma=False)
```

```python
import functools

import jax
import jax.numpy as jnp
from jax import lax
from jax.experimental import pallas as pl
from jax.experimental.pallas import tpu as pltpu
from jax.sharding import PartitionSpec as P

NORM_EPS = 1e-5
MESH = pl.DeviceIdType.MESH
F32 = jnp.float32
BF16 = jnp.bfloat16
NT = (((1,), (1,)), ((), ()))
NN = (((1,), (0,)), ((), ()))


def lane_ids(shape):
    return lax.broadcasted_iota(jnp.int32, shape, len(shape) - 1)


def lane_roll(v, shift):
    shift = shift % v.shape[-1]
    return v if shift == 0 else pltpu.roll(v, shift, v.ndim - 1)


def position(ny, nx):
    return lax.axis_index('yz'), lax.axis_index('x')


def peers(y, x, ny, nx):
    ys = [(y + d) % ny for d in range(ny)]
    xs = [(x + d) % nx for d in range(nx)]
    far_y = sorted(range(ny), key=lambda d: -min(d, ny - d))
    far_x = sorted(range(nx), key=lambda d: -min(d, nx - d))
    return [(dy * nx + dx, ys[dy], xs[dx]) for dx in far_x for dy in far_y if dy or dx]


def greet_all(others):
    barrier = pltpu.get_barrier_semaphore()
    for _, py, px in others:
        pl.semaphore_signal(barrier, inc=1, device_id={'yz': py, 'x': px}, device_id_type=MESH)
    return barrier


def remote(src, dst, send_sem, recv_sem, py, px):
    return pltpu.make_async_remote_copy(src_ref=src, dst_ref=dst, send_sem=send_sem, recv_sem=recv_sem,
                                        device_id={'yz': py, 'x': px}, device_id_type=MESH)


def qkv_kernel(ny, nx, cols, rows, width, ht_hbm, gain_hbm, w_hbm, k_hbm, v_hbm, z_ref, hrow_ref, k_ref, v_ref,
               ht_ref, gain_ref, send_buf, recv_buf, w_vmem, gain_col, h_full, u_full, zt_buf, z_send, z_recv, h_rows,
               h_sem, g_sem, w_sem, kv_sem, send_sem, recv_sem, zsend_sem, zrecv_sem):
    y, x = position(ny, nx)
    total = ny * nx
    me = x * ny + y
    qcols = w_hbm.shape[0]
    h_copy = pltpu.make_async_copy(ht_hbm, ht_ref, h_sem)
    h_copy.start()
    others = peers(y, x, ny, nx)
    barrier = greet_all(others)
    g_copy = pltpu.make_async_copy(gain_hbm, gain_ref, g_sem)
    g_copy.start()
    w_copy = pltpu.make_async_copy(w_hbm, w_vmem.at[pl.ds(0, qcols)], w_sem)
    w_copy.start()
    parts = kv_sem.shape[1]
    share = k_hbm.shape[0] // parts
    kv_copies = [pltpu.make_async_copy(src.at[pl.ds(i * share, share)], dst.at[pl.ds(i * share, share)], kv_sem.at[c, i])
                 for i in range(parts) for c, (src, dst) in enumerate(((k_hbm, k_ref), (v_hbm, v_ref)))]
    for copy in kv_copies:
        copy.start()
    h_copy.wait()

    lane = lane_ids((cols, 128))
    lane16 = lane_ids((16, 128))
    tiles = [ht_ref[:, 128 * t:128 * (t + 1)].astype(F32) for t in range(ny)]
    for px in range(nx):
        block = jnp.zeros((cols, 128), F32)
        for t in range(ny):
            piece = lane_roll(tiles[t], rows * t - rows * px)
            block = jnp.where((lane >= rows * t) & (lane < rows * (t + 1)), piece, block)
        high = lane_roll(block[32:48], 64)
        send_buf[px, 0:16] = jnp.where(lane16 < 64, block[0:16], high).astype(BF16)
        send_buf[px, 16:32] = block[16:32].astype(BF16)

    pl.semaphore_wait(barrier, total - 1)

    h_sends = [remote(send_buf.at[px], recv_buf.at[me], send_sem.at[d], recv_sem.at[d], py, px) for d, py, px in others]
    for copy in h_sends:
        copy.start()
    recv_buf[me] = send_buf[x]

    g_copy.wait()
    for j in range(width // 128):
        row = gain_ref[0:1, 128 * j:128 * (j + 1)].astype(F32)
        gain_col[128 * j:128 * (j + 1), :] = jnp.transpose(jnp.broadcast_to(row, (128, 128)))
    w_vmem[qcols:, :] = jnp.zeros((w_vmem.shape[0] - qcols, width), BF16)

    for copy in h_sends:
        copy.wait()

    square = jnp.zeros((16, 128), F32)
    for s in range(total):
        low = recv_buf[s, 0:16].astype(F32)
        mid = recv_buf[s, 16:32].astype(F32)
        high = lane_roll(low, 64)
        h_full[cols * s:cols * s + 16, :] = low
        h_full[cols * s + 16:cols * s + 32, :] = mid
        h_full[cols * s + 32:cols * s + 48, :] = high
        square = square + low * low + mid * mid + high * high
    power = jnp.sum(square, axis=0, keepdims=True)
    inv = lax.rsqrt(power / width + NORM_EPS)
    u_full[...] = (h_full[...] * inv * gain_col[...]).astype(BF16)
    w_copy.wait()
    zt_buf[...] = lax.dot_general(w_vmem[...], u_full[...], NN, preferred_element_type=F32)
    for j in range(zt_buf.shape[0] // 128):
        zj = jnp.transpose(zt_buf[128 * j:128 * (j + 1), :])
        for t in range(ny):
            z_send[t, :, 128 * j:128 * (j + 1)] = zj[rows * t:rows * (t + 1)].astype(BF16)
    for d in range(1, ny):
        py = (y + d) % ny
        remote(z_send.at[py], z_recv.at[y], zsend_sem.at[d], zrecv_sem.at[d], py, x).start()
    z_recv[y] = z_send[y]

    for j in range(width // 128):
        h_rows[:, 128 * j:128 * (j + 1)] = jnp.transpose(h_full[128 * j:128 * (j + 1), :])
    hrow_ref[...] = h_rows[pl.ds(pl.multiple_of(y * rows, rows), rows), :]

    for d in range(1, ny):
        py = (y + d) % ny
        remote(z_send.at[py], z_recv.at[y], zsend_sem.at[d], zrecv_sem.at[d], py, x).wait()

    zs = [[z_recv[t, :, 128 * j:128 * (j + 1)].astype(F32) for j in range(w_vmem.shape[0] // 128)] for t in range(ny)]
    for g in range(ny * qcols // 128):
        start = 128 * g
        t = start // qcols
        off = start - t * qcols
        j, sh = off // 128, off % 128
        take = min(128, qcols - off)
        out = lane_roll(zs[t][j], -sh)
        if sh and take > 128 - sh:
            out = jnp.where(lane16 < 128 - sh, out, lane_roll(zs[t][j + 1], -sh))
        if take < 128:
            out = jnp.where(lane16 < take, out, lane_roll(zs[t + 1][0], take))
        z_ref[:, g, :] = out
    for g in range(ny * qcols // 128, z_ref.shape[1]):
        z_ref[:, g, :] = jnp.zeros((rows, 128), F32)
    for copy in kv_copies:
        copy.wait()


def attend_kernel(heads, scale, len_ref, z_ref, k_in, v_in, k_hbm, v_hbm, o_ref, k_ref, v_ref, s_buf, o_acc, k_sem, v_sem):
    rows, slots = k_ref.shape[:2]

    def place(b, carry):
        length = len_ref[b]
        base = pl.multiple_of((length // 16) * 16, 16)
        here = lax.broadcasted_iota(jnp.int32, (16, 128), 0) == length - base
        k_new = jnp.broadcast_to(z_ref[b, heads:heads + 1, :], (16, 128)).astype(BF16)
        v_new = jnp.broadcast_to(z_ref[b, heads + 1:heads + 2, :], (16, 128)).astype(BF16)
        k_ref[b, pl.ds(base, 16), :] = jnp.where(here, k_new, k_ref[b, pl.ds(base, 16), :])
        v_ref[b, pl.ds(base, 16), :] = jnp.where(here, v_new, v_ref[b, pl.ds(base, 16), :])
        return carry

    def k_copy(b):
        return pltpu.make_async_copy(k_ref.at[b], k_hbm.at[b], k_sem.at[b])

    def v_copy(b):
        return pltpu.make_async_copy(v_ref.at[b], v_hbm.at[b], v_sem.at[b])

    def leave(b, carry):
        k_copy(b).start()
        v_copy(b).start()
        return carry

    def score(i, slot):
        blank = jnp.zeros((16, 128), BF16)
        q0, q1 = z_ref[2 * i].astype(BF16), z_ref[2 * i + 1].astype(BF16)
        q = jnp.concatenate([jnp.concatenate([q0, blank], axis=1), jnp.concatenate([blank, q1], axis=1)], axis=0)
        keys = jnp.concatenate([k_ref[2 * i], k_ref[2 * i + 1]], axis=1)
        s_buf[slot] = lax.dot_general(q, keys, NT, preferred_element_type=F32) * scale

    def finish(i, slot):
        s = s_buf[slot]
        first = lax.broadcasted_iota(jnp.int32, (32, 1), 0) < 16
        length = jnp.where(first, len_ref[2 * i], len_ref[2 * i + 1])
        s = jnp.where(lane_ids(s.shape) <= length, s, -1e30)
        e = jnp.exp(s - jnp.max(s, axis=1, keepdims=True))
        p = (e * (1.0 / jnp.sum(e, axis=1, keepdims=True))).astype(BF16)
        values = jnp.concatenate([v_ref[2 * i], v_ref[2 * i + 1]], axis=1)
        o = lax.dot_general(p, values, NN, preferred_element_type=F32)
        o_acc[2 * i] = o[0:16, 0:128]
        o_acc[2 * i + 1] = o[16:32, 128:256]

    lax.fori_loop(0, rows, place, 0)
    lax.fori_loop(0, rows, leave, 0)
    score(0, 0)
    for i in range(rows // 2 - 1):
        score(i + 1, (i + 1) % 2)
        finish(i, i % 2)
    finish(rows // 2 - 1, (rows // 2 - 1) % 2)
    for h in range(heads):
        o_ref[h] = o_acc[:, h, :].astype(BF16)

    def drain(b, carry):
        k_copy(b).wait()
        v_copy(b).wait()
        return carry

    lax.fori_loop(0, rows, drain, 0)


def proj_kernel(ny, nx, cols, rows, width, heads, o_ref, hrow_ref, gain_hbm, wo_hbm, wgu_hbm, wd_hbm,
                u_ref, tail_ref, wgu_ref, wd_ref,
                gain_ref, wo, o_recv, p_send, p_recv, hm_send, hm_recv, hm_rows, hm_cols,
                gain_sem, wo_sem, wgu_sem, wd_sem, os_sem, or_sem, ps_sem, pr_sem, hs_sem, hr_sem):
    y, x = lax.axis_index('yz'), lax.axis_index('x')
    total = ny * nx
    heads_y = heads // ny
    many = ny * rows
    ffn = wd_hbm.shape[0]
    ring = [(d, (y + d) % ny) for d in sorted(range(1, ny), key=lambda d: -min(d, ny - d))]
    barrier = pltpu.get_barrier_semaphore()
    for _, py in ring:
        pl.semaphore_signal(barrier, inc=1, device_id={'yz': py, 'x': x}, device_id_type=MESH)
    wo_copy = pltpu.make_async_copy(wo_hbm, wo, wo_sem)
    gain_copy = pltpu.make_async_copy(gain_hbm, gain_ref, gain_sem)
    parts = wgu_sem.shape[0]
    share = ffn // parts
    loads = [pltpu.make_async_copy(wgu_hbm.at[:, pl.ds(c * share, share)], wgu_ref.at[:, pl.ds(c * share, share)], wgu_sem.at[c])
             for c in range(parts)]
    loads.append(pltpu.make_async_copy(wd_hbm, wd_ref.at[pl.ds(0, ffn)], wd_sem))
    for copy in [wo_copy, gain_copy] + loads:
        copy.start()
    pl.semaphore_wait(barrier, ny - 1)

    o_sends = [remote(o_ref.at[pl.ds(py * heads_y, heads_y)], o_recv.at[y], os_sem.at[d], or_sem.at[d], py, x) for d, py in ring]
    for copy in o_sends:
        copy.start()
    o_recv[y] = o_ref[pl.ds(y * heads_y, heads_y)]
    wd_ref[ffn:, :] = jnp.zeros((wd_ref.shape[0] - ffn, width), BF16)
    wo_copy.wait()
    for copy in o_sends:
        copy.wait()
    o_rows = [jnp.concatenate([o_recv[t, h] for t in range(ny)], axis=0) for h in range(heads_y)]
    o_full = jnp.concatenate(o_rows, axis=1)

    halves = ps_sem.shape[0]
    wide = width // halves

    def p_copies(c):
        at = pl.ds(c * wide, wide)
        return [remote(p_send.at[py, :, at], p_recv.at[y, :, at], ps_sem.at[c, d], pr_sem.at[c, d], py, x) for d, py in ring]

    def h_copies(c):
        at = pl.ds(c * wide, wide)
        return [remote(hm_send.at[:, at], hm_recv.at[y, :, at], hs_sem.at[c, d], hr_sem.at[c, d], py, x) for d, py in ring]

    for c in range(halves):
        at = slice(c * wide, (c + 1) * wide)
        part = lax.dot_general(o_full, wo[:, at], NN, preferred_element_type=F32).astype(BF16)
        for t in range(ny):
            p_send[t, :, at] = part[rows * t:rows * (t + 1)]
        for copy in p_copies(c):
            copy.start()
        p_recv[y, :, at] = p_send[y, :, at]
    for c in range(halves):
        at = slice(c * wide, (c + 1) * wide)
        for copy in p_copies(c):
            copy.wait()
        summed = p_recv[0, :, at].astype(F32)
        for t in range(1, ny):
            summed = summed + p_recv[t, :, at].astype(F32)
        hm_send[:, at] = (hrow_ref[:, at] + summed).astype(BF16)
        for copy in h_copies(c):
            copy.start()
    h_mid = hm_send[...]
    hm_recv[y] = h_mid

    hm_rows[0:rows, :] = h_mid.astype(F32)
    hm_rows[rows:, :] = jnp.zeros((hm_rows.shape[0] - rows, width), F32)
    for j in range(width // 128):
        hm_cols[128 * j:128 * (j + 1), :] = jnp.transpose(hm_rows[:, 128 * j:128 * (j + 1)])
    for s in range(total):
        corner = jnp.zeros((16, 128), F32)
        for k in range(cols // 16):
            corner = corner + lane_roll(hm_cols[cols * s + 16 * k:cols * s + 16 * (k + 1), :], 64 + 16 * k)
        tail_ref[s] = corner
    u_ref[many:, :] = jnp.zeros((u_ref.shape[0] - many, width), BF16)

    gain_copy.wait()
    for c in range(halves):
        for copy in h_copies(c):
            copy.wait()
    h64 = jnp.concatenate([hm_recv[t] for t in range(ny)], axis=0).astype(F32)
    inv = lax.rsqrt(jnp.sum(h64 * h64, axis=1, keepdims=True) / width + NORM_EPS)
    u_ref[0:many, :] = (h64 * inv * gain_ref[...].astype(F32)).astype(BF16)
    for copy in loads:
        copy.wait()


def mlp_kernel(ny, nx, cols, rows, width, ffn, u_ref, tail_ref, wgu, wd, out_ref, m_rows, f_part, f_cols, f_send, f_recv, fs_sem, fr_sem):
    y, x = lax.axis_index('yz'), lax.axis_index('x')
    total = ny * nx
    me = x * ny + y
    slot = y * nx + x
    many = ny * rows
    barrier = greet_all(peers(y, x, ny, nx))
    lane16 = lane_ids((16, 128))

    for base in range(0, ffn, 512):
        size = min(512, ffn - base)
        gate = lax.dot_general(wgu[0, base:base + size, :], u_ref[...], NT, preferred_element_type=F32)
        up = lax.dot_general(wgu[1, base:base + size, :], u_ref[...], NT, preferred_element_type=F32)
        gate = gate.astype(BF16).astype(F32)
        m = jax.nn.silu(gate) * up.astype(BF16).astype(F32)
        if size % 128:
            m = jnp.concatenate([m, jnp.zeros((128 - size % 128, 128), F32)], axis=0)
        for j in range(m.shape[0] // 128):
            m_rows[:, base + 128 * j:base + 128 * (j + 1)] = jnp.transpose(m[128 * j:128 * (j + 1)])[0:many].astype(BF16)

    chunks = f_part.shape[0]
    wide = width // chunks
    group = total // chunks
    span = nx // chunks
    own = (x % span) * ny + y
    f_part[:, many:, :] = jnp.zeros((chunks, f_part.shape[1] - many, wide), F32)
    pl.semaphore_wait(barrier, total - 1)
    f_sends = []
    for i in range(chunks):
        c = (x // span + 1 + i) % chunks
        at = pl.ds(pl.multiple_of(c * wide, wide), wide)
        f_part[i, 0:many, :] = lax.dot_general(m_rows[...], wd[:, at], NN, preferred_element_type=F32)
        for j in range(wide // 128):
            f_cols[i, 128 * j:128 * (j + 1), :] = jnp.transpose(f_part[i, :, 128 * j:128 * (j + 1)])
        for s in range(group):
            a0 = f_cols[i, cols * s:cols * s + 16, :]
            a1 = f_cols[i, cols * s + 16:cols * s + 32, :]
            a2 = lane_roll(f_cols[i, cols * s + 32:cols * s + 48, :], 64)
            f_send[c * group + s, 0:16] = jnp.where(lane16 < 64, a0, a2).astype(BF16)
            f_send[c * group + s, 16:32] = jnp.where(lane16 < 64, a1, tail_ref[c * group + s]).astype(BF16)
        for k in range(1 if i == chunks - 1 else 0, group):
            j = (own + k) % group
            s = c * group + j
            f_sends.append(remote(f_send.at[s], f_recv.at[slot], fs_sem.at[s], fr_sem.at[slot], j % ny, c * span + j // ny))
            f_sends[-1].start()
    f_recv[slot] = f_send[me]
    for k in range(1, total):
        s = (slot + k) % total
        remote(f_send.at[s], f_recv.at[s], fs_sem.at[s], fr_sem.at[s], (y + 1) % ny, x).wait_recv()

    sums = [[jnp.zeros((16, 128), F32) for _ in range(3)] for _ in range(ny)]
    olds = [[jnp.zeros((16, 128), F32) for _ in range(3)] for _ in range(ny)]
    for px in range(nx):
        mine = (lane16 >= rows * px) & (lane16 < rows * (px + 1))
        low = f_recv[px, 0:16].astype(F32)
        for t in range(1, ny):
            low = low + f_recv[t * nx + px, 0:16].astype(F32)
        corner = [f_recv[t * nx + px, 16:32].astype(F32) for t in range(ny)]
        mid = corner[0]
        for t in range(1, ny):
            mid = mid + corner[t]
        high = lane_roll(low, 64)
        for t in range(ny):
            for k, v in enumerate((low, mid, high)):
                sums[t][k] = jnp.where(mine, lane_roll(v, rows * px - rows * t), sums[t][k])
                olds[t][k] = jnp.where(mine, lane_roll(corner[t], rows * px - 64 - 16 * k), olds[t][k])
    for t in range(ny):
        for k in range(3):
            out_ref[16 * k:16 * (k + 1), 128 * t:128 * (t + 1)] = (olds[t][k] + sums[t][k]).astype(BF16)
    for copy in f_sends:
        copy.wait_send()


def solution(mesh):
    group_axes = ('yz', 'x')
    batch_axes = ('replica', 'yz', 'x')
    hidden_spec = P('replica', ('x', 'yz'))
    cache_spec = P(None, batch_axes, None, None)
    ny, nx = mesh.shape['yz'], mesh.shape['x']
    vmem = pl.BlockSpec(memory_space=pltpu.VMEM)
    hbm = pl.BlockSpec(memory_space=pl.ANY)
    dma = pltpu.SemaphoreType.DMA

    def layer(ht, seq_lens, attn_gain, mlp_gain, w_qkv, w_out, w_gate_up, w_down, k_cache, v_cache):
        cols = ht.shape[0]
        rows, slots, head_dim = k_cache.shape
        width = attn_gain.shape[1]
        qcols = w_qkv.shape[0]
        qpad = -(-qcols // 128) * 128
        heads = (qcols * ny) // head_dim - 2
        total = ny * nx
        many = ny * rows
        ffn = w_down.shape[0]
        ffn_pad = -(-ffn // 128) * 128
        in_hbm = functools.partial(pltpu.with_memory_space_constraint, memory_space=pltpu.HBM)
        parts = 4
        z, hrow, k_vmem, v_vmem = pl.pallas_call(
            functools.partial(qkv_kernel, ny, nx, cols, rows, width),
            out_shape=(jax.ShapeDtypeStruct((rows, 16, head_dim), F32), jax.ShapeDtypeStruct((rows, width), F32),
                       pltpu.VMEM(k_cache.shape, BF16), pltpu.VMEM(v_cache.shape, BF16)),
            in_specs=[hbm] * 5,
            out_specs=(vmem,) * 4,
            scratch_shapes=[
                pltpu.VMEM(ht.shape, BF16), pltpu.VMEM(attn_gain.shape, BF16),
                pltpu.VMEM((nx, 32, 128), BF16), pltpu.VMEM((total, 32, 128), BF16), pltpu.VMEM((qpad, width), BF16),
                pltpu.VMEM((width, 128), F32), pltpu.VMEM((width, 128), F32), pltpu.VMEM((width, 128), BF16),
                pltpu.VMEM((qpad, 128), F32), pltpu.VMEM((ny, rows, qpad), BF16), pltpu.VMEM((ny, rows, qpad), BF16),
                pltpu.VMEM((128, width), F32),
                dma, dma, dma, dma((2, parts)), dma((total,)), dma((total,)), dma((ny,)), dma((ny,))],
            compiler_params=pltpu.CompilerParams(collective_id=0, has_side_effects=True, vmem_limit_bytes=12 << 20),
            cost_estimate=pl.CostEstimate(flops=8_000_000_000, bytes_accessed=20_000_000, transcendentals=0),
            name='qkv',
        )(in_hbm(ht), in_hbm(attn_gain), in_hbm(w_qkv), in_hbm(k_cache), in_hbm(v_cache))
        k_new, v_new, o, _, _ = pl.pallas_call(
            functools.partial(attend_kernel, heads, head_dim ** -0.5),
            out_shape=(pltpu.HBM(k_cache.shape, BF16), pltpu.HBM(v_cache.shape, BF16),
                       jax.ShapeDtypeStruct((heads, rows, head_dim), BF16),
                       pltpu.VMEM(k_cache.shape, BF16), pltpu.VMEM(v_cache.shape, BF16)),
            in_specs=[pl.BlockSpec(memory_space=pltpu.SMEM), vmem, vmem, vmem],
            out_specs=(hbm, hbm, vmem, vmem, vmem),
            input_output_aliases={2: 3, 3: 4},
            scratch_shapes=[pltpu.VMEM((2, 32, slots), F32), pltpu.VMEM((rows, 16, head_dim), F32), dma((rows,)), dma((rows,))],
            compiler_params=pltpu.CompilerParams(vmem_limit_bytes=8 << 20),
            cost_estimate=pl.CostEstimate(flops=8_000_000_000, bytes_accessed=20_000_000, transcendentals=0),
            name='attend',
        )(seq_lens, z, k_vmem, v_vmem)
        u, tail, wgu_vmem, wd_vmem = pl.pallas_call(
            functools.partial(proj_kernel, ny, nx, cols, rows, width, heads),
            out_shape=(pltpu.VMEM((128, width), BF16), pltpu.VMEM((total, 16, 128), F32),
                       pltpu.VMEM(w_gate_up.shape, BF16), pltpu.VMEM((ffn_pad, width), BF16)),
            in_specs=[vmem, vmem, hbm, hbm, hbm, hbm],
            out_specs=(vmem,) * 4,
            scratch_shapes=[
                pltpu.VMEM(mlp_gain.shape, BF16), pltpu.VMEM(w_out.shape, BF16),
                pltpu.VMEM((ny, heads // ny, rows, head_dim), BF16),
                pltpu.VMEM((ny, rows, width), BF16), pltpu.VMEM((ny, rows, width), BF16),
                pltpu.VMEM((rows, width), BF16), pltpu.VMEM((ny, rows, width), BF16),
                pltpu.VMEM((128, width), F32), pltpu.VMEM((width, 128), F32),
                dma, dma, dma((5,)), dma, dma((ny,)), dma((ny,)),
                dma((2, ny)), dma((2, ny)), dma((2, ny)), dma((2, ny))],
            compiler_params=pltpu.CompilerParams(collective_id=1, has_side_effects=True, vmem_limit_bytes=12 << 20),
            cost_estimate=pl.CostEstimate(flops=8_000_000_000, bytes_accessed=20_000_000, transcendentals=0),
            name='proj',
        )(o, hrow, in_hbm(mlp_gain), in_hbm(w_out), in_hbm(w_gate_up), in_hbm(w_down))
        out = pl.pallas_call(
            functools.partial(mlp_kernel, ny, nx, cols, rows, width, ffn),
            out_shape=jax.ShapeDtypeStruct(ht.shape, BF16),
            in_specs=[vmem] * 4,
            out_specs=vmem,
            scratch_shapes=[
                pltpu.VMEM((many, ffn_pad), BF16), pltpu.VMEM((2, 128, width // 2), F32), pltpu.VMEM((2, width // 2, 128), F32),
                pltpu.VMEM((total, 32, 128), BF16), pltpu.VMEM((total, 32, 128), BF16), dma((total,)), dma((total,))],
            compiler_params=pltpu.CompilerParams(collective_id=2, has_side_effects=True, vmem_limit_bytes=12 << 20),
            cost_estimate=pl.CostEstimate(flops=8_000_000_000, bytes_accessed=20_000_000, transcendentals=0),
            name='mlp',
        )(u, tail, wgu_vmem, wd_vmem)
        return out, k_new, v_new

    def local_step(hidden, seq_lens, attn_gain, mlp_gain, w_qkv, w_out, w_gate_up, w_down, k_cache, v_cache):
        ht = hidden.T
        k_layers = []
        v_layers = []
        for i in range(w_qkv.shape[0]):
            ht, k_new, v_new = layer(ht, seq_lens, attn_gain[i:i + 1], mlp_gain[i:i + 1], w_qkv[i].T, w_out[i],
                                     jnp.transpose(w_gate_up[i], (1, 2, 0)), w_down[i], k_cache[i], v_cache[i])
            k_layers.append(k_new)
            v_layers.append(v_new)
        return ht.T, jnp.stack(k_layers), jnp.stack(v_layers)

    return jax.shard_map(
        local_step,
        mesh=mesh,
        in_specs=(hidden_spec, P(batch_axes), P(None, None), P(None, None), P(None, None, 'yz'), P(None, 'yz', None),
                  P(None, None, None, 'yz'), P(None, 'yz', None), cache_spec, cache_spec),
        out_specs=(hidden_spec, cache_spec, cache_spec),
        check_vma=False)
```

```python
import functools

import jax
import jax.numpy as jnp
from jax import lax
from jax.experimental import pallas as pl
from jax.experimental.pallas import tpu as pltpu
from jax.sharding import PartitionSpec as P

NORM_EPS = 1e-5
MESH = pl.DeviceIdType.MESH
F32 = jnp.float32
BF16 = jnp.bfloat16
NT = (((1,), (1,)), ((), ()))
NN = (((1,), (0,)), ((), ()))


def lane_ids(shape):
    return lax.broadcasted_iota(jnp.int32, shape, len(shape) - 1)


def lane_roll(v, shift):
    shift = shift % v.shape[-1]
    return v if shift == 0 else pltpu.roll(v, shift, v.ndim - 1)


def twist(t, g, ny):
    flip = (t // (ny // 2)) % 2
    return g + flip * (1 - 2 * (g % 2))


def peers(y, x, ny, nx):
    ys = [(y + d) % ny for d in range(ny)]
    xs = [(x + d) % nx for d in range(nx)]
    far_y = sorted(range(ny), key=lambda d: -min(d, ny - d))
    far_x = sorted(range(nx), key=lambda d: -min(d, nx - d))
    return [(dy * nx + dx, ys[dy], xs[dx]) for dx in far_x for dy in far_y if dy or dx]


def ring(y, g, ny):
    far = sorted(range(1, ny), key=lambda d: -min(d, ny - d))
    return [(d, (y + d) % ny, twist((y + d) % ny, g, ny)) for d in far]


def greet_all(others):
    barrier = pltpu.get_barrier_semaphore()
    for _, py, px in others:
        pl.semaphore_signal(barrier, inc=1, device_id={'yz': py, 'x': px}, device_id_type=MESH)
    return barrier


def remote(src, dst, send_sem, recv_sem, py, px):
    return pltpu.make_async_remote_copy(src_ref=src, dst_ref=dst, send_sem=send_sem, recv_sem=recv_sem,
                                        device_id={'yz': py, 'x': px}, device_id_type=MESH)


def qkv_kernel(ny, nx, cols, rows, width, ht_hbm, gain_hbm, w_hbm, k_hbm, v_hbm, z_ref, hrow_ref, k_ref, v_ref,
               ht_ref, gain_ref, send_buf, recv_buf, w_vmem, gain_col, h_full, u_full, zt_buf, z_send, z_recv, h_rows,
               h_sem, g_sem, w_sem, kv_sem, send_sem, recv_sem, zsend_sem, zrecv_sem):
    y, x = lax.axis_index('yz'), lax.axis_index('x')
    mine = twist(y, x, ny)
    total = ny * nx
    me = x * ny + y
    qcols = w_hbm.shape[0]
    h_copy = pltpu.make_async_copy(ht_hbm, ht_ref, h_sem)
    h_copy.start()
    others = peers(y, x, ny, nx)
    barrier = greet_all(others)
    g_copy = pltpu.make_async_copy(gain_hbm, gain_ref, g_sem)
    g_copy.start()
    w_copy = pltpu.make_async_copy(w_hbm, w_vmem.at[pl.ds(0, qcols)], w_sem)
    w_copy.start()
    parts = kv_sem.shape[1]
    share = k_hbm.shape[0] // parts
    kv_copies = [pltpu.make_async_copy(src.at[pl.ds(i * share, share)], dst.at[pl.ds(i * share, share)], kv_sem.at[c, i])
                 for i in range(parts) for c, (src, dst) in enumerate(((k_hbm, k_ref), (v_hbm, v_ref)))]
    for copy in kv_copies:
        copy.start()
    h_copy.wait()

    lane = lane_ids((cols, 128))
    lane16 = lane_ids((16, 128))
    half = cols // 2
    tiles = [ht_ref[:, 128 * t:128 * (t + 1)].astype(F32) for t in range(ny)]
    for g in range(nx):
        block = jnp.zeros((cols, 128), F32)
        for t in range(ny):
            piece = lane_roll(tiles[t], rows * t - rows * twist(t, g, ny))
            block = jnp.where((lane >= rows * t) & (lane < rows * (t + 1)), piece, block)
        block = jnp.where(lane[0:half] < 64, block[0:half], lane_roll(block[half:cols], 64))
        for k in range(half // 8):
            send_buf[g, k] = block[8 * k:8 * (k + 1)].astype(BF16)

    pl.semaphore_wait(barrier, total - 1)

    h_sends = [remote(send_buf.at[twist(py, px, ny)], recv_buf.at[me], send_sem.at[d], recv_sem.at[d], py, px) for d, py, px in others]
    for copy in h_sends:
        copy.start()
    recv_buf[me] = send_buf[mine]

    g_copy.wait()
    for j in range(width // 128):
        row = gain_ref[0:1, 128 * j:128 * (j + 1)].astype(F32)
        gain_col[128 * j:128 * (j + 1), :] = jnp.transpose(jnp.broadcast_to(row, (128, 128)))
    w_vmem[qcols:, :] = jnp.zeros((w_vmem.shape[0] - qcols, width), BF16)

    for copy in h_sends:
        copy.wait()

    square = jnp.zeros((8, 128), F32)
    for s in range(total):
        for k in range(half // 8):
            low = recv_buf[s, k].astype(F32)
            high = lane_roll(low, 64)
            h_full[cols * s + 8 * k:cols * s + 8 * (k + 1), :] = low
            h_full[cols * s + half + 8 * k:cols * s + half + 8 * (k + 1), :] = high
            square = square + low * low + high * high
    power = jnp.sum(square, axis=0, keepdims=True)
    inv = lax.rsqrt(power / width + NORM_EPS)
    u_full[...] = (h_full[...] * inv * gain_col[...]).astype(BF16)
    w_copy.wait()
    zt_buf[...] = lax.dot_general(w_vmem[...], u_full[...], NN, preferred_element_type=F32)
    for j in range(zt_buf.shape[0] // 128):
        zj = jnp.transpose(zt_buf[128 * j:128 * (j + 1), :])
        for t in range(ny):
            z_send[t, :, 128 * j:128 * (j + 1)] = zj[rows * t:rows * (t + 1)].astype(BF16)
    z_sends = [remote(z_send.at[py], z_recv.at[y], zsend_sem.at[d], zrecv_sem.at[d], py, px) for d, py, px in ring(y, mine, ny)]
    for copy in z_sends:
        copy.start()
    z_recv[y] = z_send[y]

    for j in range(width // 128):
        h_rows[:, 128 * j:128 * (j + 1)] = jnp.transpose(h_full[128 * j:128 * (j + 1), :])
    hrow_ref[...] = h_rows[pl.ds(pl.multiple_of(y * rows, rows), rows), :]

    for copy in z_sends:
        copy.wait()

    zs = [[z_recv[t, :, 128 * j:128 * (j + 1)].astype(F32) for j in range(w_vmem.shape[0] // 128)] for t in range(ny)]
    for g in range(ny * qcols // 128):
        start = 128 * g
        t = start // qcols
        off = start - t * qcols
        j, sh = off // 128, off % 128
        take = min(128, qcols - off)
        out = lane_roll(zs[t][j], -sh)
        if sh and take > 128 - sh:
            out = jnp.where(lane16 < 128 - sh, out, lane_roll(zs[t][j + 1], -sh))
        if take < 128:
            out = jnp.where(lane16 < take, out, lane_roll(zs[t + 1][0], take))
        z_ref[:, g, :] = out
    for g in range(ny * qcols // 128, z_ref.shape[1]):
        z_ref[:, g, :] = jnp.zeros((rows, 128), F32)
    for copy in kv_copies:
        copy.wait()


def attend_kernel(heads, scale, len_ref, z_ref, k_in, v_in, k_hbm, v_hbm, o_ref, k_ref, v_ref, s_buf, o_acc, k_sem, v_sem):
    rows, slots = k_ref.shape[:2]

    def place(b):
        length = len_ref[b]
        base = pl.multiple_of((length // 16) * 16, 16)
        here = lax.broadcasted_iota(jnp.int32, (16, 128), 0) == length - base
        k_new = jnp.broadcast_to(z_ref[b, heads:heads + 1, :], (16, 128)).astype(BF16)
        v_new = jnp.broadcast_to(z_ref[b, heads + 1:heads + 2, :], (16, 128)).astype(BF16)
        k_ref[b, pl.ds(base, 16), :] = jnp.where(here, k_new, k_ref[b, pl.ds(base, 16), :])
        v_ref[b, pl.ds(base, 16), :] = jnp.where(here, v_new, v_ref[b, pl.ds(base, 16), :])

    def k_copy(b):
        return pltpu.make_async_copy(k_ref.at[b], k_hbm.at[b], k_sem.at[b])

    def v_copy(b):
        return pltpu.make_async_copy(v_ref.at[b], v_hbm.at[b], v_sem.at[b])

    def score(i, slot):
        blank = jnp.zeros((16, 128), BF16)
        q0, q1 = z_ref[2 * i].astype(BF16), z_ref[2 * i + 1].astype(BF16)
        q = jnp.concatenate([jnp.concatenate([q0, blank], axis=1), jnp.concatenate([blank, q1], axis=1)], axis=0)
        keys = jnp.concatenate([k_ref[2 * i], k_ref[2 * i + 1]], axis=1)
        s_buf[slot] = lax.dot_general(q, keys, NT, preferred_element_type=F32) * scale

    def finish(i, slot):
        s = s_buf[slot]
        first = lax.broadcasted_iota(jnp.int32, (32, 1), 0) < 16
        length = jnp.where(first, len_ref[2 * i], len_ref[2 * i + 1])
        s = jnp.where(lane_ids(s.shape) <= length, s, -1e30)
        e = jnp.exp(s - jnp.max(s, axis=1, keepdims=True))
        p = (e * (1.0 / jnp.sum(e, axis=1, keepdims=True))).astype(BF16)
        values = jnp.concatenate([v_ref[2 * i], v_ref[2 * i + 1]], axis=1)
        o = lax.dot_general(p, values, NN, preferred_element_type=F32)
        o_acc[2 * i] = o[0:16, 0:128]
        o_acc[2 * i + 1] = o[16:32, 128:256]

    for b in range(rows + 1):
        if b < rows:
            place(b)
        if b > 0:
            k_copy(b - 1).start()
            v_copy(b - 1).start()
    score(0, 0)
    for i in range(rows // 2 - 1):
        score(i + 1, (i + 1) % 2)
        finish(i, i % 2)
    finish(rows // 2 - 1, (rows // 2 - 1) % 2)
    for h in range(heads):
        o_ref[h] = o_acc[:, h, :].astype(BF16)

    def drain(b, carry):
        k_copy(b).wait()
        v_copy(b).wait()
        return carry

    lax.fori_loop(0, rows, drain, 0)


def proj_kernel(ny, nx, cols, rows, width, heads, o_ref, hrow_ref, gain_hbm, wo_hbm, wgu_hbm, wd_hbm,
                u_ref, tail_ref, wgu_ref, wd_ref,
                gain_ref, wo, o_recv, p_send, p_recv, hm_send, hm_recv, hm_rows, hm_cols,
                gain_sem, wo_sem, wgu_sem, wd_sem, os_sem, or_sem, ps_sem, pr_sem, hs_sem, hr_sem):
    y, x = lax.axis_index('yz'), lax.axis_index('x')
    total = ny * nx
    heads_y = heads // ny
    many = ny * rows
    ffn = wd_hbm.shape[0]
    group = ring(y, twist(y, x, ny), ny)
    barrier = pltpu.get_barrier_semaphore()
    for _, py, px in group:
        pl.semaphore_signal(barrier, inc=1, device_id={'yz': py, 'x': px}, device_id_type=MESH)
    wo_copy = pltpu.make_async_copy(wo_hbm, wo, wo_sem)
    gain_copy = pltpu.make_async_copy(gain_hbm, gain_ref, gain_sem)
    parts = wgu_sem.shape[0]
    share = ffn // parts
    loads = [pltpu.make_async_copy(wgu_hbm.at[:, pl.ds(c * share, share)], wgu_ref.at[:, pl.ds(c * share, share)], wgu_sem.at[c])
             for c in range(parts)]
    loads.append(pltpu.make_async_copy(wd_hbm, wd_ref.at[pl.ds(0, ffn)], wd_sem))
    for copy in [wo_copy, gain_copy] + loads:
        copy.start()
    pl.semaphore_wait(barrier, ny - 1)

    o_sends = [remote(o_ref.at[pl.ds(py * heads_y, heads_y)], o_recv.at[y], os_sem.at[d], or_sem.at[d], py, px) for d, py, px in group]
    for copy in o_sends:
        copy.start()
    o_recv[y] = o_ref[pl.ds(y * heads_y, heads_y)]
    wd_ref[ffn:, :] = jnp.zeros((wd_ref.shape[0] - ffn, width), BF16)
    wo_copy.wait()
    for copy in o_sends:
        copy.wait()
    o_rows = [jnp.concatenate([o_recv[t, h] for t in range(ny)], axis=0) for h in range(heads_y)]
    o_full = jnp.concatenate(o_rows, axis=1)

    halves = ps_sem.shape[0]
    wide = width // halves

    def p_copies(c):
        at = pl.ds(c * wide, wide)
        return [remote(p_send.at[py, :, at], p_recv.at[y, :, at], ps_sem.at[c, d], pr_sem.at[c, d], py, px) for d, py, px in group]

    def h_copies(c):
        at = pl.ds(c * wide, wide)
        return [remote(hm_send.at[:, at], hm_recv.at[y, :, at], hs_sem.at[c, d], hr_sem.at[c, d], py, px) for d, py, px in group]

    for c in range(halves):
        at = slice(c * wide, (c + 1) * wide)
        part = lax.dot_general(o_full, wo[:, at], NN, preferred_element_type=F32).astype(BF16)
        for t in range(ny):
            p_send[t, :, at] = part[rows * t:rows * (t + 1)]
        for copy in p_copies(c):
            copy.start()
        p_recv[y, :, at] = p_send[y, :, at]
    for c in range(halves):
        at = slice(c * wide, (c + 1) * wide)
        for copy in p_copies(c):
            copy.wait()
        summed = p_recv[0, :, at].astype(F32)
        for t in range(1, ny):
            summed = summed + p_recv[t, :, at].astype(F32)
        hm_send[:, at] = (hrow_ref[:, at] + summed).astype(BF16)
        for copy in h_copies(c):
            copy.start()
    h_mid = hm_send[...]
    hm_recv[y] = h_mid

    hm_rows[0:rows, :] = h_mid.astype(F32)
    hm_rows[rows:, :] = jnp.zeros((hm_rows.shape[0] - rows, width), F32)
    for j in range(width // 128):
        hm_cols[128 * j:128 * (j + 1), :] = jnp.transpose(hm_rows[:, 128 * j:128 * (j + 1)])
    for s in range(total):
        corner = jnp.zeros((16, 128), F32)
        for k in range(cols // 16):
            corner = corner + lane_roll(hm_cols[cols * s + 16 * k:cols * s + 16 * (k + 1), :], 64 + 16 * k)
        tail_ref[s] = corner
    u_ref[many:, :] = jnp.zeros((u_ref.shape[0] - many, width), BF16)

    gain_copy.wait()
    for c in range(halves):
        for copy in h_copies(c):
            copy.wait()
    h64 = jnp.concatenate([hm_recv[t] for t in range(ny)], axis=0).astype(F32)
    inv = lax.rsqrt(jnp.sum(h64 * h64, axis=1, keepdims=True) / width + NORM_EPS)
    u_ref[0:many, :] = (h64 * inv * gain_ref[...].astype(F32)).astype(BF16)
    for copy in loads:
        copy.wait()


def mlp_kernel(ny, nx, cols, rows, width, ffn, u_ref, tail_ref, wgu, wd, out_ref, m_rows, f_part, f_cols, f_send, f_recv, fs_sem, fr_sem):
    y, x = lax.axis_index('yz'), lax.axis_index('x')
    total = ny * nx
    me = x * ny + y
    slot = y * nx + x
    many = ny * rows
    barrier = greet_all(peers(y, x, ny, nx))
    lane16 = lane_ids((16, 128))

    for base in range(0, ffn, 512):
        size = min(512, ffn - base)
        gate = lax.dot_general(wgu[0, base:base + size, :], u_ref[...], NT, preferred_element_type=F32)
        up = lax.dot_general(wgu[1, base:base + size, :], u_ref[...], NT, preferred_element_type=F32)
        gate = gate.astype(BF16).astype(F32)
        m = jax.nn.silu(gate) * up.astype(BF16).astype(F32)
        if size % 128:
            m = jnp.concatenate([m, jnp.zeros((128 - size % 128, 128), F32)], axis=0)
        for j in range(m.shape[0] // 128):
            m_rows[:, base + 128 * j:base + 128 * (j + 1)] = jnp.transpose(m[128 * j:128 * (j + 1)])[0:many].astype(BF16)

    chunks = f_part.shape[0]
    wide = width // chunks
    group = total // chunks
    span = nx // chunks
    own = (x % span) * ny + y
    f_part[:, many:, :] = jnp.zeros((chunks, f_part.shape[1] - many, wide), F32)
    pl.semaphore_wait(barrier, total - 1)
    f_sends = []
    for i in range(chunks):
        c = (x // span + 1 + i) % chunks
        at = pl.ds(pl.multiple_of(c * wide, wide), wide)
        f_part[i, 0:many, :] = lax.dot_general(m_rows[...], wd[:, at], NN, preferred_element_type=F32)
        for j in range(wide // 128):
            f_cols[i, 128 * j:128 * (j + 1), :] = jnp.transpose(f_part[i, :, 128 * j:128 * (j + 1)])
        for s in range(group):
            a0 = f_cols[i, cols * s:cols * s + 16, :]
            a1 = f_cols[i, cols * s + 16:cols * s + 32, :]
            a2 = lane_roll(f_cols[i, cols * s + 32:cols * s + 48, :], 64)
            f_send[c * group + s, 0:16] = jnp.where(lane16 < 64, a0, a2).astype(BF16)
            f_send[c * group + s, 16:32] = jnp.where(lane16 < 64, a1, tail_ref[c * group + s]).astype(BF16)
        for k in range(1 if i == chunks - 1 else 0, group):
            j = (own + k) % group
            s = c * group + j
            f_sends.append(remote(f_send.at[s], f_recv.at[slot], fs_sem.at[s], fr_sem.at[slot], j % ny, c * span + j // ny))
            f_sends[-1].start()
    f_recv[slot] = f_send[me]
    for k in range(1, total):
        s = (slot + k) % total
        remote(f_send.at[s], f_recv.at[s], fs_sem.at[s], fr_sem.at[s], (y + 1) % ny, x).wait_recv()

    sums = [[jnp.zeros((16, 128), F32) for _ in range(3)] for _ in range(ny)]
    olds = [[jnp.zeros((16, 128), F32) for _ in range(3)] for _ in range(ny)]
    for g in range(nx):
        members = [twist(t, g, ny) for t in range(ny)]
        low = f_recv[members[0], 0:16].astype(F32)
        for t in range(1, ny):
            low = low + f_recv[t * nx + members[t], 0:16].astype(F32)
        corner = [f_recv[t * nx + members[t], 16:32].astype(F32) for t in range(ny)]
        mid = corner[0]
        for t in range(1, ny):
            mid = mid + corner[t]
        high = lane_roll(low, 64)
        for t in range(ny):
            at = rows * members[t]
            here = (lane16 >= at) & (lane16 < at + rows)
            for k, v in enumerate((low, mid, high)):
                sums[t][k] = jnp.where(here, lane_roll(v, at - rows * t), sums[t][k])
                olds[t][k] = jnp.where(here, lane_roll(corner[t], at - 64 - 16 * k), olds[t][k])
    for t in range(ny):
        for k in range(3):
            out_ref[16 * k:16 * (k + 1), 128 * t:128 * (t + 1)] = (olds[t][k] + sums[t][k]).astype(BF16)
    for copy in f_sends:
        copy.wait_send()


def solution(mesh):
    group_axes = ('yz', 'x')
    batch_axes = ('replica', 'yz', 'x')
    hidden_spec = P('replica', ('x', 'yz'))
    cache_spec = P(None, batch_axes, None, None)
    ny, nx = mesh.shape['yz'], mesh.shape['x']
    vmem = pl.BlockSpec(memory_space=pltpu.VMEM)
    hbm = pl.BlockSpec(memory_space=pl.ANY)
    dma = pltpu.SemaphoreType.DMA

    def layer(ht, seq_lens, attn_gain, mlp_gain, w_qkv, w_out, w_gate_up, w_down, k_cache, v_cache):
        cols = ht.shape[0]
        rows, slots, head_dim = k_cache.shape
        width = attn_gain.shape[1]
        qcols = w_qkv.shape[0]
        qpad = -(-qcols // 128) * 128
        heads = (qcols * ny) // head_dim - 2
        total = ny * nx
        many = ny * rows
        ffn = w_down.shape[0]
        ffn_pad = -(-ffn // 128) * 128
        in_hbm = functools.partial(pltpu.with_memory_space_constraint, memory_space=pltpu.HBM)
        parts = 4
        z, hrow, k_vmem, v_vmem = pl.pallas_call(
            functools.partial(qkv_kernel, ny, nx, cols, rows, width),
            out_shape=(jax.ShapeDtypeStruct((rows, 16, head_dim), F32), jax.ShapeDtypeStruct((rows, width), F32),
                       pltpu.VMEM(k_cache.shape, BF16), pltpu.VMEM(v_cache.shape, BF16)),
            in_specs=[hbm] * 5,
            out_specs=(vmem,) * 4,
            scratch_shapes=[
                pltpu.VMEM(ht.shape, BF16), pltpu.VMEM(attn_gain.shape, BF16),
                pltpu.VMEM((nx, cols // 16, 8, 128), BF16), pltpu.VMEM((total, cols // 16, 8, 128), BF16), pltpu.VMEM((qpad, width), BF16),
                pltpu.VMEM((width, 128), F32), pltpu.VMEM((width, 128), F32), pltpu.VMEM((width, 128), BF16),
                pltpu.VMEM((qpad, 128), F32), pltpu.VMEM((ny, rows, qpad), BF16), pltpu.VMEM((ny, rows, qpad), BF16),
                pltpu.VMEM((128, width), F32),
                dma, dma, dma, dma((2, parts)), dma((total,)), dma((total,)), dma((ny,)), dma((ny,))],
            compiler_params=pltpu.CompilerParams(collective_id=0, has_side_effects=True, vmem_limit_bytes=12 << 20),
            cost_estimate=pl.CostEstimate(flops=8_000_000_000, bytes_accessed=20_000_000, transcendentals=0),
            name='qkv',
        )(in_hbm(ht), in_hbm(attn_gain), in_hbm(w_qkv), in_hbm(k_cache), in_hbm(v_cache))
        k_new, v_new, o, _, _ = pl.pallas_call(
            functools.partial(attend_kernel, heads, head_dim ** -0.5),
            out_shape=(pltpu.HBM(k_cache.shape, BF16), pltpu.HBM(v_cache.shape, BF16),
                       jax.ShapeDtypeStruct((heads, rows, head_dim), BF16),
                       pltpu.VMEM(k_cache.shape, BF16), pltpu.VMEM(v_cache.shape, BF16)),
            in_specs=[pl.BlockSpec(memory_space=pltpu.SMEM), vmem, vmem, vmem],
            out_specs=(hbm, hbm, vmem, vmem, vmem),
            input_output_aliases={2: 3, 3: 4},
            scratch_shapes=[pltpu.VMEM((2, 32, slots), F32), pltpu.VMEM((rows, 16, head_dim), F32), dma((rows,)), dma((rows,))],
            compiler_params=pltpu.CompilerParams(vmem_limit_bytes=8 << 20),
            cost_estimate=pl.CostEstimate(flops=8_000_000_000, bytes_accessed=20_000_000, transcendentals=0),
            name='attend',
        )(seq_lens, z, k_vmem, v_vmem)
        u, tail, wgu_vmem, wd_vmem = pl.pallas_call(
            functools.partial(proj_kernel, ny, nx, cols, rows, width, heads),
            out_shape=(pltpu.VMEM((128, width), BF16), pltpu.VMEM((total, 16, 128), F32),
                       pltpu.VMEM(w_gate_up.shape, BF16), pltpu.VMEM((ffn_pad, width), BF16)),
            in_specs=[vmem, vmem, hbm, hbm, hbm, hbm],
            out_specs=(vmem,) * 4,
            scratch_shapes=[
                pltpu.VMEM(mlp_gain.shape, BF16), pltpu.VMEM(w_out.shape, BF16),
                pltpu.VMEM((ny, heads // ny, rows, head_dim), BF16),
                pltpu.VMEM((ny, rows, width), BF16), pltpu.VMEM((ny, rows, width), BF16),
                pltpu.VMEM((rows, width), BF16), pltpu.VMEM((ny, rows, width), BF16),
                pltpu.VMEM((128, width), F32), pltpu.VMEM((width, 128), F32),
                dma, dma, dma((5,)), dma, dma((ny,)), dma((ny,)),
                dma((2, ny)), dma((2, ny)), dma((2, ny)), dma((2, ny))],
            compiler_params=pltpu.CompilerParams(collective_id=1, has_side_effects=True, vmem_limit_bytes=12 << 20),
            cost_estimate=pl.CostEstimate(flops=8_000_000_000, bytes_accessed=20_000_000, transcendentals=0),
            name='proj',
        )(o, hrow, in_hbm(mlp_gain), in_hbm(w_out), in_hbm(w_gate_up), in_hbm(w_down))
        out = pl.pallas_call(
            functools.partial(mlp_kernel, ny, nx, cols, rows, width, ffn),
            out_shape=jax.ShapeDtypeStruct(ht.shape, BF16),
            in_specs=[vmem] * 4,
            out_specs=vmem,
            scratch_shapes=[
                pltpu.VMEM((many, ffn_pad), BF16), pltpu.VMEM((2, 128, width // 2), F32), pltpu.VMEM((2, width // 2, 128), F32),
                pltpu.VMEM((total, 32, 128), BF16), pltpu.VMEM((total, 32, 128), BF16), dma((total,)), dma((total,))],
            compiler_params=pltpu.CompilerParams(collective_id=2, has_side_effects=True, vmem_limit_bytes=12 << 20),
            cost_estimate=pl.CostEstimate(flops=8_000_000_000, bytes_accessed=20_000_000, transcendentals=0),
            name='mlp',
        )(u, tail, wgu_vmem, wd_vmem)
        return out, k_new, v_new

    def local_step(hidden, seq_lens, attn_gain, mlp_gain, w_qkv, w_out, w_gate_up, w_down, k_cache, v_cache):
        ht = hidden.T
        k_layers = []
        v_layers = []
        for i in range(w_qkv.shape[0]):
            ht, k_new, v_new = layer(ht, seq_lens, attn_gain[i:i + 1], mlp_gain[i:i + 1], w_qkv[i].T, w_out[i],
                                     jnp.transpose(w_gate_up[i], (1, 2, 0)), w_down[i], k_cache[i], v_cache[i])
            k_layers.append(k_new)
            v_layers.append(v_new)
        return ht.T, jnp.stack(k_layers), jnp.stack(v_layers)

    return jax.shard_map(
        local_step,
        mesh=mesh,
        in_specs=(hidden_spec, P(batch_axes), P(None, None), P(None, None), P(None, None, 'yz'), P(None, 'yz', None),
                  P(None, None, None, 'yz'), P(None, 'yz', None), cache_spec, cache_spec),
        out_specs=(hidden_spec, cache_spec, cache_spec),
        check_vma=False)
```

```python
import functools

import jax
import jax.numpy as jnp
from jax import lax
from jax.experimental import pallas as pl
from jax.experimental.pallas import tpu as pltpu
from jax.sharding import PartitionSpec as P

NORM_EPS = 1e-5
MESH = pl.DeviceIdType.MESH
F32 = jnp.float32
BF16 = jnp.bfloat16
NT = (((1,), (1,)), ((), ()))
NN = (((1,), (0,)), ((), ()))


def lane_ids(shape):
    return lax.broadcasted_iota(jnp.int32, shape, len(shape) - 1)


def lane_roll(v, shift):
    shift = shift % v.shape[-1]
    return v if shift == 0 else pltpu.roll(v, shift, v.ndim - 1)


def twist(t, g, ny):
    flip = (t // (ny // 2)) % 2
    return g + flip * (1 - 2 * (g % 2))


def peers(y, x, ny, nx):
    ys = [(y + d) % ny for d in range(ny)]
    xs = [(x + d) % nx for d in range(nx)]
    far_y = sorted(range(ny), key=lambda d: -min(d, ny - d))
    far_x = sorted(range(nx), key=lambda d: -min(d, nx - d))
    return [(dy * nx + dx, ys[dy], xs[dx]) for dx in far_x for dy in far_y if dy or dx]


def ring(y, g, ny):
    far = sorted(range(1, ny), key=lambda d: -min(d, ny - d))
    return [(d, (y + d) % ny, twist((y + d) % ny, g, ny)) for d in far]


def greet_all(others):
    barrier = pltpu.get_barrier_semaphore()
    for _, py, px in others:
        pl.semaphore_signal(barrier, inc=1, device_id={'yz': py, 'x': px}, device_id_type=MESH)
    return barrier


def remote(src, dst, send_sem, recv_sem, py, px):
    return pltpu.make_async_remote_copy(src_ref=src, dst_ref=dst, send_sem=send_sem, recv_sem=recv_sem,
                                        device_id={'yz': py, 'x': px}, device_id_type=MESH)


def qkv_kernel(ny, nx, cols, rows, width, ht_hbm, gain_hbm, w_hbm, k_hbm, v_hbm, z_ref, hrow_ref, k_ref, v_ref,
               ht_ref, gain_ref, send_buf, recv_buf, w_vmem, gain_col, h_full, u_full, zt_buf, z_send, z_recv, h_rows,
               h_sem, g_sem, w_sem, kv_sem, send_sem, recv_sem, zsend_sem, zrecv_sem):
    y, x = lax.axis_index('yz'), lax.axis_index('x')
    mine = twist(y, x, ny)
    total = ny * nx
    me = x * ny + y
    qcols = w_hbm.shape[0]
    h_copy = pltpu.make_async_copy(ht_hbm, ht_ref, h_sem)
    h_copy.start()
    others = peers(y, x, ny, nx)
    barrier = greet_all(others)
    g_copy = pltpu.make_async_copy(gain_hbm, gain_ref, g_sem)
    g_copy.start()
    w_copy = pltpu.make_async_copy(w_hbm, w_vmem.at[pl.ds(0, qcols)], w_sem)
    w_copy.start()
    parts = kv_sem.shape[1]
    share = k_hbm.shape[0] // parts
    kv_copies = [pltpu.make_async_copy(src.at[pl.ds(i * share, share)], dst.at[pl.ds(i * share, share)], kv_sem.at[c, i])
                 for i in range(parts) for c, (src, dst) in enumerate(((k_hbm, k_ref), (v_hbm, v_ref)))]
    for copy in kv_copies:
        copy.start()
    h_copy.wait()

    lane = lane_ids((cols, 128))
    lane16 = lane_ids((16, 128))
    half = cols // 2
    tiles = [ht_ref[:, 128 * t:128 * (t + 1)].astype(F32) for t in range(ny)]
    for g in range(nx):
        block = jnp.zeros((cols, 128), F32)
        for t in range(ny):
            piece = lane_roll(tiles[t], rows * t - rows * twist(t, g, ny))
            block = jnp.where((lane >= rows * t) & (lane < rows * (t + 1)), piece, block)
        block = jnp.where(lane[0:half] < 64, block[0:half], lane_roll(block[half:cols], 64))
        for k in range(half // 8):
            send_buf[g, k] = block[8 * k:8 * (k + 1)].astype(BF16)

    pl.semaphore_wait(barrier, total - 1)

    h_sends = [remote(send_buf.at[twist(py, px, ny)], recv_buf.at[me], send_sem.at[d], recv_sem.at[d], py, px) for d, py, px in others]
    for copy in h_sends:
        copy.start()
    recv_buf[me] = send_buf[mine]

    g_copy.wait()
    for j in range(width // 128):
        row = gain_ref[0:1, 128 * j:128 * (j + 1)].astype(F32)
        gain_col[128 * j:128 * (j + 1), :] = jnp.transpose(jnp.broadcast_to(row, (128, 128)))
    w_vmem[qcols:, :] = jnp.zeros((w_vmem.shape[0] - qcols, width), BF16)

    for copy in h_sends:
        copy.wait()

    square = jnp.zeros((8, 128), F32)
    for s in range(total):
        for k in range(half // 8):
            low = recv_buf[s, k].astype(F32)
            high = lane_roll(low, 64)
            h_full[cols * s + 8 * k:cols * s + 8 * (k + 1), :] = low
            h_full[cols * s + half + 8 * k:cols * s + half + 8 * (k + 1), :] = high
            square = square + low * low + high * high
    power = jnp.sum(square, axis=0, keepdims=True)
    inv = lax.rsqrt(power / width + NORM_EPS)
    u_full[...] = (h_full[...] * inv * gain_col[...]).astype(BF16)
    w_copy.wait()
    zt_buf[...] = lax.dot_general(w_vmem[...], u_full[...], NN, preferred_element_type=F32)
    for j in range(zt_buf.shape[0] // 128):
        zj = jnp.transpose(zt_buf[128 * j:128 * (j + 1), :])
        for t in range(ny):
            z_send[t, :, 128 * j:128 * (j + 1)] = zj[rows * t:rows * (t + 1)].astype(BF16)
    z_sends = [remote(z_send.at[py], z_recv.at[y], zsend_sem.at[d], zrecv_sem.at[d], py, px) for d, py, px in ring(y, mine, ny)]
    for copy in z_sends:
        copy.start()
    z_recv[y] = z_send[y]

    for j in range(width // 128):
        h_rows[:, 128 * j:128 * (j + 1)] = jnp.transpose(h_full[128 * j:128 * (j + 1), :])
    hrow_ref[...] = h_rows[pl.ds(pl.multiple_of(y * rows, rows), rows), :]

    for copy in z_sends:
        copy.wait()

    z_ref[...] = z_recv[...]
    for copy in kv_copies:
        copy.wait()


def attend_kernel(heads, qcols, scale, len_ref, z_recv, k_in, v_in, k_hbm, v_hbm, o_ref, k_ref, v_ref, z_ref, new_rows, s_buf, o_acc, k_sem, v_sem):
    rows, slots = k_ref.shape[:2]
    ny = z_recv.shape[0]
    lane16 = lane_ids((16, 128))

    def column(g):
        t, off = 128 * g // qcols, 128 * g % qcols
        j, sh = off // 128, off % 128
        take = min(128, qcols - off)

        def tile(t, j):
            return z_recv[t, :, 128 * j:128 * (j + 1)].astype(F32)

        out = lane_roll(tile(t, j), -sh)
        if sh and take > 128 - sh:
            out = jnp.where(lane16 < 128 - sh, out, lane_roll(tile(t, j + 1), -sh))
        if take < 128:
            out = jnp.where(lane16 < take, out, lane_roll(tile(t + 1, 0), take))
        return out

    new_rows[0] = column(heads)
    new_rows[1] = column(heads + 1)

    def place(b):
        length = len_ref[b]
        base = pl.multiple_of((length // 16) * 16, 16)
        here = lax.broadcasted_iota(jnp.int32, (16, 128), 0) == length - base
        k_new = jnp.broadcast_to(new_rows[0, pl.ds(b, 1), :], (16, 128)).astype(BF16)
        v_new = jnp.broadcast_to(new_rows[1, pl.ds(b, 1), :], (16, 128)).astype(BF16)
        k_ref[b, pl.ds(base, 16), :] = jnp.where(here, k_new, k_ref[b, pl.ds(base, 16), :])
        v_ref[b, pl.ds(base, 16), :] = jnp.where(here, v_new, v_ref[b, pl.ds(base, 16), :])

    def k_copy(b):
        return pltpu.make_async_copy(k_ref.at[b], k_hbm.at[b], k_sem.at[b])

    def v_copy(b):
        return pltpu.make_async_copy(v_ref.at[b], v_hbm.at[b], v_sem.at[b])

    def score(i, slot):
        blank = jnp.zeros((16, 128), BF16)
        q0, q1 = z_ref[2 * i].astype(BF16), z_ref[2 * i + 1].astype(BF16)
        q = jnp.concatenate([jnp.concatenate([q0, blank], axis=1), jnp.concatenate([blank, q1], axis=1)], axis=0)
        keys = jnp.concatenate([k_ref[2 * i], k_ref[2 * i + 1]], axis=1)
        s_buf[slot] = lax.dot_general(q, keys, NT, preferred_element_type=F32) * scale

    def finish(i, slot):
        s = s_buf[slot]
        first = lax.broadcasted_iota(jnp.int32, (32, 1), 0) < 16
        length = jnp.where(first, len_ref[2 * i], len_ref[2 * i + 1])
        s = jnp.where(lane_ids(s.shape) <= length, s, -1e30)
        e = jnp.exp(s - jnp.max(s, axis=1, keepdims=True))
        p = (e * (1.0 / jnp.sum(e, axis=1, keepdims=True))).astype(BF16)
        values = jnp.concatenate([v_ref[2 * i], v_ref[2 * i + 1]], axis=1)
        o = lax.dot_general(p, values, NN, preferred_element_type=F32)
        o_acc[2 * i] = o[0:16, 0:128]
        o_acc[2 * i + 1] = o[16:32, 128:256]

    def leave(b, carry):
        k_copy(b).start()
        v_copy(b).start()
        return carry

    def enter(i, carry):
        place(2 * i)
        place(2 * i + 1)
        leave(2 * i - 2, 0)
        leave(2 * i - 1, 0)
        return carry

    place(0)
    place(1)
    lax.fori_loop(1, rows // 2, enter, 0)
    lax.fori_loop(rows - 2, rows, leave, 0)
    for h in range(heads):
        z_ref[:, h, :] = column(h)
    for h in range(heads, 16):
        z_ref[:, h, :] = jnp.zeros((rows, 128), F32)
    score(0, 0)
    for i in range(rows // 2 - 1):
        score(i + 1, (i + 1) % 2)
        finish(i, i % 2)
    finish(rows // 2 - 1, (rows // 2 - 1) % 2)
    for h in range(heads):
        o_ref[h] = o_acc[:, h, :].astype(BF16)

    def drain(b, carry):
        k_copy(b).wait()
        v_copy(b).wait()
        return carry

    lax.fori_loop(0, rows, drain, 0)


def proj_kernel(ny, nx, cols, rows, width, heads, o_ref, hrow_ref, gain_hbm, wo_hbm, wgu_hbm, wd_hbm,
                u_ref, tail_ref, wgu_ref, wd_ref,
                gain_ref, wo, o_recv, p_send, p_recv, hm_send, hm_recv, hm_rows, hm_cols,
                gain_sem, wo_sem, wgu_sem, wd_sem, os_sem, or_sem, ps_sem, pr_sem, hs_sem, hr_sem):
    y, x = lax.axis_index('yz'), lax.axis_index('x')
    total = ny * nx
    heads_y = heads // ny
    many = ny * rows
    ffn = wd_hbm.shape[0]
    group = ring(y, twist(y, x, ny), ny)
    barrier = pltpu.get_barrier_semaphore()
    for _, py, px in group:
        pl.semaphore_signal(barrier, inc=1, device_id={'yz': py, 'x': px}, device_id_type=MESH)
    wo_copy = pltpu.make_async_copy(wo_hbm, wo, wo_sem)
    gain_copy = pltpu.make_async_copy(gain_hbm, gain_ref, gain_sem)
    parts = wgu_sem.shape[0]
    share = ffn // parts
    loads = [pltpu.make_async_copy(wgu_hbm.at[:, pl.ds(c * share, share)], wgu_ref.at[:, pl.ds(c * share, share)], wgu_sem.at[c])
             for c in range(parts)]
    loads.append(pltpu.make_async_copy(wd_hbm, wd_ref.at[pl.ds(0, ffn)], wd_sem))
    for copy in [wo_copy, gain_copy] + loads:
        copy.start()
    pl.semaphore_wait(barrier, ny - 1)

    o_sends = [remote(o_ref.at[pl.ds(py * heads_y, heads_y)], o_recv.at[y], os_sem.at[d], or_sem.at[d], py, px) for d, py, px in group]
    for copy in o_sends:
        copy.start()
    o_recv[y] = o_ref[pl.ds(y * heads_y, heads_y)]
    wd_ref[ffn:, :] = jnp.zeros((wd_ref.shape[0] - ffn, width), BF16)
    wo_copy.wait()
    for copy in o_sends:
        copy.wait()
    o_rows = [jnp.concatenate([o_recv[t, h] for t in range(ny)], axis=0) for h in range(heads_y)]
    o_full = jnp.concatenate(o_rows, axis=1)

    halves = ps_sem.shape[0]
    wide = width // halves

    def p_copies(c):
        at = pl.ds(c * wide, wide)
        return [remote(p_send.at[py, :, at], p_recv.at[y, :, at], ps_sem.at[c, d], pr_sem.at[c, d], py, px) for d, py, px in group]

    def h_copies(c):
        at = pl.ds(c * wide, wide)
        return [remote(hm_send.at[:, at], hm_recv.at[y, :, at], hs_sem.at[c, d], hr_sem.at[c, d], py, px) for d, py, px in group]

    for c in range(halves):
        at = slice(c * wide, (c + 1) * wide)
        part = lax.dot_general(o_full, wo[:, at], NN, preferred_element_type=F32).astype(BF16)
        for t in range(ny):
            p_send[t, :, at] = part[rows * t:rows * (t + 1)]
        for copy in p_copies(c):
            copy.start()
        p_recv[y, :, at] = p_send[y, :, at]
    for c in range(halves):
        at = slice(c * wide, (c + 1) * wide)
        for copy in p_copies(c):
            copy.wait()
        summed = p_recv[0, :, at].astype(F32)
        for t in range(1, ny):
            summed = summed + p_recv[t, :, at].astype(F32)
        hm_send[:, at] = (hrow_ref[:, at] + summed).astype(BF16)
        for copy in h_copies(c):
            copy.start()
    h_mid = hm_send[...]
    hm_recv[y] = h_mid

    hm_rows[0:rows, :] = h_mid.astype(F32)
    hm_rows[rows:, :] = jnp.zeros((hm_rows.shape[0] - rows, width), F32)
    for j in range(width // 128):
        hm_cols[128 * j:128 * (j + 1), :] = jnp.transpose(hm_rows[:, 128 * j:128 * (j + 1)])
    for s in range(total):
        corner = jnp.zeros((16, 128), F32)
        for k in range(cols // 16):
            corner = corner + lane_roll(hm_cols[cols * s + 16 * k:cols * s + 16 * (k + 1), :], 64 + 16 * k)
        tail_ref[s] = corner
    u_ref[many:, :] = jnp.zeros((u_ref.shape[0] - many, width), BF16)

    gain_copy.wait()
    for c in range(halves):
        for copy in h_copies(c):
            copy.wait()
    h64 = jnp.concatenate([hm_recv[t] for t in range(ny)], axis=0).astype(F32)
    inv = lax.rsqrt(jnp.sum(h64 * h64, axis=1, keepdims=True) / width + NORM_EPS)
    u_ref[0:many, :] = (h64 * inv * gain_ref[...].astype(F32)).astype(BF16)
    for copy in loads:
        copy.wait()


def mlp_kernel(ny, nx, cols, rows, width, ffn, u_ref, tail_ref, wgu, wd, out_ref, m_rows, f_part, f_cols, f_send, f_recv, fs_sem, fr_sem):
    y, x = lax.axis_index('yz'), lax.axis_index('x')
    total = ny * nx
    me = x * ny + y
    slot = y * nx + x
    many = ny * rows
    barrier = greet_all(peers(y, x, ny, nx))
    lane16 = lane_ids((16, 128))

    for base in range(0, ffn, 512):
        size = min(512, ffn - base)
        gate = lax.dot_general(wgu[0, base:base + size, :], u_ref[...], NT, preferred_element_type=F32)
        up = lax.dot_general(wgu[1, base:base + size, :], u_ref[...], NT, preferred_element_type=F32)
        gate = gate.astype(BF16).astype(F32)
        m = jax.nn.silu(gate) * up.astype(BF16).astype(F32)
        if size % 128:
            m = jnp.concatenate([m, jnp.zeros((128 - size % 128, 128), F32)], axis=0)
        for j in range(m.shape[0] // 128):
            m_rows[:, base + 128 * j:base + 128 * (j + 1)] = jnp.transpose(m[128 * j:128 * (j + 1)])[0:many].astype(BF16)

    chunks = f_cols.shape[0]
    wide = width // chunks
    group = total // chunks
    span = nx // chunks
    f_cols[:, :, many:] = jnp.zeros((chunks, wide, 128 - many), F32)
    pl.semaphore_wait(barrier, total - 1)
    f_sends = []
    def product(i):
        c = (x // span + 1 + i) % chunks
        at = pl.ds(pl.multiple_of(c * wide, wide), wide)
        f_part[i] = lax.dot_general(m_rows[...], wd[:, at], NN, preferred_element_type=F32)

    def pack(i):
        c = (x // span + 1 + i) % chunks
        for j in range(wide // 128):
            f_cols[i, 128 * j:128 * (j + 1), 0:many] = jnp.transpose(f_part[i, :, 128 * j:128 * (j + 1)])
        for s in range(group):
            a0 = f_cols[i, cols * s:cols * s + 16, :]
            a1 = f_cols[i, cols * s + 16:cols * s + 32, :]
            a2 = lane_roll(f_cols[i, cols * s + 32:cols * s + 48, :], 64)
            f_send[c * group + s, 0:16] = jnp.where(lane16 < 64, a0, a2).astype(BF16)
            f_send[c * group + s, 16:32] = jnp.where(lane16 < 64, a1, tail_ref[c * group + s]).astype(BF16)

    product(0)
    for i in range(chunks):
        pack(i)
        if i + 1 < chunks:
            product(i + 1)
        c = (x // span + 1 + i) % chunks
        last = i == chunks - 1
        order = [((x + (2 if last else 0)) // 2 * 2 + p) % span for p in range(2)]
        order += [((x + (0 if last else 2)) // 2 * 2 + p) % span for p in range(2)]
        places = [(px, (y + d) % ny) for px in order for d in (2, 1, 3, 0)]
        if last:
            places = places[:8] + [((x + 1 - 2 * (x % 2)) % span, (y + d) % ny) for d in (2, 1, 3, 0)] + [(x % span, (y + d) % ny) for d in (2, 1, 3)]
        for qx, qy in places:
            j = qx * ny + qy
            s = c * group + j
            f_sends.append(remote(f_send.at[s], f_recv.at[slot], fs_sem.at[s], fr_sem.at[slot], j % ny, c * span + j // ny))
            f_sends[-1].start()
    f_recv[slot] = f_send[me]
    for k in range(1, total):
        s = (slot + k) % total
        remote(f_send.at[s], f_recv.at[s], fs_sem.at[s], fr_sem.at[s], (y + 1) % ny, x).wait_recv()

    sums = [[jnp.zeros((16, 128), F32) for _ in range(3)] for _ in range(ny)]
    olds = [[jnp.zeros((16, 128), F32) for _ in range(3)] for _ in range(ny)]
    for g in range(nx):
        members = [twist(t, g, ny) for t in range(ny)]
        low = f_recv[members[0], 0:16].astype(F32)
        for t in range(1, ny):
            low = low + f_recv[t * nx + members[t], 0:16].astype(F32)
        corner = [f_recv[t * nx + members[t], 16:32].astype(F32) for t in range(ny)]
        mid = corner[0]
        for t in range(1, ny):
            mid = mid + corner[t]
        high = lane_roll(low, 64)
        for t in range(ny):
            at = rows * members[t]
            here = (lane16 >= at) & (lane16 < at + rows)
            for k, v in enumerate((low, mid, high)):
                sums[t][k] = jnp.where(here, lane_roll(v, at - rows * t), sums[t][k])
                olds[t][k] = jnp.where(here, lane_roll(corner[t], at - 64 - 16 * k), olds[t][k])
    for t in range(ny):
        for k in range(3):
            out_ref[16 * k:16 * (k + 1), 128 * t:128 * (t + 1)] = (olds[t][k] + sums[t][k]).astype(BF16)
    for copy in f_sends:
        copy.wait_send()


def solution(mesh):
    group_axes = ('yz', 'x')
    batch_axes = ('replica', 'yz', 'x')
    hidden_spec = P('replica', ('x', 'yz'))
    cache_spec = P(None, batch_axes, None, None)
    ny, nx = mesh.shape['yz'], mesh.shape['x']
    vmem = pl.BlockSpec(memory_space=pltpu.VMEM)
    hbm = pl.BlockSpec(memory_space=pl.ANY)
    dma = pltpu.SemaphoreType.DMA

    def layer(ht, seq_lens, attn_gain, mlp_gain, w_qkv, w_out, w_gate_up, w_down, k_cache, v_cache):
        cols = ht.shape[0]
        rows, slots, head_dim = k_cache.shape
        width = attn_gain.shape[1]
        qcols = w_qkv.shape[0]
        qpad = -(-qcols // 128) * 128
        heads = (qcols * ny) // head_dim - 2
        total = ny * nx
        many = ny * rows
        ffn = w_down.shape[0]
        ffn_pad = -(-ffn // 128) * 128
        in_hbm = functools.partial(pltpu.with_memory_space_constraint, memory_space=pltpu.HBM)
        parts = 4
        z, hrow, k_vmem, v_vmem = pl.pallas_call(
            functools.partial(qkv_kernel, ny, nx, cols, rows, width),
            out_shape=(jax.ShapeDtypeStruct((ny, rows, qpad), BF16), jax.ShapeDtypeStruct((rows, width), F32),
                       pltpu.VMEM(k_cache.shape, BF16), pltpu.VMEM(v_cache.shape, BF16)),
            in_specs=[hbm] * 5,
            out_specs=(vmem,) * 4,
            scratch_shapes=[
                pltpu.VMEM(ht.shape, BF16), pltpu.VMEM(attn_gain.shape, BF16),
                pltpu.VMEM((nx, cols // 16, 8, 128), BF16), pltpu.VMEM((total, cols // 16, 8, 128), BF16), pltpu.VMEM((qpad, width), BF16),
                pltpu.VMEM((width, 128), F32), pltpu.VMEM((width, 128), F32), pltpu.VMEM((width, 128), BF16),
                pltpu.VMEM((qpad, 128), F32), pltpu.VMEM((ny, rows, qpad), BF16), pltpu.VMEM((ny, rows, qpad), BF16),
                pltpu.VMEM((128, width), F32),
                dma, dma, dma, dma((2, parts)), dma((total,)), dma((total,)), dma((ny,)), dma((ny,))],
            compiler_params=pltpu.CompilerParams(collective_id=0, has_side_effects=True, vmem_limit_bytes=12 << 20),
            cost_estimate=pl.CostEstimate(flops=8_000_000_000, bytes_accessed=20_000_000, transcendentals=0),
            name='qkv',
        )(in_hbm(ht), in_hbm(attn_gain), in_hbm(w_qkv), in_hbm(k_cache), in_hbm(v_cache))
        k_new, v_new, o, _, _ = pl.pallas_call(
            functools.partial(attend_kernel, heads, qcols, head_dim ** -0.5),
            out_shape=(pltpu.HBM(k_cache.shape, BF16), pltpu.HBM(v_cache.shape, BF16),
                       jax.ShapeDtypeStruct((heads, rows, head_dim), BF16),
                       pltpu.VMEM(k_cache.shape, BF16), pltpu.VMEM(v_cache.shape, BF16)),
            in_specs=[pl.BlockSpec(memory_space=pltpu.SMEM), vmem, vmem, vmem],
            out_specs=(hbm, hbm, vmem, vmem, vmem),
            input_output_aliases={2: 3, 3: 4},
            scratch_shapes=[pltpu.VMEM((rows, 16, head_dim), F32), pltpu.VMEM((2, rows, head_dim), F32), pltpu.VMEM((2, 32, slots), F32), pltpu.VMEM((rows, 16, head_dim), F32), dma((rows,)), dma((rows,))],
            compiler_params=pltpu.CompilerParams(vmem_limit_bytes=8 << 20),
            cost_estimate=pl.CostEstimate(flops=8_000_000_000, bytes_accessed=20_000_000, transcendentals=0),
            name='attend',
        )(seq_lens, z, k_vmem, v_vmem)
        u, tail, wgu_vmem, wd_vmem = pl.pallas_call(
            functools.partial(proj_kernel, ny, nx, cols, rows, width, heads),
            out_shape=(pltpu.VMEM((128, width), BF16), pltpu.VMEM((total, 16, 128), F32),
                       pltpu.VMEM(w_gate_up.shape, BF16), pltpu.VMEM((ffn_pad, width), BF16)),
            in_specs=[vmem, vmem, hbm, hbm, hbm, hbm],
            out_specs=(vmem,) * 4,
            scratch_shapes=[
                pltpu.VMEM(mlp_gain.shape, BF16), pltpu.VMEM(w_out.shape, BF16),
                pltpu.VMEM((ny, heads // ny, rows, head_dim), BF16),
                pltpu.VMEM((ny, rows, width), BF16), pltpu.VMEM((ny, rows, width), BF16),
                pltpu.VMEM((rows, width), BF16), pltpu.VMEM((ny, rows, width), BF16),
                pltpu.VMEM((128, width), F32), pltpu.VMEM((width, 128), F32),
                dma, dma, dma((5,)), dma, dma((ny,)), dma((ny,)),
                dma((2, ny)), dma((2, ny)), dma((2, ny)), dma((2, ny))],
            compiler_params=pltpu.CompilerParams(collective_id=1, has_side_effects=True, vmem_limit_bytes=12 << 20),
            cost_estimate=pl.CostEstimate(flops=8_000_000_000, bytes_accessed=20_000_000, transcendentals=0),
            name='proj',
        )(o, hrow, in_hbm(mlp_gain), in_hbm(w_out), in_hbm(w_gate_up), in_hbm(w_down))
        out = pl.pallas_call(
            functools.partial(mlp_kernel, ny, nx, cols, rows, width, ffn),
            out_shape=jax.ShapeDtypeStruct(ht.shape, BF16),
            in_specs=[vmem] * 4,
            out_specs=vmem,
            scratch_shapes=[
                pltpu.VMEM((many, ffn_pad), BF16), pltpu.VMEM((2, many, width // 2), F32), pltpu.VMEM((2, width // 2, 128), F32),
                pltpu.VMEM((total, 32, 128), BF16), pltpu.VMEM((total, 32, 128), BF16), dma((total,)), dma((total,))],
            compiler_params=pltpu.CompilerParams(collective_id=2, has_side_effects=True, vmem_limit_bytes=12 << 20),
            cost_estimate=pl.CostEstimate(flops=8_000_000_000, bytes_accessed=20_000_000, transcendentals=0),
            name='mlp',
        )(u, tail, wgu_vmem, wd_vmem)
        return out, k_new, v_new

    def local_step(hidden, seq_lens, attn_gain, mlp_gain, w_qkv, w_out, w_gate_up, w_down, k_cache, v_cache):
        ht = hidden.T
        k_layers = []
        v_layers = []
        for i in range(w_qkv.shape[0]):
            ht, k_new, v_new = layer(ht, seq_lens, attn_gain[i:i + 1], mlp_gain[i:i + 1], w_qkv[i].T, w_out[i],
                                     jnp.transpose(w_gate_up[i], (1, 2, 0)), w_down[i], k_cache[i], v_cache[i])
            k_layers.append(k_new)
            v_layers.append(v_new)
        return ht.T, jnp.stack(k_layers), jnp.stack(v_layers)

    return jax.shard_map(
        local_step,
        mesh=mesh,
        in_specs=(hidden_spec, P(batch_axes), P(None, None), P(None, None), P(None, None, 'yz'), P(None, 'yz', None),
                  P(None, None, None, 'yz'), P(None, 'yz', None), cache_spec, cache_spec),
        out_specs=(hidden_spec, cache_spec, cache_spec),
        check_vma=False)
```

```python
import functools

import jax
import jax.numpy as jnp
from jax import lax
from jax.experimental import pallas as pl
from jax.experimental.pallas import tpu as pltpu
from jax.sharding import PartitionSpec as P

NORM_EPS = 1e-5
MESH = pl.DeviceIdType.MESH
F32 = jnp.float32
BF16 = jnp.bfloat16
NT = (((1,), (1,)), ((), ()))
NN = (((1,), (0,)), ((), ()))


def lane_ids(shape):
    return lax.broadcasted_iota(jnp.int32, shape, len(shape) - 1)


def lane_roll(v, shift):
    shift = shift % v.shape[-1]
    return v if shift == 0 else pltpu.roll(v, shift, v.ndim - 1)


def peers(y, x, ny, nx):
    ys = [(y + d) % ny for d in range(ny)]
    xs = [(x + d) % nx for d in range(nx)]
    far_y = sorted(range(ny), key=lambda d: -min(d, ny - d))
    far_x = sorted(range(nx), key=lambda d: -min(d, nx - d))
    return [(dy * nx + dx, ys[dy], xs[dx]) for dx in far_x for dy in far_y if dy or dx]


def ring(y, x, ny):
    far = sorted(range(1, ny), key=lambda d: -min(d, ny - d))
    return [(d, (y + d) % ny, x) for d in far]


def greet_all(others):
    barrier = pltpu.get_barrier_semaphore()
    for _, py, px in others:
        pl.semaphore_signal(barrier, inc=1, device_id={'yz': py, 'x': px}, device_id_type=MESH)
    return barrier


def remote(src, dst, send_sem, recv_sem, py, px):
    return pltpu.make_async_remote_copy(src_ref=src, dst_ref=dst, send_sem=send_sem, recv_sem=recv_sem,
                                        device_id={'yz': py, 'x': px}, device_id_type=MESH)


def qkv_kernel(ny, nx, cols, rows, width, len_hbm, ht_hbm, gain_hbm, w_hbm, k_hbm, v_hbm, z_ref, hrow_ref, k_ref, v_ref, len_ref,
               ht_ref, gain_ref, send_buf, recv_buf, w_vmem, gain_col, h_full, u_full, zt_buf, z_send, z_recv, h_rows,
               len_sem, h_sem, g_sem, w_sem, kv_sem, send_sem, recv_sem, zsend_sem, zrecv_sem):
    y, x = lax.axis_index('yz'), lax.axis_index('x')
    total = ny * nx
    me = x * ny + y
    qcols = w_hbm.shape[0]
    h_copy = pltpu.make_async_copy(ht_hbm, ht_ref, h_sem)
    h_copy.start()
    others = peers(y, x, ny, nx)
    barrier = greet_all(others)
    g_copy = pltpu.make_async_copy(gain_hbm, gain_ref, g_sem)
    g_copy.start()
    len_copy = pltpu.make_async_copy(len_hbm, len_ref, len_sem)
    len_copy.start()
    w_copy = pltpu.make_async_copy(w_hbm, w_vmem.at[pl.ds(0, qcols)], w_sem)
    w_copy.start()
    parts = kv_sem.shape[1]
    share = k_hbm.shape[0] // parts
    kv_copies = [pltpu.make_async_copy(src.at[pl.ds(i * share, share)], dst.at[pl.ds(i * share, share)], kv_sem.at[c, i])
                 for i in range(parts) for c, (src, dst) in enumerate(((k_hbm, k_ref), (v_hbm, v_ref)))]
    for copy in kv_copies:
        copy.start()
    h_copy.wait()

    lane = lane_ids((cols, 128))
    lane16 = lane_ids((16, 128))
    half = cols // 2
    tiles = [ht_ref[:, 128 * t:128 * (t + 1)].astype(F32) for t in range(ny)]
    for g in range(nx):
        block = jnp.zeros((cols, 128), F32)
        for t in range(ny):
            piece = lane_roll(tiles[t], rows * t - rows * g)
            block = jnp.where((lane >= rows * t) & (lane < rows * (t + 1)), piece, block)
        block = jnp.where(lane[0:half] < 64, block[0:half], lane_roll(block[half:cols], 64))
        for k in range(half // 8):
            send_buf[g, k] = block[8 * k:8 * (k + 1)].astype(BF16)

    pl.semaphore_wait(barrier, total - 1)

    h_sends = [remote(send_buf.at[px], recv_buf.at[me], send_sem.at[d], recv_sem.at[d], py, px) for d, py, px in others]
    for copy in h_sends:
        copy.start()
    recv_buf[me] = send_buf[x]

    g_copy.wait()
    for j in range(width // 128):
        row = gain_ref[0:1, 128 * j:128 * (j + 1)].astype(F32)
        gain_col[128 * j:128 * (j + 1), :] = jnp.transpose(jnp.broadcast_to(row, (128, 128)))
    w_vmem[qcols:, :] = jnp.zeros((w_vmem.shape[0] - qcols, width), BF16)

    for copy in h_sends:
        copy.wait()

    square = jnp.zeros((8, 128), F32)
    for s in range(total):
        for k in range(half // 8):
            low = recv_buf[s, k].astype(F32)
            high = lane_roll(low, 64)
            h_full[cols * s + 8 * k:cols * s + 8 * (k + 1), :] = low
            h_full[cols * s + half + 8 * k:cols * s + half + 8 * (k + 1), :] = high
            square = square + low * low + high * high
    power = jnp.sum(square, axis=0, keepdims=True)
    inv = lax.rsqrt(power / width + NORM_EPS)
    u_full[...] = (h_full[...] * inv * gain_col[...]).astype(BF16)
    w_copy.wait()
    zt_buf[...] = lax.dot_general(w_vmem[...], u_full[...], NN, preferred_element_type=F32)
    for j in range(zt_buf.shape[0] // 128):
        zj = jnp.transpose(zt_buf[128 * j:128 * (j + 1), :])
        for t in range(ny):
            z_send[t, :, 128 * j:128 * (j + 1)] = zj[rows * t:rows * (t + 1)].astype(BF16)
    z_sends = [remote(z_send.at[py], z_recv.at[y], zsend_sem.at[d], zrecv_sem.at[d], py, px) for d, py, px in ring(y, x, ny)]
    for copy in z_sends:
        copy.start()
    z_recv[y] = z_send[y]

    for j in range(width // 128):
        h_rows[:, 128 * j:128 * (j + 1)] = jnp.transpose(h_full[128 * j:128 * (j + 1), :])
    hrow_ref[...] = h_rows[pl.ds(pl.multiple_of(y * rows, rows), rows), :]

    for copy in z_sends:
        copy.wait()

    z_ref[...] = z_recv[...]
    for copy in kv_copies + [len_copy]:
        copy.wait()


def attend_kernel(heads, qcols, scale, len_ref, z_recv, k_in, v_in, k_hbm, v_hbm, o_ref, k_ref, v_ref, z_ref, new_rows, s_buf, o_acc, k_sem, v_sem):
    rows, slots = k_ref.shape[:2]
    ny = z_recv.shape[0]
    lane16 = lane_ids((16, 128))

    def column(g):
        t, off = 128 * g // qcols, 128 * g % qcols
        j, sh = off // 128, off % 128
        take = min(128, qcols - off)

        def tile(t, j):
            return z_recv[t, :, 128 * j:128 * (j + 1)].astype(F32)

        out = lane_roll(tile(t, j), -sh)
        if sh and take > 128 - sh:
            out = jnp.where(lane16 < 128 - sh, out, lane_roll(tile(t, j + 1), -sh))
        if take < 128:
            out = jnp.where(lane16 < take, out, lane_roll(tile(t + 1, 0), take))
        return out

    new_rows[0] = column(heads)
    new_rows[1] = column(heads + 1)

    def place(b):
        length = len_ref[b]
        base = pl.multiple_of((length // 16) * 16, 16)
        here = lax.broadcasted_iota(jnp.int32, (16, 128), 0) == length - base
        k_new = jnp.broadcast_to(new_rows[0, pl.ds(b, 1), :], (16, 128)).astype(BF16)
        v_new = jnp.broadcast_to(new_rows[1, pl.ds(b, 1), :], (16, 128)).astype(BF16)
        k_ref[b, pl.ds(base, 16), :] = jnp.where(here, k_new, k_ref[b, pl.ds(base, 16), :])
        v_ref[b, pl.ds(base, 16), :] = jnp.where(here, v_new, v_ref[b, pl.ds(base, 16), :])

    def k_copy(b):
        return pltpu.make_async_copy(k_ref.at[b], k_hbm.at[b], k_sem.at[b])

    def v_copy(b):
        return pltpu.make_async_copy(v_ref.at[b], v_hbm.at[b], v_sem.at[b])

    def score(i, slot):
        blank = jnp.zeros((16, 128), BF16)
        q0, q1 = z_ref[2 * i].astype(BF16), z_ref[2 * i + 1].astype(BF16)
        q = jnp.concatenate([jnp.concatenate([q0, blank], axis=1), jnp.concatenate([blank, q1], axis=1)], axis=0)
        keys = jnp.concatenate([k_ref[2 * i], k_ref[2 * i + 1]], axis=1)
        s_buf[slot] = lax.dot_general(q, keys, NT, preferred_element_type=F32) * scale

    def finish(i, slot):
        s = s_buf[slot]
        first = lax.broadcasted_iota(jnp.int32, (32, 1), 0) < 16
        length = jnp.where(first, len_ref[2 * i], len_ref[2 * i + 1])
        s = jnp.where(lane_ids(s.shape) <= length, s, -1e30)
        e = jnp.exp(s - jnp.max(s, axis=1, keepdims=True))
        p = (e * (1.0 / jnp.sum(e, axis=1, keepdims=True))).astype(BF16)
        values = jnp.concatenate([v_ref[2 * i], v_ref[2 * i + 1]], axis=1)
        o = lax.dot_general(p, values, NN, preferred_element_type=F32)
        o_acc[2 * i] = o[0:16, 0:128]
        o_acc[2 * i + 1] = o[16:32, 128:256]

    def leave(b, carry):
        k_copy(b).start()
        v_copy(b).start()
        return carry

    def enter(i, carry):
        place(2 * i)
        place(2 * i + 1)
        leave(2 * i - 2, 0)
        leave(2 * i - 1, 0)
        return carry

    place(0)
    place(1)
    lax.fori_loop(1, rows // 2, enter, 0)
    lax.fori_loop(rows - 2, rows, leave, 0)
    for h in range(heads):
        z_ref[:, h, :] = column(h)
    for h in range(heads, 16):
        z_ref[:, h, :] = jnp.zeros((rows, 128), F32)
    score(0, 0)
    for i in range(rows // 2 - 1):
        score(i + 1, (i + 1) % 2)
        finish(i, i % 2)
    finish(rows // 2 - 1, (rows // 2 - 1) % 2)
    for h in range(heads):
        o_ref[h] = o_acc[:, h, :].astype(BF16)

    def drain(b, carry):
        k_copy(b).wait()
        v_copy(b).wait()
        return carry

    lax.fori_loop(0, rows, drain, 0)


def proj_kernel(ny, nx, cols, rows, width, heads, o_ref, hrow_ref, gain_hbm, wo_hbm, wgu_hbm, wd_hbm,
                u_ref, tail_ref, wgu_ref, wd_ref,
                gain_ref, wo, o_recv, p_send, p_recv, hm_send, hm_recv, hm_rows, hm_cols,
                gain_sem, wo_sem, wgu_sem, wd_sem, os_sem, or_sem, ps_sem, pr_sem, hs_sem, hr_sem):
    y, x = lax.axis_index('yz'), lax.axis_index('x')
    total = ny * nx
    heads_y = heads // ny
    many = ny * rows
    ffn = wd_hbm.shape[0]
    group = ring(y, x, ny)
    barrier = pltpu.get_barrier_semaphore()
    for _, py, px in group:
        pl.semaphore_signal(barrier, inc=1, device_id={'yz': py, 'x': px}, device_id_type=MESH)
    wo_copy = pltpu.make_async_copy(wo_hbm, wo, wo_sem)
    gain_copy = pltpu.make_async_copy(gain_hbm, gain_ref, gain_sem)
    parts = wgu_sem.shape[0]
    share = ffn // parts
    loads = [pltpu.make_async_copy(wgu_hbm.at[:, pl.ds(c * share, share)], wgu_ref.at[:, pl.ds(c * share, share)], wgu_sem.at[c])
             for c in range(parts)]
    loads.append(pltpu.make_async_copy(wd_hbm, wd_ref.at[pl.ds(0, ffn)], wd_sem))
    for copy in [wo_copy, gain_copy] + loads:
        copy.start()
    pl.semaphore_wait(barrier, ny - 1)

    o_sends = [remote(o_ref.at[pl.ds(py * heads_y, heads_y)], o_recv.at[y], os_sem.at[d], or_sem.at[d], py, px) for d, py, px in group]
    for copy in o_sends:
        copy.start()
    o_recv[y] = o_ref[pl.ds(y * heads_y, heads_y)]
    wd_ref[ffn:, :] = jnp.zeros((wd_ref.shape[0] - ffn, width), BF16)
    wo_copy.wait()
    for copy in o_sends:
        copy.wait()
    o_rows = [jnp.concatenate([o_recv[t, h] for t in range(ny)], axis=0) for h in range(heads_y)]
    o_full = jnp.concatenate(o_rows, axis=1)

    halves = ps_sem.shape[0]
    wide = width // halves

    def p_copies(c):
        at = pl.ds(c * wide, wide)
        return [remote(p_send.at[py, :, at], p_recv.at[y, :, at], ps_sem.at[c, d], pr_sem.at[c, d], py, px) for d, py, px in group]

    def h_copies(c):
        at = pl.ds(c * wide, wide)
        return [remote(hm_send.at[:, at], hm_recv.at[y, :, at], hs_sem.at[c, d], hr_sem.at[c, d], py, px) for d, py, px in group]

    for c in range(halves):
        at = slice(c * wide, (c + 1) * wide)
        part = lax.dot_general(o_full, wo[:, at], NN, preferred_element_type=F32).astype(BF16)
        for t in range(ny):
            p_send[t, :, at] = part[rows * t:rows * (t + 1)]
        for copy in p_copies(c):
            copy.start()
        p_recv[y, :, at] = p_send[y, :, at]
    for c in range(halves):
        at = slice(c * wide, (c + 1) * wide)
        for copy in p_copies(c):
            copy.wait()
        summed = p_recv[0, :, at].astype(F32)
        for t in range(1, ny):
            summed = summed + p_recv[t, :, at].astype(F32)
        hm_send[:, at] = (hrow_ref[:, at] + summed).astype(BF16)
        for copy in h_copies(c):
            copy.start()
    h_mid = hm_send[...]
    hm_recv[y] = h_mid

    hm_rows[0:rows, :] = h_mid.astype(F32)
    hm_rows[rows:, :] = jnp.zeros((hm_rows.shape[0] - rows, width), F32)
    for j in range(width // 128):
        hm_cols[128 * j:128 * (j + 1), :] = jnp.transpose(hm_rows[:, 128 * j:128 * (j + 1)])
    for s in range(total):
        corner = jnp.zeros((16, 128), F32)
        for k in range(cols // 16):
            corner = corner + lane_roll(hm_cols[cols * s + 16 * k:cols * s + 16 * (k + 1), :], 64 + 16 * k)
        tail_ref[s] = corner
    u_ref[many:, :] = jnp.zeros((u_ref.shape[0] - many, width), BF16)

    gain_copy.wait()
    for c in range(halves):
        for copy in h_copies(c):
            copy.wait()
    h64 = jnp.concatenate([hm_recv[t] for t in range(ny)], axis=0).astype(F32)
    inv = lax.rsqrt(jnp.sum(h64 * h64, axis=1, keepdims=True) / width + NORM_EPS)
    u_ref[0:many, :] = (h64 * inv * gain_ref[...].astype(F32)).astype(BF16)
    for copy in loads:
        copy.wait()


def mlp_kernel(ny, nx, cols, rows, width, ffn, u_ref, tail_ref, wgu, wd, out_ref, m_rows, f_part, f_cols, f_send, f_recv, fs_sem, fr_sem):
    y, x = lax.axis_index('yz'), lax.axis_index('x')
    total = ny * nx
    me = x * ny + y
    slot = y * nx + x
    many = ny * rows
    barrier = greet_all(peers(y, x, ny, nx))
    lane16 = lane_ids((16, 128))

    for base in range(0, ffn, 512):
        size = min(512, ffn - base)
        gate = lax.dot_general(wgu[0, base:base + size, :], u_ref[...], NT, preferred_element_type=F32)
        up = lax.dot_general(wgu[1, base:base + size, :], u_ref[...], NT, preferred_element_type=F32)
        gate = gate.astype(BF16).astype(F32)
        m = jax.nn.silu(gate) * up.astype(BF16).astype(F32)
        if size % 128:
            m = jnp.concatenate([m, jnp.zeros((128 - size % 128, 128), F32)], axis=0)
        for j in range(m.shape[0] // 128):
            m_rows[:, base + 128 * j:base + 128 * (j + 1)] = jnp.transpose(m[128 * j:128 * (j + 1)])[0:many].astype(BF16)

    chunks = f_cols.shape[0]
    wide = width // chunks
    group = total // chunks
    span = nx // chunks
    f_cols[:, :, many:] = jnp.zeros((chunks, wide, 128 - many), F32)
    f_sends = []
    def product(i):
        c = (x // span + 1 + i) % chunks
        at = pl.ds(pl.multiple_of(c * wide, wide), wide)
        f_part[i] = lax.dot_general(m_rows[...], wd[:, at], NN, preferred_element_type=F32)

    def pack(i):
        c = (x // span + 1 + i) % chunks
        for j in range(wide // 128):
            f_cols[i, 128 * j:128 * (j + 1), 0:many] = jnp.transpose(f_part[i, :, 128 * j:128 * (j + 1)])
        for s in range(group):
            a0 = f_cols[i, cols * s:cols * s + 16, :]
            a1 = f_cols[i, cols * s + 16:cols * s + 32, :]
            a2 = lane_roll(f_cols[i, cols * s + 32:cols * s + 48, :], 64)
            f_send[c * group + s, 0:16] = jnp.where(lane16 < 64, a0, a2).astype(BF16)
            f_send[c * group + s, 16:32] = jnp.where(lane16 < 64, a1, tail_ref[c * group + s]).astype(BF16)

    product(0)
    for i in range(chunks):
        pack(i)
        if i + 1 < chunks:
            product(i + 1)
        if i == 0:
            pl.semaphore_wait(barrier, total - 1)
        c = (x // span + 1 + i) % chunks
        last = i == chunks - 1
        order = [((x + (2 if last else 0)) // 2 * 2 + p) % span for p in range(2)]
        order += [((x + (0 if last else 2)) // 2 * 2 + p) % span for p in range(2)]
        places = [(px, (y + d) % ny) for px in order for d in (2, 1, 3, 0)]
        if last:
            places = places[:8] + [((x + 1 - 2 * (x % 2)) % span, (y + d) % ny) for d in (2, 1, 3, 0)] + [(x % span, (y + d) % ny) for d in (2, 1, 3)]
        for qx, qy in places:
            j = qx * ny + qy
            s = c * group + j
            f_sends.append(remote(f_send.at[s], f_recv.at[slot], fs_sem.at[s], fr_sem.at[slot], j % ny, c * span + j // ny))
            f_sends[-1].start()
    f_recv[slot] = f_send[me]
    for k in range(1, total):
        s = (slot + k) % total
        remote(f_send.at[s], f_recv.at[s], fs_sem.at[s], fr_sem.at[s], (y + 1) % ny, x).wait_recv()

    sums = [[jnp.zeros((16, 128), F32) for _ in range(3)] for _ in range(ny)]
    olds = [[jnp.zeros((16, 128), F32) for _ in range(3)] for _ in range(ny)]
    for g in range(nx):
        low = f_recv[g, 0:16].astype(F32)
        for t in range(1, ny):
            low = low + f_recv[t * nx + g, 0:16].astype(F32)
        corner = [f_recv[t * nx + g, 16:32].astype(F32) for t in range(ny)]
        mid = corner[0]
        for t in range(1, ny):
            mid = mid + corner[t]
        high = lane_roll(low, 64)
        at = rows * g
        here = (lane16 >= at) & (lane16 < at + rows)
        for t in range(ny):
            for k, v in enumerate((low, mid, high)):
                sums[t][k] = jnp.where(here, lane_roll(v, at - rows * t), sums[t][k])
                olds[t][k] = jnp.where(here, lane_roll(corner[t], at - 64 - 16 * k), olds[t][k])
    for t in range(ny):
        for k in range(3):
            out_ref[16 * k:16 * (k + 1), 128 * t:128 * (t + 1)] = (olds[t][k] + sums[t][k]).astype(BF16)
    for copy in f_sends:
        copy.wait_send()


def solution(mesh):
    group_axes = ('yz', 'x')
    batch_axes = ('replica', 'yz', 'x')
    hidden_spec = P('replica', ('x', 'yz'))
    cache_spec = P(None, batch_axes, None, None)
    ny, nx = mesh.shape['yz'], mesh.shape['x']
    vmem = pl.BlockSpec(memory_space=pltpu.VMEM)
    hbm = pl.BlockSpec(memory_space=pl.ANY)
    dma = pltpu.SemaphoreType.DMA

    def layer(ht, seq_lens, attn_gain, mlp_gain, w_qkv, w_out, w_gate_up, w_down, k_cache, v_cache):
        cols = ht.shape[0]
        rows, slots, head_dim = k_cache.shape
        width = attn_gain.shape[1]
        qcols = w_qkv.shape[0]
        qpad = -(-qcols // 128) * 128
        heads = (qcols * ny) // head_dim - 2
        total = ny * nx
        many = ny * rows
        ffn = w_down.shape[0]
        ffn_pad = -(-ffn // 128) * 128
        in_hbm = functools.partial(pltpu.with_memory_space_constraint, memory_space=pltpu.HBM)
        parts = 4
        z, hrow, k_vmem, v_vmem, lens = pl.pallas_call(
            functools.partial(qkv_kernel, ny, nx, cols, rows, width),
            out_shape=(jax.ShapeDtypeStruct((ny, rows, qpad), BF16), jax.ShapeDtypeStruct((rows, width), F32),
                       pltpu.VMEM(k_cache.shape, BF16), pltpu.VMEM(v_cache.shape, BF16), pltpu.SMEM((rows,), jnp.int32)),
            in_specs=[hbm] * 6,
            out_specs=(vmem,) * 4 + (pl.BlockSpec(memory_space=pltpu.SMEM),),
            scratch_shapes=[
                pltpu.VMEM(ht.shape, BF16), pltpu.VMEM(attn_gain.shape, BF16),
                pltpu.VMEM((nx, cols // 16, 8, 128), BF16), pltpu.VMEM((total, cols // 16, 8, 128), BF16), pltpu.VMEM((qpad, width), BF16),
                pltpu.VMEM((width, 128), F32), pltpu.VMEM((width, 128), F32), pltpu.VMEM((width, 128), BF16),
                pltpu.VMEM((qpad, 128), F32), pltpu.VMEM((ny, rows, qpad), BF16), pltpu.VMEM((ny, rows, qpad), BF16),
                pltpu.VMEM((128, width), F32),
                dma, dma, dma, dma, dma((2, parts)), dma((total,)), dma((total,)), dma((ny,)), dma((ny,))],
            compiler_params=pltpu.CompilerParams(collective_id=0, has_side_effects=True, vmem_limit_bytes=12 << 20),
            cost_estimate=pl.CostEstimate(flops=8_000_000_000, bytes_accessed=20_000_000, transcendentals=0),
            name='qkv',
        )(in_hbm(seq_lens), in_hbm(ht), in_hbm(attn_gain), in_hbm(w_qkv), in_hbm(k_cache), in_hbm(v_cache))
        k_new, v_new, o, _, _ = pl.pallas_call(
            functools.partial(attend_kernel, heads, qcols, head_dim ** -0.5),
            out_shape=(pltpu.HBM(k_cache.shape, BF16), pltpu.HBM(v_cache.shape, BF16),
                       jax.ShapeDtypeStruct((heads, rows, head_dim), BF16),
                       pltpu.VMEM(k_cache.shape, BF16), pltpu.VMEM(v_cache.shape, BF16)),
            in_specs=[pl.BlockSpec(memory_space=pltpu.SMEM), vmem, vmem, vmem],
            out_specs=(hbm, hbm, vmem, vmem, vmem),
            input_output_aliases={2: 3, 3: 4},
            scratch_shapes=[pltpu.VMEM((rows, 16, head_dim), F32), pltpu.VMEM((2, rows, head_dim), F32), pltpu.VMEM((2, 32, slots), F32), pltpu.VMEM((rows, 16, head_dim), F32), dma((rows,)), dma((rows,))],
            compiler_params=pltpu.CompilerParams(vmem_limit_bytes=8 << 20),
            cost_estimate=pl.CostEstimate(flops=8_000_000_000, bytes_accessed=20_000_000, transcendentals=0),
            name='attend',
        )(lens, z, k_vmem, v_vmem)
        u, tail, wgu_vmem, wd_vmem = pl.pallas_call(
            functools.partial(proj_kernel, ny, nx, cols, rows, width, heads),
            out_shape=(pltpu.VMEM((128, width), BF16), pltpu.VMEM((total, 16, 128), F32),
                       pltpu.VMEM(w_gate_up.shape, BF16), pltpu.VMEM((ffn_pad, width), BF16)),
            in_specs=[vmem, vmem, hbm, hbm, hbm, hbm],
            out_specs=(vmem,) * 4,
            scratch_shapes=[
                pltpu.VMEM(mlp_gain.shape, BF16), pltpu.VMEM(w_out.shape, BF16),
                pltpu.VMEM((ny, heads // ny, rows, head_dim), BF16),
                pltpu.VMEM((ny, rows, width), BF16), pltpu.VMEM((ny, rows, width), BF16),
                pltpu.VMEM((rows, width), BF16), pltpu.VMEM((ny, rows, width), BF16),
                pltpu.VMEM((128, width), F32), pltpu.VMEM((width, 128), F32),
                dma, dma, dma((5,)), dma, dma((ny,)), dma((ny,)),
                dma((2, ny)), dma((2, ny)), dma((2, ny)), dma((2, ny))],
            compiler_params=pltpu.CompilerParams(collective_id=1, has_side_effects=True, vmem_limit_bytes=12 << 20),
            cost_estimate=pl.CostEstimate(flops=8_000_000_000, bytes_accessed=20_000_000, transcendentals=0),
            name='proj',
        )(o, hrow, in_hbm(mlp_gain), in_hbm(w_out), in_hbm(w_gate_up), in_hbm(w_down))
        out = pl.pallas_call(
            functools.partial(mlp_kernel, ny, nx, cols, rows, width, ffn),
            out_shape=jax.ShapeDtypeStruct(ht.shape, BF16),
            in_specs=[vmem] * 4,
            out_specs=vmem,
            scratch_shapes=[
                pltpu.VMEM((many, ffn_pad), BF16), pltpu.VMEM((2, many, width // 2), F32), pltpu.VMEM((2, width // 2, 128), F32),
                pltpu.VMEM((total, 32, 128), BF16), pltpu.VMEM((total, 32, 128), BF16), dma((total,)), dma((total,))],
            compiler_params=pltpu.CompilerParams(collective_id=2, has_side_effects=True, vmem_limit_bytes=12 << 20),
            cost_estimate=pl.CostEstimate(flops=8_000_000_000, bytes_accessed=20_000_000, transcendentals=0),
            name='mlp',
        )(u, tail, wgu_vmem, wd_vmem)
        return out, k_new, v_new

    def local_step(hidden, seq_lens, attn_gain, mlp_gain, w_qkv, w_out, w_gate_up, w_down, k_cache, v_cache):
        ht = hidden.T
        k_layers = []
        v_layers = []
        for i in range(w_qkv.shape[0]):
            ht, k_new, v_new = layer(ht, seq_lens, attn_gain[i:i + 1], mlp_gain[i:i + 1], w_qkv[i].T, w_out[i],
                                     jnp.transpose(w_gate_up[i], (1, 2, 0)), w_down[i], k_cache[i], v_cache[i])
            k_layers.append(k_new)
            v_layers.append(v_new)
        return ht.T, jnp.stack(k_layers), jnp.stack(v_layers)

    return jax.shard_map(
        local_step,
        mesh=mesh,
        in_specs=(hidden_spec, P(batch_axes), P(None, None), P(None, None), P(None, None, 'yz'), P(None, 'yz', None),
                  P(None, None, None, 'yz'), P(None, 'yz', None), cache_spec, cache_spec),
        out_specs=(hidden_spec, cache_spec, cache_spec),
        check_vma=False)
```

```python
import functools

import jax
import jax.numpy as jnp
from jax import lax
from jax.experimental import pallas as pl
from jax.experimental.pallas import tpu as pltpu
from jax.sharding import PartitionSpec as P

NORM_EPS = 1e-5
MESH = pl.DeviceIdType.MESH
F32 = jnp.float32
BF16 = jnp.bfloat16
NT = (((1,), (1,)), ((), ()))
NN = (((1,), (0,)), ((), ()))


def lane_ids(shape):
    return lax.broadcasted_iota(jnp.int32, shape, len(shape) - 1)


def lane_roll(v, shift):
    shift = shift % v.shape[-1]
    return v if shift == 0 else pltpu.roll(v, shift, v.ndim - 1)


def peers(y, x, ny, nx):
    ys = [(y + d) % ny for d in range(ny)]
    xs = [(x + d) % nx for d in range(nx)]
    far_y = sorted(range(ny), key=lambda d: -min(d, ny - d))
    far_x = sorted(range(nx), key=lambda d: -min(d, nx - d))
    return [(dy * nx + dx, ys[dy], xs[dx]) for dx in far_x for dy in far_y if dy or dx]


def ring(y, x, ny):
    far = sorted(range(1, ny), key=lambda d: -min(d, ny - d))
    return [(d, (y + d) % ny, x) for d in far]


def greet_all(others):
    barrier = pltpu.get_barrier_semaphore()
    for _, py, px in others:
        pl.semaphore_signal(barrier, inc=1, device_id={'yz': py, 'x': px}, device_id_type=MESH)
    return barrier


def remote(src, dst, send_sem, recv_sem, py, px):
    return pltpu.make_async_remote_copy(src_ref=src, dst_ref=dst, send_sem=send_sem, recv_sem=recv_sem,
                                        device_id={'yz': py, 'x': px}, device_id_type=MESH)


def qkv_kernel(ny, nx, cols, rows, width, len_hbm, ht_hbm, gain_hbm, w_hbm, k_hbm, v_hbm, z_ref, hrow_ref, k_ref, v_ref, len_ref,
               ht_ref, gain_ref, send_buf, recv_buf, w_vmem, gain_col, h_full, u_full, zt_buf, z_send, z_recv, h_rows,
               len_sem, h_sem, g_sem, w_sem, kv_sem, send_sem, recv_sem, zsend_sem, zrecv_sem):
    y, x = lax.axis_index('yz'), lax.axis_index('x')
    total = ny * nx
    me = x * ny + y
    qcols = w_hbm.shape[0]
    h_copy = pltpu.make_async_copy(ht_hbm, ht_ref, h_sem)
    h_copy.start()
    others = peers(y, x, ny, nx)
    barrier = greet_all(others)
    g_copy = pltpu.make_async_copy(gain_hbm, gain_ref, g_sem)
    g_copy.start()
    len_copy = pltpu.make_async_copy(len_hbm, len_ref, len_sem)
    len_copy.start()
    w_copy = pltpu.make_async_copy(w_hbm, w_vmem.at[pl.ds(0, qcols)], w_sem)
    w_copy.start()
    parts = kv_sem.shape[1]
    share = k_hbm.shape[0] // parts
    kv_copies = [pltpu.make_async_copy(src.at[pl.ds(i * share, share)], dst.at[pl.ds(i * share, share)], kv_sem.at[c, i])
                 for i in range(parts) for c, (src, dst) in enumerate(((k_hbm, k_ref), (v_hbm, v_ref)))]
    for copy in kv_copies:
        copy.start()
    h_copy.wait()

    lane = lane_ids((cols, 128))
    lane16 = lane_ids((16, 128))
    half = cols // 2
    tiles = [ht_ref[:, 128 * t:128 * (t + 1)].astype(F32) for t in range(ny)]
    for g in range(nx):
        block = jnp.zeros((cols, 128), F32)
        for t in range(ny):
            piece = lane_roll(tiles[t], rows * t - rows * g)
            block = jnp.where((lane >= rows * t) & (lane < rows * (t + 1)), piece, block)
        block = jnp.where(lane[0:half] < 64, block[0:half], lane_roll(block[half:cols], 64))
        for k in range(half // 8):
            send_buf[g, k] = block[8 * k:8 * (k + 1)].astype(BF16)

    pl.semaphore_wait(barrier, total - 1)

    h_sends = [remote(send_buf.at[px], recv_buf.at[me], send_sem.at[d], recv_sem.at[d], py, px) for d, py, px in others]
    for copy in h_sends:
        copy.start()
    recv_buf[me] = send_buf[x]

    g_copy.wait()
    for j in range(width // 128):
        row = gain_ref[0:1, 128 * j:128 * (j + 1)].astype(F32)
        gain_col[128 * j:128 * (j + 1), :] = jnp.transpose(jnp.broadcast_to(row, (128, 128)))
    w_vmem[qcols:, :] = jnp.zeros((w_vmem.shape[0] - qcols, width), BF16)

    for copy in h_sends:
        copy.wait()

    square = jnp.zeros((8, 128), F32)
    for s in range(total):
        for k in range(half // 8):
            low = recv_buf[s, k].astype(F32)
            high = lane_roll(low, 64)
            h_full[cols * s + 8 * k:cols * s + 8 * (k + 1), :] = low
            h_full[cols * s + half + 8 * k:cols * s + half + 8 * (k + 1), :] = high
            square = square + low * low + high * high
    power = jnp.sum(square, axis=0, keepdims=True)
    inv = lax.rsqrt(power / width + NORM_EPS)
    u_full[...] = (h_full[...] * inv * gain_col[...]).astype(BF16)
    w_copy.wait()
    zt_buf[...] = lax.dot_general(w_vmem[...], u_full[...], NN, preferred_element_type=F32)
    for j in range(zt_buf.shape[0] // 128):
        zj = jnp.transpose(zt_buf[128 * j:128 * (j + 1), :])
        for t in range(ny):
            z_send[t, :, 128 * j:128 * (j + 1)] = zj[rows * t:rows * (t + 1)].astype(BF16)
    z_sends = [remote(z_send.at[py], z_recv.at[y], zsend_sem.at[d], zrecv_sem.at[d], py, px) for d, py, px in ring(y, x, ny)]
    for copy in z_sends:
        copy.start()
    z_recv[y] = z_send[y]

    for j in range(width // 128):
        h_rows[:, 128 * j:128 * (j + 1)] = jnp.transpose(h_full[128 * j:128 * (j + 1), :])
    hrow_ref[...] = h_rows[pl.ds(pl.multiple_of(y * rows, rows), rows), :]

    for copy in z_sends:
        copy.wait()

    z_ref[...] = z_recv[...]
    for copy in kv_copies + [len_copy]:
        copy.wait()


def attend_kernel(heads, qcols, scale, len_ref, z_recv, k_in, v_in, k_hbm, v_hbm, o_ref, k_ref, v_ref, z_ref, new_rows, s_buf, o_acc, k_sem, v_sem):
    rows, slots = k_ref.shape[:2]
    ny = z_recv.shape[0]
    lane16 = lane_ids((16, 128))

    def column(g):
        t, off = 128 * g // qcols, 128 * g % qcols
        j, sh = off // 128, off % 128
        take = min(128, qcols - off)

        def tile(t, j):
            return z_recv[t, :, 128 * j:128 * (j + 1)].astype(F32)

        out = lane_roll(tile(t, j), -sh)
        if sh and take > 128 - sh:
            out = jnp.where(lane16 < 128 - sh, out, lane_roll(tile(t, j + 1), -sh))
        if take < 128:
            out = jnp.where(lane16 < take, out, lane_roll(tile(t + 1, 0), take))
        return out

    new_rows[0] = column(heads)
    new_rows[1] = column(heads + 1)

    def place(b):
        length = len_ref[b]
        base = pl.multiple_of((length // 16) * 16, 16)
        here = lax.broadcasted_iota(jnp.int32, (16, 128), 0) == length - base
        k_new = jnp.broadcast_to(new_rows[0, pl.ds(b, 1), :], (16, 128)).astype(BF16)
        v_new = jnp.broadcast_to(new_rows[1, pl.ds(b, 1), :], (16, 128)).astype(BF16)
        k_ref[b, pl.ds(base, 16), :] = jnp.where(here, k_new, k_ref[b, pl.ds(base, 16), :])
        v_ref[b, pl.ds(base, 16), :] = jnp.where(here, v_new, v_ref[b, pl.ds(base, 16), :])

    def k_copy(b):
        return pltpu.make_async_copy(k_ref.at[b], k_hbm.at[b], k_sem.at[b])

    def v_copy(b):
        return pltpu.make_async_copy(v_ref.at[b], v_hbm.at[b], v_sem.at[b])

    def score(i, slot):
        blank = jnp.zeros((16, 128), BF16)
        q0, q1 = z_ref[2 * i].astype(BF16), z_ref[2 * i + 1].astype(BF16)
        q = jnp.concatenate([jnp.concatenate([q0, blank], axis=1), jnp.concatenate([blank, q1], axis=1)], axis=0)
        keys = jnp.concatenate([k_ref[2 * i], k_ref[2 * i + 1]], axis=1)
        s_buf[slot] = lax.dot_general(q, keys, NT, preferred_element_type=F32) * scale

    def finish(i, slot):
        s = s_buf[slot]
        first = lax.broadcasted_iota(jnp.int32, (32, 1), 0) < 16
        length = jnp.where(first, len_ref[2 * i], len_ref[2 * i + 1])
        s = jnp.where(lane_ids(s.shape) <= length, s, -1e30)
        e = jnp.exp(s - jnp.max(s, axis=1, keepdims=True))
        p = (e * (1.0 / jnp.sum(e, axis=1, keepdims=True))).astype(BF16)
        values = jnp.concatenate([v_ref[2 * i], v_ref[2 * i + 1]], axis=1)
        o = lax.dot_general(p, values, NN, preferred_element_type=F32)
        o_acc[2 * i] = o[0:16, 0:128]
        o_acc[2 * i + 1] = o[16:32, 128:256]

    def leave(b, carry):
        k_copy(b).start()
        v_copy(b).start()
        return carry

    def enter(i, carry):
        place(2 * i)
        place(2 * i + 1)
        leave(2 * i - 2, 0)
        leave(2 * i - 1, 0)
        return carry

    place(0)
    place(1)
    lax.fori_loop(1, rows // 2, enter, 0)
    lax.fori_loop(rows - 2, rows, leave, 0)
    for h in range(heads):
        z_ref[:, h, :] = column(h)
    for h in range(heads, 16):
        z_ref[:, h, :] = jnp.zeros((rows, 128), F32)
    score(0, 0)
    for i in range(rows // 2 - 1):
        score(i + 1, (i + 1) % 2)
        finish(i, i % 2)
    finish(rows // 2 - 1, (rows // 2 - 1) % 2)
    for h in range(heads):
        o_ref[h] = o_acc[:, h, :].astype(BF16)

    def drain(b, carry):
        k_copy(b).wait()
        v_copy(b).wait()
        return carry

    lax.fori_loop(0, rows, drain, 0)


def proj_kernel(ny, nx, cols, rows, width, heads, o_ref, hrow_ref, gain_hbm, wo_hbm, wgu_hbm, wd_hbm,
                h_ref, gain_ref, tail_ref, wgu_ref, wd_ref,
                wo, o_recv, p_send, p_recv, hm_send, hm_recv, hm_rows, hm_cols,
                gain_sem, wo_sem, wgu_sem, wd_sem, os_sem, or_sem, ps_sem, pr_sem, hs_sem, hr_sem):
    y, x = lax.axis_index('yz'), lax.axis_index('x')
    total = ny * nx
    heads_y = heads // ny
    ffn = wd_hbm.shape[0]
    group = ring(y, x, ny)
    barrier = pltpu.get_barrier_semaphore()
    for _, py, px in group:
        pl.semaphore_signal(barrier, inc=1, device_id={'yz': py, 'x': px}, device_id_type=MESH)
    wo_copy = pltpu.make_async_copy(wo_hbm, wo, wo_sem)
    gain_copy = pltpu.make_async_copy(gain_hbm, gain_ref, gain_sem)
    parts = wgu_sem.shape[0]
    share = ffn // parts
    loads = [pltpu.make_async_copy(wgu_hbm.at[:, pl.ds(c * share, share)], wgu_ref.at[:, pl.ds(c * share, share)], wgu_sem.at[c])
             for c in range(parts)]
    loads.append(pltpu.make_async_copy(wd_hbm, wd_ref.at[pl.ds(0, ffn)], wd_sem))
    for copy in [wo_copy, gain_copy] + loads:
        copy.start()
    pl.semaphore_wait(barrier, ny - 1)

    o_sends = [remote(o_ref.at[pl.ds(py * heads_y, heads_y)], o_recv.at[y], os_sem.at[d], or_sem.at[d], py, px) for d, py, px in group]
    for copy in o_sends:
        copy.start()
    o_recv[y] = o_ref[pl.ds(y * heads_y, heads_y)]
    wd_ref[ffn:, :] = jnp.zeros((wd_ref.shape[0] - ffn, width), BF16)
    wo_copy.wait()
    for copy in o_sends:
        copy.wait()
    o_rows = [jnp.concatenate([o_recv[t, h] for t in range(ny)], axis=0) for h in range(heads_y)]
    o_full = jnp.concatenate(o_rows, axis=1)

    halves = ps_sem.shape[0]
    wide = width // halves

    def p_copies(c):
        at = pl.ds(c * wide, wide)
        return [remote(p_send.at[py, :, at], p_recv.at[y, :, at], ps_sem.at[c, d], pr_sem.at[c, d], py, px) for d, py, px in group]

    def h_copies(c):
        at = pl.ds(c * wide, wide)
        return [remote(hm_send.at[:, at], hm_recv.at[y, :, at], hs_sem.at[c, d], hr_sem.at[c, d], py, px) for d, py, px in group]

    for c in range(halves):
        at = slice(c * wide, (c + 1) * wide)
        part = lax.dot_general(o_full, wo[:, at], NN, preferred_element_type=F32).astype(BF16)
        for t in range(ny):
            p_send[t, :, at] = part[rows * t:rows * (t + 1)]
        for copy in p_copies(c):
            copy.start()
        p_recv[y, :, at] = p_send[y, :, at]
    for c in range(halves):
        at = slice(c * wide, (c + 1) * wide)
        for copy in p_copies(c):
            copy.wait()
        summed = p_recv[0, :, at].astype(F32)
        for t in range(1, ny):
            summed = summed + p_recv[t, :, at].astype(F32)
        hm_send[:, at] = (hrow_ref[:, at] + summed).astype(BF16)
        for copy in h_copies(c):
            copy.start()
    h_mid = hm_send[...]
    hm_recv[y] = h_mid

    hm_rows[0:rows, :] = h_mid.astype(F32)
    hm_rows[rows:, :] = jnp.zeros((hm_rows.shape[0] - rows, width), F32)
    for j in range(width // 128):
        hm_cols[128 * j:128 * (j + 1), :] = jnp.transpose(hm_rows[:, 128 * j:128 * (j + 1)])
    for s in range(total):
        corner = jnp.zeros((16, 128), F32)
        for k in range(cols // 16):
            corner = corner + lane_roll(hm_cols[cols * s + 16 * k:cols * s + 16 * (k + 1), :], 64 + 16 * k)
        tail_ref[s] = corner

    gain_copy.wait()
    for c in range(halves):
        for copy in h_copies(c):
            copy.wait()
    h_ref[...] = hm_recv[...]
    for copy in loads:
        copy.wait()


def mlp_kernel(ny, nx, cols, rows, width, ffn, h_ref, gain_ref, tail_ref, wgu, wd, out_ref, u_ref, m_rows, f_part, f_cols, f_send, f_recv, fs_sem, fr_sem):
    y, x = lax.axis_index('yz'), lax.axis_index('x')
    total = ny * nx
    me = x * ny + y
    slot = y * nx + x
    many = ny * rows
    barrier = greet_all(peers(y, x, ny, nx))
    lane16 = lane_ids((16, 128))
    h64 = jnp.concatenate([h_ref[t] for t in range(ny)], axis=0).astype(F32)
    inv = lax.rsqrt(jnp.sum(h64 * h64, axis=1, keepdims=True) / width + NORM_EPS)
    u_ref[0:many, :] = (h64 * inv * gain_ref[...].astype(F32)).astype(BF16)
    u_ref[many:, :] = jnp.zeros((u_ref.shape[0] - many, width), BF16)

    for base in range(0, ffn, 512):
        size = min(512, ffn - base)
        gate = lax.dot_general(wgu[0, base:base + size, :], u_ref[...], NT, preferred_element_type=F32)
        up = lax.dot_general(wgu[1, base:base + size, :], u_ref[...], NT, preferred_element_type=F32)
        gate = gate.astype(BF16).astype(F32)
        m = jax.nn.silu(gate) * up.astype(BF16).astype(F32)
        if size % 128:
            m = jnp.concatenate([m, jnp.zeros((128 - size % 128, 128), F32)], axis=0)
        for j in range(m.shape[0] // 128):
            m_rows[:, base + 128 * j:base + 128 * (j + 1)] = jnp.transpose(m[128 * j:128 * (j + 1)])[0:many].astype(BF16)

    chunks = f_cols.shape[0]
    wide = width // chunks
    group = total // chunks
    span = nx // chunks
    f_cols[:, :, many:] = jnp.zeros((chunks, wide, 128 - many), F32)
    f_sends = []
    def product(i):
        c = (x // span + 1 + i) % chunks
        at = pl.ds(pl.multiple_of(c * wide, wide), wide)
        f_part[i] = lax.dot_general(m_rows[...], wd[:, at], NN, preferred_element_type=F32)

    def pack(i):
        c = (x // span + 1 + i) % chunks
        for j in range(wide // 128):
            f_cols[i, 128 * j:128 * (j + 1), 0:many] = jnp.transpose(f_part[i, :, 128 * j:128 * (j + 1)])
        for s in range(group):
            a0 = f_cols[i, cols * s:cols * s + 16, :]
            a1 = f_cols[i, cols * s + 16:cols * s + 32, :]
            a2 = lane_roll(f_cols[i, cols * s + 32:cols * s + 48, :], 64)
            f_send[c * group + s, 0:16] = jnp.where(lane16 < 64, a0, a2).astype(BF16)
            f_send[c * group + s, 16:32] = jnp.where(lane16 < 64, a1, tail_ref[c * group + s]).astype(BF16)

    product(0)
    for i in range(chunks):
        pack(i)
        if i + 1 < chunks:
            product(i + 1)
        if i == 0:
            pl.semaphore_wait(barrier, total - 1)
        c = (x // span + 1 + i) % chunks
        last = i == chunks - 1
        order = [((x + (2 if last else 0)) // 2 * 2 + p) % span for p in range(2)]
        order += [((x + (0 if last else 2)) // 2 * 2 + p) % span for p in range(2)]
        places = [(px, (y + d) % ny) for px in order for d in (2, 1, 3, 0)]
        if last:
            places = places[:8] + [((x + 1 - 2 * (x % 2)) % span, (y + d) % ny) for d in (2, 1, 3, 0)] + [(x % span, (y + d) % ny) for d in (2, 1, 3)]
        for qx, qy in places:
            j = qx * ny + qy
            s = c * group + j
            f_sends.append(remote(f_send.at[s], f_recv.at[slot], fs_sem.at[s], fr_sem.at[slot], j % ny, c * span + j // ny))
            f_sends[-1].start()
    f_recv[slot] = f_send[me]
    for k in range(1, total):
        s = (slot + k) % total
        remote(f_send.at[s], f_recv.at[s], fs_sem.at[s], fr_sem.at[s], (y + 1) % ny, x).wait_recv()

    sums = [[jnp.zeros((16, 128), F32) for _ in range(3)] for _ in range(ny)]
    olds = [[jnp.zeros((16, 128), F32) for _ in range(3)] for _ in range(ny)]
    for g in range(nx):
        low = f_recv[g, 0:16].astype(F32)
        for t in range(1, ny):
            low = low + f_recv[t * nx + g, 0:16].astype(F32)
        corner = [f_recv[t * nx + g, 16:32].astype(F32) for t in range(ny)]
        mid = corner[0]
        for t in range(1, ny):
            mid = mid + corner[t]
        high = lane_roll(low, 64)
        at = rows * g
        here = (lane16 >= at) & (lane16 < at + rows)
        for t in range(ny):
            for k, v in enumerate((low, mid, high)):
                sums[t][k] = jnp.where(here, lane_roll(v, at - rows * t), sums[t][k])
                olds[t][k] = jnp.where(here, lane_roll(corner[t], at - 64 - 16 * k), olds[t][k])
    for t in range(ny):
        for k in range(3):
            out_ref[16 * k:16 * (k + 1), 128 * t:128 * (t + 1)] = (olds[t][k] + sums[t][k]).astype(BF16)
    for copy in f_sends:
        copy.wait_send()


def solution(mesh):
    group_axes = ('yz', 'x')
    batch_axes = ('replica', 'yz', 'x')
    hidden_spec = P('replica', ('x', 'yz'))
    cache_spec = P(None, batch_axes, None, None)
    ny, nx = mesh.shape['yz'], mesh.shape['x']
    vmem = pl.BlockSpec(memory_space=pltpu.VMEM)
    hbm = pl.BlockSpec(memory_space=pl.ANY)
    dma = pltpu.SemaphoreType.DMA

    def layer(ht, seq_lens, attn_gain, mlp_gain, w_qkv, w_out, w_gate_up, w_down, k_cache, v_cache):
        cols = ht.shape[0]
        rows, slots, head_dim = k_cache.shape
        width = attn_gain.shape[1]
        qcols = w_qkv.shape[0]
        qpad = -(-qcols // 128) * 128
        heads = (qcols * ny) // head_dim - 2
        total = ny * nx
        many = ny * rows
        ffn = w_down.shape[0]
        ffn_pad = -(-ffn // 128) * 128
        in_hbm = functools.partial(pltpu.with_memory_space_constraint, memory_space=pltpu.HBM)
        parts = 4
        z, hrow, k_vmem, v_vmem, lens = pl.pallas_call(
            functools.partial(qkv_kernel, ny, nx, cols, rows, width),
            out_shape=(jax.ShapeDtypeStruct((ny, rows, qpad), BF16), jax.ShapeDtypeStruct((rows, width), F32),
                       pltpu.VMEM(k_cache.shape, BF16), pltpu.VMEM(v_cache.shape, BF16), pltpu.SMEM((rows,), jnp.int32)),
            in_specs=[hbm] * 6,
            out_specs=(vmem,) * 4 + (pl.BlockSpec(memory_space=pltpu.SMEM),),
            scratch_shapes=[
                pltpu.VMEM(ht.shape, BF16), pltpu.VMEM(attn_gain.shape, BF16),
                pltpu.VMEM((nx, cols // 16, 8, 128), BF16), pltpu.VMEM((total, cols // 16, 8, 128), BF16), pltpu.VMEM((qpad, width), BF16),
                pltpu.VMEM((width, 128), F32), pltpu.VMEM((width, 128), F32), pltpu.VMEM((width, 128), BF16),
                pltpu.VMEM((qpad, 128), F32), pltpu.VMEM((ny, rows, qpad), BF16), pltpu.VMEM((ny, rows, qpad), BF16),
                pltpu.VMEM((128, width), F32),
                dma, dma, dma, dma, dma((2, parts)), dma((total,)), dma((total,)), dma((ny,)), dma((ny,))],
            compiler_params=pltpu.CompilerParams(collective_id=0, has_side_effects=True, vmem_limit_bytes=12 << 20),
            cost_estimate=pl.CostEstimate(flops=8_000_000_000, bytes_accessed=20_000_000, transcendentals=0),
            name='qkv',
        )(in_hbm(seq_lens), in_hbm(ht), in_hbm(attn_gain), in_hbm(w_qkv), in_hbm(k_cache), in_hbm(v_cache))
        k_new, v_new, o, _, _ = pl.pallas_call(
            functools.partial(attend_kernel, heads, qcols, head_dim ** -0.5),
            out_shape=(pltpu.HBM(k_cache.shape, BF16), pltpu.HBM(v_cache.shape, BF16),
                       jax.ShapeDtypeStruct((heads, rows, head_dim), BF16),
                       pltpu.VMEM(k_cache.shape, BF16), pltpu.VMEM(v_cache.shape, BF16)),
            in_specs=[pl.BlockSpec(memory_space=pltpu.SMEM), vmem, vmem, vmem],
            out_specs=(hbm, hbm, vmem, vmem, vmem),
            input_output_aliases={2: 3, 3: 4},
            scratch_shapes=[pltpu.VMEM((rows, 16, head_dim), F32), pltpu.VMEM((2, rows, head_dim), F32), pltpu.VMEM((2, 32, slots), F32), pltpu.VMEM((rows, 16, head_dim), F32), dma((rows,)), dma((rows,))],
            compiler_params=pltpu.CompilerParams(vmem_limit_bytes=8 << 20),
            cost_estimate=pl.CostEstimate(flops=8_000_000_000, bytes_accessed=20_000_000, transcendentals=0),
            name='attend',
        )(lens, z, k_vmem, v_vmem)
        h_mid, gain, tail, wgu_vmem, wd_vmem = pl.pallas_call(
            functools.partial(proj_kernel, ny, nx, cols, rows, width, heads),
            out_shape=(pltpu.VMEM((ny, rows, width), BF16), pltpu.VMEM(mlp_gain.shape, BF16), pltpu.VMEM((total, 16, 128), F32),
                       pltpu.VMEM(w_gate_up.shape, BF16), pltpu.VMEM((ffn_pad, width), BF16)),
            in_specs=[vmem, vmem, hbm, hbm, hbm, hbm],
            out_specs=(vmem,) * 5,
            scratch_shapes=[
                pltpu.VMEM(w_out.shape, BF16),
                pltpu.VMEM((ny, heads // ny, rows, head_dim), BF16),
                pltpu.VMEM((ny, rows, width), BF16), pltpu.VMEM((ny, rows, width), BF16),
                pltpu.VMEM((rows, width), BF16), pltpu.VMEM((ny, rows, width), BF16),
                pltpu.VMEM((128, width), F32), pltpu.VMEM((width, 128), F32),
                dma, dma, dma((5,)), dma, dma((ny,)), dma((ny,)),
                dma((3, ny)), dma((3, ny)), dma((3, ny)), dma((3, ny))],
            compiler_params=pltpu.CompilerParams(collective_id=1, has_side_effects=True, vmem_limit_bytes=12 << 20),
            cost_estimate=pl.CostEstimate(flops=8_000_000_000, bytes_accessed=20_000_000, transcendentals=0),
            name='proj',
        )(o, hrow, in_hbm(mlp_gain), in_hbm(w_out), in_hbm(w_gate_up), in_hbm(w_down))
        out = pl.pallas_call(
            functools.partial(mlp_kernel, ny, nx, cols, rows, width, ffn),
            out_shape=jax.ShapeDtypeStruct(ht.shape, BF16),
            in_specs=[vmem] * 5,
            out_specs=vmem,
            scratch_shapes=[
                pltpu.VMEM((128, width), BF16), pltpu.VMEM((many, ffn_pad), BF16), pltpu.VMEM((2, many, width // 2), F32), pltpu.VMEM((2, width // 2, 128), F32),
                pltpu.VMEM((total, 32, 128), BF16), pltpu.VMEM((total, 32, 128), BF16), dma((total,)), dma((total,))],
            compiler_params=pltpu.CompilerParams(collective_id=2, has_side_effects=True, vmem_limit_bytes=12 << 20),
            cost_estimate=pl.CostEstimate(flops=8_000_000_000, bytes_accessed=20_000_000, transcendentals=0),
            name='mlp',
        )(h_mid, gain, tail, wgu_vmem, wd_vmem)
        return out, k_new, v_new

    def local_step(hidden, seq_lens, attn_gain, mlp_gain, w_qkv, w_out, w_gate_up, w_down, k_cache, v_cache):
        ht = hidden.T
        k_layers = []
        v_layers = []
        for i in range(w_qkv.shape[0]):
            ht, k_new, v_new = layer(ht, seq_lens, attn_gain[i:i + 1], mlp_gain[i:i + 1], w_qkv[i].T, w_out[i],
                                     jnp.transpose(w_gate_up[i], (1, 2, 0)), w_down[i], k_cache[i], v_cache[i])
            k_layers.append(k_new)
            v_layers.append(v_new)
        return ht.T, jnp.stack(k_layers), jnp.stack(v_layers)

    return jax.shard_map(
        local_step,
        mesh=mesh,
        in_specs=(hidden_spec, P(batch_axes), P(None, None), P(None, None), P(None, None, 'yz'), P(None, 'yz', None),
                  P(None, None, None, 'yz'), P(None, 'yz', None), cache_spec, cache_spec),
        out_specs=(hidden_spec, cache_spec, cache_spec),
        check_vma=False)
```
